32 devices in a mesh: dp: 4 (over y, z), tp: 8 (over x, core).
Axes of the slice: x: 4, y: 2, z: 2, core: 2. Of those that a mesh axis runs over, the one named last changes fastest.
The devices are a block of a 4x4x8 slice.
Arguments:
- layer_in: bfloat16 [8, 1024, 1024], P('dp', 'tp'), parts along dimension 0
- grad_out: bfloat16 [8, 1024, 1024], P('dp', 'tp'), parts along dimension 0
- w_qkv: bfloat16 [1024, 16, 3, 64], P(None, 'tp')
- w_out: bfloat16 [16, 1, 64, 1024], P('tp')
- w_up: bfloat16 [1024, 4096], P(None, 'tp')
- w_down: bfloat16 [4096, 1024], P('tp')
- ln_params: float32 [4, 1024], replicated
Outputs:
- output 1: bfloat16 [8, 1024, 1024], P('dp', 'tp'), parts along dimension 0
- output 2: bfloat16 [4096, 16, 3, 64], P('dp', 'tp'), parts along dimension 0
- output 3: bfloat16 [64, 1, 64, 1024], P(('dp', 'tp')), parts along dimension 0
- output 4: bfloat16 [4096, 4096], P('dp', 'tp'), parts along dimension 0
- output 5: bfloat16 [16384, 1024], P(('dp', 'tp')), parts along dimension 0
- output 6: float32 [16, 1024], P('dp'), parts along dimension 0
There are 4 independent parts. The reference program is written for one: setup_inputs(seed, part) draws one part's arguments, and reference() takes and returns one part's arrays. A program takes and returns all parts, laid end to end along the dimension named above; an argument that names none is the same for every part.
All inputs are finite; a program needn't handle non-finite values.
Results may differ from the reference program's by a relative error of at most 0.0061746.
Values are sent between devices in bfloat16 or wider.
A program may use at most 768 MiB of HBM per device.

```python
import jax
import jax.numpy as jnp
from jax import lax

D = 1024
HEADS = 16
KV_HEADS = 16
HEAD = 64
FF = 4096
BATCH = 2
SEQ = 1024

NORM_EPS = 1e-5
ROPE_BASE = 10000.0
NEG_BIG = -1e30


def setup_inputs(seed: int = 0, part: int = 0) -> dict:
    part_key = jax.random.fold_in(jax.random.key(seed), part)
    key_in, key_grad = jax.random.split(part_key, 2)
    key_qkv, key_out, key_up, key_down, key_norm = jax.random.split(jax.random.key(seed + 1), 5)
    group_size = HEADS // KV_HEADS
    layer_in = jax.random.normal(key_in, (BATCH, SEQ, D), jnp.float32).astype(jnp.bfloat16)
    grad_out = jax.random.normal(key_grad, (BATCH, SEQ, D), jnp.float32).astype(jnp.bfloat16)
    w_qkv = (jax.random.normal(key_qkv, (D, KV_HEADS, group_size + 2, HEAD), jnp.float32) * D ** -0.5).astype(jnp.bfloat16)
    w_out = (jax.random.normal(key_out, (KV_HEADS, group_size, HEAD, D), jnp.float32) * (HEADS * HEAD) ** -0.5).astype(jnp.bfloat16)
    w_up = (jax.random.normal(key_up, (D, FF), jnp.float32) * D ** -0.5).astype(jnp.bfloat16)
    w_down = (jax.random.normal(key_down, (FF, D), jnp.float32) * FF ** -0.5).astype(jnp.bfloat16)
    centre = jnp.array([1.0, 0.0, 1.0, 0.0], jnp.float32)
    ln_params = centre[:, None] + 0.25 * jax.random.normal(key_norm, (4, D), jnp.float32)
    return {'layer_in': layer_in, 'grad_out': grad_out, 'w_qkv': w_qkv, 'w_out': w_out, 'w_up': w_up, 'w_down': w_down, 'ln_params': ln_params}


def norm_stats(source):
    widened = source.astype(jnp.float32)
    centred = widened - jnp.mean(widened, axis=-1, keepdims=True)
    inv_std = lax.rsqrt(jnp.mean(centred * centred, axis=-1, keepdims=True) + NORM_EPS)
    return centred * inv_std, inv_std


def norm_backward(cotangent, normed, inv_std, gain_row):
    scaled = cotangent * gain_row
    return inv_std * (scaled - jnp.mean(scaled, axis=-1, keepdims=True) - normed * jnp.mean(scaled * normed, axis=-1, keepdims=True))


def rope_tables(seq_len, head_dim):
    half_dim = head_dim // 2
    inv_freq = ROPE_BASE ** (-2.0 * jnp.arange(half_dim, dtype=jnp.float32) / head_dim)
    angles = jnp.arange(seq_len, dtype=jnp.float32)[:, None] * inv_freq[None, :]
    angles = jnp.concatenate([angles, angles], axis=-1)
    return jnp.cos(angles), jnp.sin(angles)


def rotate_half(tensor):
    half_dim = tensor.shape[-1] // 2
    return jnp.concatenate([-tensor[..., half_dim:], tensor[..., :half_dim]], axis=-1)


def rotate_half_back(tensor):
    half_dim = tensor.shape[-1] // 2
    return jnp.concatenate([tensor[..., half_dim:], -tensor[..., :half_dim]], axis=-1)


def apply_rope(tensor, cos_tab, sin_tab):
    widened = tensor.astype(jnp.float32)
    return (widened * cos_tab + rotate_half(widened) * sin_tab).astype(jnp.bfloat16)


def rope_backward(cotangent, cos_tab, sin_tab):
    return cotangent * cos_tab + rotate_half_back(cotangent * sin_tab)


def exact_gelu(pre_vals):
    return jax.nn.gelu(pre_vals, approximate=False)


def group_attention(operands):
    queries, key_rot, val_rows, ctx_grad = operands
    seq_len = queries.shape[1]
    score_scale = queries.shape[-1] ** -0.5
    positions = jnp.arange(seq_len)
    causal = positions[:, None] >= positions[None, :]
    scores = jnp.einsum('bqjh,bkh->bjqk', queries.astype(jnp.float32), key_rot.astype(jnp.float32)) * score_scale
    scores = jnp.where(causal, scores, NEG_BIG)
    attn_probs = jax.nn.softmax(scores, axis=-1)
    probs_bf16 = attn_probs.astype(jnp.bfloat16).astype(jnp.float32)
    context = jnp.einsum('bjqk,bkh->bqjh', probs_bf16, val_rows.astype(jnp.float32)).astype(jnp.bfloat16)
    prob_grad = jnp.einsum('bqjh,bkh->bjqk', ctx_grad.astype(jnp.float32), val_rows.astype(jnp.float32))
    val_grad = jnp.einsum('bjqk,bqjh->bkh', probs_bf16, ctx_grad.astype(jnp.float32))
    score_grad = attn_probs * (prob_grad - jnp.sum(prob_grad * attn_probs, axis=-1, keepdims=True))
    score_grad = (score_grad * score_scale).astype(jnp.bfloat16).astype(jnp.float32)
    query_grad = jnp.einsum('bjqk,bkh->bqjh', score_grad, key_rot.astype(jnp.float32))
    key_grad = jnp.einsum('bjqk,bqjh->bkh', score_grad, queries.astype(jnp.float32))
    return context, query_grad, key_grad, val_grad


def reference(layer_in, grad_out, w_qkv, w_out, w_up, w_down, ln_params):
    group_size = HEADS // KV_HEADS
    row_count = BATCH * SEQ
    normed, inv_std = norm_stats(layer_in.reshape(row_count, D))
    attn_in = (normed * ln_params[0] + ln_params[1]).astype(jnp.bfloat16)
    mlp_in = (normed * ln_params[2] + ln_params[3]).astype(jnp.bfloat16)
    qkv_flat = w_qkv.reshape(D, KV_HEADS * (group_size + 2) * HEAD)
    proj_qkv = jnp.dot(attn_in, qkv_flat, preferred_element_type=jnp.float32).astype(jnp.bfloat16)
    proj_qkv = proj_qkv.reshape(BATCH, SEQ, KV_HEADS, group_size + 2, HEAD)
    cos_tab, sin_tab = rope_tables(SEQ, HEAD)
    cos_q = cos_tab[:, None, None, :]
    sin_q = sin_tab[:, None, None, :]
    cos_k = cos_tab[:, None, :]
    sin_k = sin_tab[:, None, :]
    queries = apply_rope(proj_qkv[:, :, :, :group_size], cos_q, sin_q)
    key_rot = apply_rope(proj_qkv[:, :, :, group_size], cos_k, sin_k)
    val_rows = proj_qkv[:, :, :, group_size + 1]
    grad_rows = grad_out.reshape(row_count, D)
    out_flat = w_out.reshape(HEADS * HEAD, D)
    ctx_grad = jnp.dot(grad_rows, out_flat.T, preferred_element_type=jnp.float32).astype(jnp.bfloat16)
    ctx_grad = ctx_grad.reshape(BATCH, SEQ, KV_HEADS, group_size, HEAD)
    by_group = (jnp.moveaxis(queries, 2, 0), jnp.moveaxis(key_rot, 2, 0), jnp.moveaxis(val_rows, 2, 0), jnp.moveaxis(ctx_grad, 2, 0))
    context, query_grad, key_grad, val_grad = lax.map(group_attention, by_group)
    context = jnp.moveaxis(context, 0, 2)
    query_grad = rope_backward(jnp.moveaxis(query_grad, 0, 2), cos_q, sin_q)
    key_grad = rope_backward(jnp.moveaxis(key_grad, 0, 2), cos_k, sin_k)
    val_grad = jnp.moveaxis(val_grad, 0, 2)
    qkv_grad = jnp.concatenate([query_grad, key_grad[:, :, :, None], val_grad[:, :, :, None]], axis=3)
    qkv_grad = qkv_grad.astype(jnp.bfloat16).reshape(row_count, KV_HEADS * (group_size + 2) * HEAD)
    attn_cot = jnp.dot(qkv_grad, qkv_flat.T, preferred_element_type=jnp.float32)
    grad_qkv = jnp.dot(attn_in.T, qkv_grad, preferred_element_type=jnp.float32).astype(jnp.bfloat16).reshape(w_qkv.shape)
    grad_wout = jnp.dot(context.reshape(row_count, HEADS * HEAD).T, grad_rows, preferred_element_type=jnp.float32).astype(jnp.bfloat16).reshape(w_out.shape)
    pre_act = jnp.dot(mlp_in, w_up, preferred_element_type=jnp.float32)
    act_vals, gelu_vjp = jax.vjp(exact_gelu, pre_act)
    act_grad = jnp.dot(grad_rows, w_down.T, preferred_element_type=jnp.float32)
    hidden_grad = gelu_vjp(act_grad)[0].astype(jnp.bfloat16)
    grad_down = jnp.dot(act_vals.astype(jnp.bfloat16).T, grad_rows, preferred_element_type=jnp.float32).astype(jnp.bfloat16)
    grad_up = jnp.dot(mlp_in.T, hidden_grad, preferred_element_type=jnp.float32).astype(jnp.bfloat16)
    mlp_cot = jnp.dot(hidden_grad, w_up.T, preferred_element_type=jnp.float32)
    grad_in = grad_rows.astype(jnp.float32) + norm_backward(attn_cot, normed, inv_std, ln_params[0]) + norm_backward(mlp_cot, normed, inv_std, ln_params[2])
    grad_ln = jnp.stack([jnp.sum(attn_cot * normed, axis=0), jnp.sum(attn_cot, axis=0), jnp.sum(mlp_cot * normed, axis=0), jnp.sum(mlp_cot, axis=0)])
    return (grad_in.astype(jnp.bfloat16).reshape(BATCH, SEQ, D), grad_qkv, grad_wout, grad_up, grad_down, grad_ln)
```

```python
import functools

import jax
import jax.numpy as jnp
from jax import lax
from jax.experimental import pallas as pl
from jax.experimental.pallas import tpu as pltpu
from jax.sharding import PartitionSpec as P

NORM_EPS = 1e-5
ROPE_BASE = 10000.0
NEG_BIG = -1e30
LOG2E = 1.4426950408889634
SQRT_HALF = 0.7071067811865476
INV_SQRT_2PI = 0.3989422804014327
F32 = jnp.float32
BF16 = jnp.bfloat16
MESH_ID = pl.DeviceIdType.MESH
BLK = 256
LN_ROWS = 32
GATHER_ORDER = (0, 1, 3, 2)
SCATTER_ORDER = (2, 1, 3, 0)


def pick(index, values):
    out = values[-1]
    for i in range(len(values) - 2, -1, -1):
        out = jnp.where(index == i, values[i], out)
    return out


def dot_nn(lhs, rhs):
    return lax.dot_general(lhs, rhs, (((1,), (0,)), ((), ())), preferred_element_type=F32)


def dot_nt(lhs, rhs):
    return lax.dot_general(lhs, rhs, (((1,), (1,)), ((), ())), preferred_element_type=F32)


def dot_tn(lhs, rhs):
    return lax.dot_general(lhs, rhs, (((0,), (0,)), ((), ())), preferred_element_type=F32)


def fold8(value):
    rows, cols = value.shape
    return jnp.sum(value.reshape(rows // 8, 8, cols), axis=0)


def layer_kernel(nt, x_in, dy_in, wq_in, wo_in, wu_in, wd_in, ln_ref, cos_in, sin_in,
                 gi_out, gq_out, go_out, gu_out, gd_out, gl_out,
                 x_ref, dy_ref, a_ref, m_ref, wq_ref, wo_ref, wu_ref, wd_ref, cos_ref, sin_ref,
                 q_ref, k_ref, v_ref, dc_ref, kt_ref, vt_ref, u_ref, dh_ref, t_ref, p_ref,
                 hp_ref, hm_ref, fp_ref, fm_ref, mu_ref, rstd_ref, s_ref, dp_ref, pt_ref, ds_ref,
                 qm_ref, dcm_ref, dka_ref, dva_ref, dqt_ref, dqkv_ref, ct_ref, acc_ref, gl_ref, gls_ref,
                 gi_ref, gq_ref, go_ref, gu_ref, gd_ref,
                 load_sem, store_sem, ag_send, ag_recv, rs_send, rs_recv, gl_send, gl_recv):
    nc = nt // 2
    batch, seq, width = x_ref.shape
    ff = wu_ref.shape[1]
    rows = x_in.shape[1]
    half = rows // 2
    pair = 2 * rows
    hd = wo_in.shape[0] // 2
    hh = hd // 2
    scale = hd ** -0.5

    me = lax.axis_index("tp")
    chip = me // 2
    core = lax.rem(me, 2)
    partner = chip * 2 + (1 - core)

    def dev(off, which):
        return lax.rem(chip + off, nc) * 2 + which

    plus = dev(1, core)
    minus = dev(nc - 1, core)

    def row0(device):
        return pl.multiple_of(device * rows, rows)

    loads = []

    def load(src, dst):
        loads.append(pltpu.make_async_copy(src, dst, load_sem.at[len(loads)]))
        loads[-1].start()

    barrier = pltpu.get_barrier_semaphore()
    for j in range(1, nt):
        pl.semaphore_signal(barrier, inc=1, device_id={"tp": lax.rem(me + j, nt)}, device_id_type=MESH_ID)

    load(x_in, x_ref.at[:, pl.ds(row0(me), rows), :])
    load(dy_in, dy_ref.at[:, pl.ds(row0(me), rows), :])
    for t, base in ((0, 0), (1, 2 * hd)):
        for part in range(2):
            for g in range(2):
                load(wq_in.at[pl.ds(g * 3 * hd + t * hd + part * hh, hh), :],
                     wq_ref.at[pl.ds(base + part * hd + g * hh, hh), :])
    for g in range(2):
        load(wq_in.at[pl.ds(g * 3 * hd + 2 * hd, hd), :], wq_ref.at[pl.ds(4 * hd + g * hd, hd), :])
    load(cos_in, cos_ref)
    load(sin_in, sin_ref)
    load(wo_in, wo_ref)
    load(wu_in, wu_ref)
    load(wd_in, wd_ref)

    pl.semaphore_wait(barrier, nt - 1)

    def ag(kind, src, dst, b, target):
        return pltpu.make_async_remote_copy(
            src_ref=src, dst_ref=dst, send_sem=ag_send.at[b, kind], recv_sem=ag_recv.at[b, kind],
            device_id={"tp": target}, device_id_type=MESH_ID)

    def rows_of(ref, b, device):
        return ref.at[b, pl.ds(row0(device), rows), :]

    def own(kind, b):
        ref, src = ((x_ref, x_in), (dy_ref, dy_in))[kind % 2]
        target = (plus, minus, partner)[kind // 2]
        return ag(kind, src.at[b], rows_of(ref, b, me), b, target)

    def forward(kind, b):
        if kind == 6:
            return ag(kind, rows_of(x_ref, b, minus), rows_of(x_ref, b, minus), b, plus)
        if kind == 7:
            return ag(kind, rows_of(dy_ref, b, plus), rows_of(dy_ref, b, plus), b, minus)
        ref = (x_ref, dy_ref)[kind % 2]
        source = dev((nc - 1, 1, 2)[(kind - 8) // 2], core)
        return ag(kind, rows_of(ref, b, source), rows_of(ref, b, source), b, partner)

    def arrived(kind, b):
        ref = (x_ref, dy_ref)[kind % 2]
        if kind < 6:
            source = (minus, plus, partner)[kind // 2]
        elif kind < 8:
            source = dev(2, core)
        else:
            source = dev((nc - 1, 1, 2)[(kind - 8) // 2], 1 - core)
        ag(kind, rows_of(ref, b, source), rows_of(ref, b, source), b, partner).wait_recv()

    def send_own(b):
        for kind in (0, 2, 4, 1, 3, 5):
            own(kind, b).start()

    def service_x(b):
        arrived(0, b)
        forward(6, b).start()
        forward(8, b).start()
        arrived(2, b)
        forward(10, b).start()

    def service_dy(b):
        arrived(3, b)
        forward(7, b).start()
        forward(11, b).start()
        arrived(1, b)
        forward(9, b).start()

    def service_far(b):
        arrived(6, b)
        forward(12, b).start()
        arrived(7, b)
        forward(13, b).start()
        arrived(12, b)
        arrived(13, b)

    def rs(kind, src, dst, b, target):
        return pltpu.make_async_remote_copy(
            src_ref=src, dst_ref=dst, send_sem=rs_send.at[b, kind], recv_sem=rs_recv.at[b, kind],
            device_id={"tp": target}, device_id_type=MESH_ID)

    def part_rows(b, device, part):
        if part is None:
            return t_ref.at[b, pl.ds(row0(device), rows), :]
        return t_ref.at[b, pl.ds(pl.multiple_of(device * rows + part * half, half), half), :]

    def to_partner(b, j, off):
        return rs(j, part_rows(b, dev(off, 1 - core), None), p_ref.at[b, j], b, partner)

    def ring(kind, b):
        lo, hi = pl.ds(0, half), pl.ds(half, half)
        if kind == 4:
            return rs(kind, part_rows(b, dev(2, core), 0), hp_ref.at[b], b, plus)
        if kind == 5:
            return rs(kind, part_rows(b, dev(2, core), 1), hm_ref.at[b], b, minus)
        if kind == 6:
            return rs(kind, part_rows(b, plus, 1), fp_ref.at[b, hi, :], b, plus)
        if kind == 7:
            return rs(kind, part_rows(b, plus, 0), fp_ref.at[b, lo, :], b, plus)
        if kind == 8:
            return rs(kind, part_rows(b, minus, 0), fm_ref.at[b, lo, :], b, minus)
        return rs(kind, part_rows(b, minus, 1), fm_ref.at[b, hi, :], b, minus)

    def add_partner(b, j):
        off = pick(j, SCATTER_ORDER)
        target = dev(off, core)
        rs(j, part_rows(b, target, None), p_ref.at[b, j], b, partner).wait_recv()

        @pl.loop(0, rows, step=LN_ROWS)
        def _(i):
            at = pl.ds(pl.multiple_of(target * rows + i, LN_ROWS), LN_ROWS)
            t_ref[b, at, :] += p_ref[b, j, pl.ds(pl.multiple_of(i, LN_ROWS), LN_ROWS), :]

    def ring_after_partner(b, j):
        @pl.when(j == 0)
        def _():
            ring(4, b).start()
            ring(5, b).start()

        @pl.when(j == 1)
        def _():
            ring(6, b).start()

        @pl.when(j == 2)
        def _():
            ring(8, b).start()

    def add_half(b, device, part, ref):
        @pl.loop(0, half, step=LN_ROWS)
        def _(i):
            at = pl.ds(pl.multiple_of(device * rows + part * half + i, LN_ROWS), LN_ROWS)
            t_ref[b, at, :] += ref[b, pl.ds(pl.multiple_of(i, LN_ROWS), LN_ROWS), :]

    def ring_second(b):
        ring(4, b).wait_recv()
        add_half(b, plus, 0, hp_ref)
        ring(7, b).start()
        ring(5, b).wait_recv()
        add_half(b, minus, 1, hm_ref)
        ring(9, b).start()

    def unit(b, cc):
        r0 = pl.multiple_of(cc * pair, pair)
        at = pl.ds(r0, pair)

        @pl.loop(0, pair, step=LN_ROWS)
        def _(i):
            sub = pl.ds(pl.multiple_of(r0 + i, LN_ROWS), LN_ROWS)
            xs = x_ref[b, sub, :].astype(F32)
            mu = jnp.mean(xs, axis=-1, keepdims=True)
            xc = xs - mu
            rstd = lax.rsqrt(jnp.mean(xc * xc, axis=-1, keepdims=True) + NORM_EPS)
            xh = xc * rstd
            mu_ref[b, sub, :] = mu
            rstd_ref[b, sub, :] = rstd
            a_ref[b, sub, :] = (xh * ln_ref[0:1, :] + ln_ref[1:2, :]).astype(BF16)
            m_ref[b, sub, :] = (xh * ln_ref[2:3, :] + ln_ref[3:4, :]).astype(BF16)

        a = a_ref[b, at, :]
        dy = dy_ref[b, at, :]
        cos = cos_ref[at, :]
        sin = sin_ref[at, :]
        q = dot_nt(a, wq_ref[0:2 * hd, :]).astype(BF16).astype(F32)
        q_ref[b, at, :] = (q * cos + pltpu.roll(q, hd, 1) * sin).astype(BF16)
        k = dot_nt(a, wq_ref[2 * hd:4 * hd, :]).astype(BF16).astype(F32)
        k2 = k * cos + pltpu.roll(k, hd, 1) * sin
        k_ref[b, at, :] = k2.astype(BF16)
        kt_ref[b, :, at] = k2.T.astype(BF16)
        v = dot_nt(a, wq_ref[4 * hd:6 * hd, :])
        v_ref[b, at, :] = v.astype(BF16)
        vt_ref[b, :, at] = v.T.astype(BF16)
        dc_ref[b, at, :] = dot_nt(dy, wo_ref[...]).astype(BF16)
        m = m_ref[b, at, :]
        for f in range(0, ff, BLK):
            h = dot_nn(m, wu_ref[:, f:f + BLK])
            du = dot_nt(dy, wd_ref[f:f + BLK, :])
            cdf = 0.5 * (1.0 + lax.erf(h * SQRT_HALF))
            pdf = jnp.exp2(h * h * (-0.5 * LOG2E)) * INV_SQRT_2PI
            u_ref[b, at, f:f + BLK] = (h * cdf).astype(BF16)
            dh_ref[b, at, f:f + BLK] = (du * (cdf + h * pdf)).astype(BF16)
        dh = dh_ref[b, at, :]
        mu = mu_ref[b, at, :]
        rstd = rstd_ref[b, at, :]
        for d in range(0, width, BLK):
            cols = slice(d, d + BLK)
            dm = dot_nt(dh, wu_ref[cols, :])
            xh = (x_ref[b, at, cols].astype(F32) - mu) * rstd
            t_ref[b, at, cols] = dm * ln_ref[2:3, cols]
            acc_ref[2, :, cols] += fold8(dm * xh)
            acc_ref[3, :, cols] += fold8(dm)

    def attention_head(b, h):
        lane = lax.broadcasted_iota(jnp.int32, (1, 2 * hd), 1)
        q_mask = lax.rem(lane // hh, 2) == h
        v_mask = (lane // hd) == h
        qm_ref[...] = jnp.where(q_mask, q_ref[b], jnp.zeros((), BF16))
        dcm_ref[...] = jnp.where(v_mask, dc_ref[b], jnp.zeros((), BF16))
        v_rows = pl.ds(pl.multiple_of(h * hd, hd), hd)
        k_lo = pl.ds(pl.multiple_of(h * hh, hh), hh)
        k_hi = pl.ds(pl.multiple_of(hd + h * hh, hh), hh)
        for qb in range(seq // BLK):
            qs = slice(qb * BLK, (qb + 1) * BLK)
            kl = (qb + 1) * BLK
            qm = qm_ref[qs, :]
            dcm = dcm_ref[qs, :]
            top = None
            for kb in range(qb + 1):
                ks = slice(kb * BLK, (kb + 1) * BLK)
                s = dot_nt(k_ref[b, ks, :], qm)
                if kb == qb:
                    key = lax.broadcasted_iota(jnp.int32, (BLK, BLK), 0)
                    query = lax.broadcasted_iota(jnp.int32, (BLK, BLK), 1)
                    s = jnp.where(key <= query, s, NEG_BIG)
                s_ref[ks, :] = s
                best = jnp.max(s.reshape(BLK // 8, 8, BLK), axis=0)
                top = best if top is None else jnp.maximum(top, best)
            top = jnp.max(top, axis=0, keepdims=True)
            total = jnp.zeros((8, BLK), F32)
            weighted = jnp.zeros((8, BLK), F32)
            for kb in range(qb + 1):
                ks = slice(kb * BLK, (kb + 1) * BLK)
                e = jnp.exp2((s_ref[ks, :] - top) * (scale * LOG2E))
                dpr = dot_nt(v_ref[b, ks, :], dcm)
                s_ref[ks, :] = e
                dp_ref[ks, :] = dpr
                total += fold8(e)
                weighted += fold8(e * dpr)
            inv = 1.0 / jnp.sum(total, axis=0, keepdims=True)
            mean_dp = jnp.sum(weighted, axis=0, keepdims=True) * inv
            for kb in range(qb + 1):
                ks = slice(kb * BLK, (kb + 1) * BLK)
                p = s_ref[ks, :] * inv
                pt_ref[ks, qs] = p.astype(BF16)
                ds_ref[ks, qs] = (p * (dp_ref[ks, :] - mean_dp) * scale).astype(BF16)
            c = dot_nn(vt_ref[b, v_rows, 0:kl], pt_ref[0:kl, qs])
            ct_ref[b, v_rows, qs] = c.astype(BF16)
            kt = jnp.concatenate([kt_ref[b, k_lo, 0:kl], kt_ref[b, k_hi, 0:kl]], axis=0)
            dq = dot_nn(kt, ds_ref[0:kl, qs])
            dqt_ref[k_lo, qs] = dq[0:hh]
            dqt_ref[k_hi, qs] = dq[hh:hd]
        for kb in range(seq // BLK):
            ks = slice(kb * BLK, (kb + 1) * BLK)
            dva_ref[ks, :] += dot_nn(pt_ref[ks, kb * BLK:], dcm_ref[kb * BLK:, :])
            dka_ref[ks, :] += dot_nn(ds_ref[ks, kb * BLK:], qm_ref[kb * BLK:, :])

    def attention_finish(b):
        @pl.loop(0, seq, step=BLK)
        def _(i):
            at = pl.ds(pl.multiple_of(i, BLK), BLK)
            cos = cos_ref[at, :]
            sin = sin_ref[at, :]
            dq = dqt_ref[:, at].T
            dqkv_ref[b, at, 0:2 * hd] = (dq * cos - pltpu.roll(dq, hd, 1) * sin).astype(BF16)
            dk = dka_ref[at, :]
            dqkv_ref[b, at, 2 * hd:4 * hd] = (dk * cos - pltpu.roll(dk, hd, 1) * sin).astype(BF16)
            dqkv_ref[b, at, 4 * hd:6 * hd] = dva_ref[at, :].astype(BF16)

    def input_grad(b, cc):
        at = pl.ds(pl.multiple_of(cc * pair, pair), pair)
        dqkv = dqkv_ref[b, at, :]
        mu = mu_ref[b, at, :]
        rstd = rstd_ref[b, at, :]
        for d in range(0, width, BLK):
            cols = slice(d, d + BLK)
            da = dot_nn(dqkv, wq_ref[:, cols])
            xh = (x_ref[b, at, cols].astype(F32) - mu) * rstd
            t_ref[b, at, cols] += da * ln_ref[0:1, cols]
            acc_ref[0, :, cols] += fold8(da * xh)
            acc_ref[1, :, cols] += fold8(da)

    def finish(b):
        for kind, ref in ((6, fp_ref), (7, fp_ref), (8, fm_ref), (9, fm_ref)):
            ring(kind, b).wait_recv()

        @pl.loop(0, rows, step=LN_ROWS)
        def _(i):
            at = pl.ds(pl.multiple_of(me * rows + i, LN_ROWS), LN_ROWS)
            sub = pl.ds(pl.multiple_of(i, LN_ROWS), LN_ROWS)
            t = t_ref[b, at, :] + fp_ref[b, sub, :] + fm_ref[b, sub, :]
            rstd = rstd_ref[b, at, :]
            xh = (x_ref[b, at, :].astype(F32) - mu_ref[b, at, :]) * rstd
            n = rstd * (t - jnp.mean(t, axis=-1, keepdims=True) - xh * jnp.mean(t * xh, axis=-1, keepdims=True))
            gi_ref[b, sub, :] = (dy_ref[b, at, :].astype(F32) + n).astype(BF16)

        pltpu.make_async_copy(gi_ref.at[b], gi_out.at[b], store_sem.at[b]).start()

    send_own(0)
    acc_ref[...] = jnp.zeros_like(acc_ref)
    for copy in loads:
        copy.wait()

    @pl.loop(0, batch)
    def _(b):
        @pl.loop(0, nc)
        def _(i):
            @pl.when(i == 0)
            def _():
                arrived(4, b)
                arrived(5, b)

            @pl.when((i == 1) & (b == 0))
            def _():
                service_x(b)
                send_own(1)
                service_dy(b)

            @pl.when(i == 1)
            def _():
                arrived(10, b)
                arrived(11, b)

            @pl.when(i == 2)
            def _():
                arrived(8, b)
                arrived(9, b)

            @pl.when((i == 2) & (b == 1))
            def _():
                ring_second(0)

            @pl.when(i == 3)
            def _():
                service_far(b)

            unit(b, lax.rem(chip + pick(i, GATHER_ORDER), nc))

        dka_ref[...] = jnp.zeros_like(dka_ref)
        dva_ref[...] = jnp.zeros_like(dva_ref)

        @pl.loop(0, 2)
        def _(h):
            attention_head(b, h)

            @pl.when((b == 0) & (h == 0))
            def _():
                service_x(1)

        @pl.when(b == 0)
        def _():
            service_dy(1)

        attention_finish(b)

        @pl.loop(0, nc + 1)
        def _(j):
            @pl.when(j < nc)
            def _():
                input_grad(b, lax.rem(chip + pick(j, SCATTER_ORDER + (0,)), nc))

            for jj in range(nc):
                @pl.when(j == jj)
                def _(jj=jj):
                    to_partner(b, jj, SCATTER_ORDER[jj]).start()

            @pl.when(j > 0)
            def _():
                add_partner(b, j - 1)
                ring_after_partner(b, j - 1)

    for r in range(4):
        gls_ref[r:r + 1, :] = jnp.sum(acc_ref[r], axis=0, keepdims=True)
    gl_ref[me] = gls_ref[...]

    def gl_copy(j, source):
        return pltpu.make_async_remote_copy(
            src_ref=gls_ref, dst_ref=gl_ref.at[source], send_sem=gl_send.at[j], recv_sem=gl_recv.at[j],
            device_id={"tp": lax.rem(me + j, nt)}, device_id_type=MESH_ID)

    for j in range(1, nt):
        gl_copy(j, me).start()

    @pl.loop(0, width, step=BLK)
    def _(i):
        cols = pl.ds(pl.multiple_of(i, BLK), BLK)
        total = dot_tn(m_ref[0, :, cols], dh_ref[0])
        for b in range(1, batch):
            total += dot_tn(m_ref[b, :, cols], dh_ref[b])
        gu_ref[cols, :] = total.astype(BF16)

    ring_second(1)
    stores = [pltpu.make_async_copy(gu_ref, gu_out, store_sem.at[batch])]
    stores[-1].start()

    @pl.loop(0, width, step=BLK)
    def _(i):
        cols = pl.ds(pl.multiple_of(i, BLK), BLK)
        total = dot_tn(u_ref[0], dy_ref[0, :, cols])
        for b in range(1, batch):
            total += dot_tn(u_ref[b], dy_ref[b, :, cols])
        gd_ref[:, cols] = total.astype(BF16)

    stores.append(pltpu.make_async_copy(gd_ref, gd_out, store_sem.at[batch + 1]))
    stores[-1].start()

    @pl.loop(0, width, step=BLK)
    def _(i):
        cols = pl.ds(pl.multiple_of(i, BLK), BLK)
        total = dot_tn(dqkv_ref[0], a_ref[0, :, cols])
        out = dot_nn(ct_ref[0], dy_ref[0, :, cols])
        for b in range(1, batch):
            total += dot_tn(dqkv_ref[b], a_ref[b, :, cols])
            out += dot_nn(ct_ref[b], dy_ref[b, :, cols])
        gq_ref[:, cols] = total.astype(BF16)
        go_ref[:, cols] = out.astype(BF16)

    def store(src, dst):
        stores.append(pltpu.make_async_copy(src, dst, store_sem.at[batch + len(stores)]))
        stores[-1].start()

    store(go_ref, go_out)
    for t, base in ((0, 0), (1, 2 * hd)):
        for part in range(2):
            for g in range(2):
                store(gq_ref.at[pl.ds(base + part * hd + g * hh, hh), :],
                      gq_out.at[pl.ds(g * 3 * hd + t * hd + part * hh, hh), :])
    for g in range(2):
        store(gq_ref.at[pl.ds(4 * hd + g * hd, hd), :], gq_out.at[pl.ds(g * 3 * hd + 2 * hd, hd), :])

    for j in range(1, nt):
        gl_copy(j, lax.rem(me + nt - j, nt)).wait_recv()
    total = gl_ref[0]
    for j in range(1, nt):
        total += gl_ref[j]
    gl_out[...] = total

    finish(0)
    finish(1)

    for b in range(batch):
        pltpu.make_async_copy(gi_ref.at[b], gi_out.at[b], store_sem.at[b]).wait()
        for kind in range(6):
            own(kind, b).wait_send()
        for kind in range(6, 14):
            forward(kind, b).wait_send()
        for j in range(nc):
            to_partner(b, j, SCATTER_ORDER[j]).wait_send()
        for kind in range(4, 10):
            ring(kind, b).wait_send()
    for j in range(1, nt):
        gl_copy(j, me).wait_send()
    for copy in stores:
        copy.wait()


def rope_tables(seq_len, head_dim):
    half_dim = head_dim // 2
    inv_freq = ROPE_BASE ** (-2.0 * jnp.arange(half_dim, dtype=F32) / head_dim)
    angles = jnp.arange(seq_len, dtype=F32)[:, None] * inv_freq[None, :]
    cos, sin = jnp.cos(angles), jnp.sin(angles)
    return jnp.concatenate([cos] * 4, axis=1), jnp.concatenate([-sin, -sin, sin, sin], axis=1)


def solution(mesh):
    act_spec = P('dp', 'tp', None)
    nt = mesh.shape['tp']
    nc = nt // 2

    def device_step(layer_in, grad_out, w_qkv, w_out, w_up, w_down, ln_params):
        batch, rows, width = layer_in.shape
        seq = rows * nt
        groups, _, hd = w_qkv.shape[1:]
        ff = w_up.shape[1]
        wq = jnp.transpose(w_qkv, (1, 2, 3, 0)).reshape(groups * 3 * hd, width)
        wo = w_out.reshape(groups * hd, width)
        cos, sin = rope_tables(seq, hd)
        lanes = groups * hd
        any_spec = pl.BlockSpec(memory_space=pl.ANY)
        vmem_spec = pl.BlockSpec(memory_space=pltpu.VMEM)
        vm = pltpu.VMEM
        dma = pltpu.SemaphoreType.DMA
        outs = pl.pallas_call(
            functools.partial(layer_kernel, nt),
            out_shape=(
                jax.ShapeDtypeStruct((batch, rows, width), BF16),
                jax.ShapeDtypeStruct((groups * 3 * hd, width), BF16),
                jax.ShapeDtypeStruct((lanes, width), BF16),
                jax.ShapeDtypeStruct((width, ff), BF16),
                jax.ShapeDtypeStruct((ff, width), BF16),
                jax.ShapeDtypeStruct((4, width), F32),
            ),
            in_specs=[any_spec] * 6 + [vmem_spec] + [any_spec] * 2,
            out_specs=(any_spec,) * 5 + (vmem_spec,),
            scratch_shapes=[
                vm((batch, seq, width), BF16), vm((batch, seq, width), BF16),
                vm((batch, seq, width), BF16), vm((batch, seq, width), BF16),
                vm((groups * 3 * hd, width), BF16), vm((lanes, width), BF16), vm((width, ff), BF16), vm((ff, width), BF16),
                vm((seq, lanes), F32), vm((seq, lanes), F32),
                vm((batch, seq, lanes), BF16), vm((batch, seq, lanes), BF16), vm((batch, seq, lanes), BF16), vm((batch, seq, lanes), BF16),
                vm((batch, lanes, seq), BF16), vm((batch, lanes, seq), BF16),
                vm((batch, seq, ff), BF16), vm((batch, seq, ff), BF16),
                vm((batch, seq, width), F32), vm((batch, nc, rows, width), F32),
                vm((batch, rows // 2, width), F32), vm((batch, rows // 2, width), F32),
                vm((batch, rows, width), F32), vm((batch, rows, width), F32),
                vm((batch, seq, 1), F32), vm((batch, seq, 1), F32),
                vm((seq, BLK), F32), vm((seq, BLK), F32), vm((seq, seq), BF16), vm((seq, seq), BF16),
                vm((seq, lanes), BF16), vm((seq, lanes), BF16), vm((seq, lanes), F32), vm((seq, lanes), F32),
                vm((lanes, seq), F32), vm((batch, seq, 3 * lanes), BF16), vm((batch, lanes, seq), BF16),
                vm((4, 8, width), F32), vm((nt, 4, width), F32), vm((4, width), F32),
                vm((batch, rows, width), BF16), vm((3 * lanes, width), BF16), vm((lanes, width), BF16), vm((width, ff), BF16), vm((ff, width), BF16),
                dma((17,)), dma((batch + 13,)), dma((batch, 14)), dma((batch, 14)), dma((batch, 10)), dma((batch, 10)), dma((nt,)), dma((nt,)),
            ],
            compiler_params=pltpu.CompilerParams(collective_id=0, has_side_effects=True, vmem_limit_bytes=66000000),
            name="layer_backward",
        )(layer_in, grad_out, wq, wo, w_up, w_down, ln_params, cos, sin)
        grad_in, gq, go, gu, gd, gl = outs
        gq = jnp.transpose(gq.reshape(groups, 3, hd, width), (3, 0, 1, 2))
        return grad_in, gq, go.reshape(w_out.shape), gu, gd, gl

    return jax.shard_map(
        device_step,
        mesh=mesh,
        in_specs=(act_spec, act_spec, P(None, 'tp', None, None), P('tp', None, None, None), P(None, 'tp'), P('tp', None), P(None, None)),
        out_specs=(act_spec, P('dp', 'tp', None, None), P(('dp', 'tp'), None, None, None), P('dp', 'tp'), P(('dp', 'tp'), None), P('dp', None)),
        check_vma=False,
    )
```

```python
import functools

import jax
import jax.numpy as jnp
import numpy as np
from jax import lax
from jax.experimental import pallas as pl
from jax.experimental.pallas import tpu as pltpu
from jax.sharding import PartitionSpec as P

NORM_EPS = 1e-5
ROPE_BASE = 10000.0
NEG_BIG = -1e30
LOG2E = 1.4426950408889634
SQRT_HALF = 0.7071067811865476
INV_SQRT_2PI = 0.3989422804014327
F32 = jnp.float32
BF16 = jnp.bfloat16
MESH_ID = pl.DeviceIdType.MESH
BLK = 256
LN_ROWS = 32
GATHER_ORDER = (0, 1, 3, 2)
SCATTER_ORDER = (2, 1, 3, 0)


def pick(index, values):
    out = values[-1]
    for i in range(len(values) - 2, -1, -1):
        out = jnp.where(index == i, values[i], out)
    return out


def dot_nn(lhs, rhs):
    return lax.dot_general(lhs, rhs, (((1,), (0,)), ((), ())), preferred_element_type=F32)


def dot_nt(lhs, rhs):
    return lax.dot_general(lhs, rhs, (((1,), (1,)), ((), ())), preferred_element_type=F32)


def dot_tn(lhs, rhs):
    return lax.dot_general(lhs, rhs, (((0,), (0,)), ((), ())), preferred_element_type=F32)


def fold8(value):
    rows, cols = value.shape
    return jnp.sum(value.reshape(rows // 8, 8, cols), axis=0)


def layer_kernel(nt, x_in, dy_in, wq_in, wo_in, wu_in, wd_in, ln_ref, cos_in, sin_in,
                 gi_out, gq_out, go_out, gu_out, gd_out, gl_out,
                 x_ref, dy_ref, a_ref, m_ref, wq_ref, wo_ref, wu_ref, wd_ref, cos_ref, sin_ref,
                 q_ref, k_ref, v_ref, dc_ref, kt_ref, vt_ref, u_ref, dh_ref, t_ref, p_ref,
                 hp_ref, hm_ref, fp_ref, fm_ref, mu_ref, rstd_ref, s_ref, dp_ref, pt_ref, ds_ref,
                 qm_ref, dcm_ref, dka_ref, dva_ref, dqt_ref, dqkv_ref, ct_ref, acc_ref, gl_ref, gls_ref,
                 gi_ref, gq_ref, go_ref, gu_ref, gd_ref,
                 load_sem, store_sem, ag_send, ag_recv, rs_send, rs_recv, gl_send, gl_recv):
    nc = nt // 2
    batch, seq, width = x_ref.shape
    ff = wu_ref.shape[1]
    rows = x_in.shape[1]
    half = rows // 2
    pair = 2 * rows
    hd = wo_in.shape[0] // 2
    hh = hd // 2
    scale = hd ** -0.5

    me = lax.axis_index("tp")
    chip = me // 2
    core = lax.rem(me, 2)
    partner = chip * 2 + (1 - core)

    def dev(off, which):
        return lax.rem(chip + off, nc) * 2 + which

    plus = dev(1, core)
    minus = dev(nc - 1, core)

    def row0(device):
        return pl.multiple_of(device * rows, rows)

    loads = []

    def load(src, dst):
        loads.append(pltpu.make_async_copy(src, dst, load_sem.at[len(loads)]))
        loads[-1].start()

    barrier = pltpu.get_barrier_semaphore()
    for j in range(1, nt):
        pl.semaphore_signal(barrier, inc=1, device_id={"tp": lax.rem(me + j, nt)}, device_id_type=MESH_ID)

    load(x_in, x_ref.at[:, pl.ds(row0(me), rows), :])
    load(dy_in, dy_ref.at[:, pl.ds(row0(me), rows), :])
    for t, base in ((0, 0), (1, 2 * hd)):
        for part in range(2):
            for g in range(2):
                load(wq_in.at[pl.ds(g * 3 * hd + t * hd + part * hh, hh), :],
                     wq_ref.at[pl.ds(base + part * hd + g * hh, hh), :])
    for g in range(2):
        load(wq_in.at[pl.ds(g * 3 * hd + 2 * hd, hd), :], wq_ref.at[pl.ds(4 * hd + g * hd, hd), :])
    load(cos_in, cos_ref)
    load(sin_in, sin_ref)
    load(wo_in, wo_ref)
    load(wu_in, wu_ref)
    load(wd_in, wd_ref)

    pl.semaphore_wait(barrier, nt - 1)

    def ag(kind, src, dst, b, target):
        return pltpu.make_async_remote_copy(
            src_ref=src, dst_ref=dst, send_sem=ag_send.at[b, kind], recv_sem=ag_recv.at[b, kind],
            device_id={"tp": target}, device_id_type=MESH_ID)

    def rows_of(ref, b, device):
        return ref.at[b, pl.ds(row0(device), rows), :]

    def own(kind, b):
        ref, src = ((x_ref, x_in), (dy_ref, dy_in))[kind % 2]
        target = (plus, minus, partner)[kind // 2]
        return ag(kind, src.at[b], rows_of(ref, b, me), b, target)

    def forward(kind, b):
        if kind == 6:
            return ag(kind, rows_of(x_ref, b, minus), rows_of(x_ref, b, minus), b, plus)
        if kind == 7:
            return ag(kind, rows_of(dy_ref, b, plus), rows_of(dy_ref, b, plus), b, minus)
        ref = (x_ref, dy_ref)[kind % 2]
        source = dev((nc - 1, 1, 2)[(kind - 8) // 2], core)
        return ag(kind, rows_of(ref, b, source), rows_of(ref, b, source), b, partner)

    def arrived(kind, b):
        ref = (x_ref, dy_ref)[kind % 2]
        if kind < 6:
            source = (minus, plus, partner)[kind // 2]
        elif kind < 8:
            source = dev(2, core)
        else:
            source = dev((nc - 1, 1, 2)[(kind - 8) // 2], 1 - core)
        ag(kind, rows_of(ref, b, source), rows_of(ref, b, source), b, partner).wait_recv()

    def send_ring(b):
        for kind in (0, 3, 1, 2):
            own(kind, b).start()

    def send_partner(b):
        for kind in (4, 5):
            own(kind, b).start()

    def service_first(b):
        arrived(0, b)
        forward(6, b).start()
        forward(8, b).start()
        arrived(3, b)
        forward(7, b).start()
        forward(11, b).start()

    def service_second(b):
        arrived(2, b)
        forward(10, b).start()
        arrived(1, b)
        forward(9, b).start()

    def service_far(b):
        arrived(6, b)
        forward(12, b).start()
        arrived(7, b)
        forward(13, b).start()
        arrived(12, b)
        arrived(13, b)

    def rs(kind, src, dst, b, target):
        return pltpu.make_async_remote_copy(
            src_ref=src, dst_ref=dst, send_sem=rs_send.at[b, kind], recv_sem=rs_recv.at[b, kind],
            device_id={"tp": target}, device_id_type=MESH_ID)

    def part_rows(b, device, part):
        if part is None:
            return t_ref.at[b, pl.ds(row0(device), rows), :]
        return t_ref.at[b, pl.ds(pl.multiple_of(device * rows + part * half, half), half), :]

    def to_partner(b, j, off):
        return rs(j, part_rows(b, dev(off, 1 - core), None), p_ref.at[b, j], b, partner)

    def ring(kind, b):
        lo, hi = pl.ds(0, half), pl.ds(half, half)
        if kind == 4:
            return rs(kind, part_rows(b, dev(2, core), 0), hp_ref.at[b], b, plus)
        if kind == 5:
            return rs(kind, part_rows(b, dev(2, core), 1), hm_ref.at[b], b, minus)
        if kind == 6:
            return rs(kind, part_rows(b, plus, 1), fp_ref.at[b, hi, :], b, plus)
        if kind == 7:
            return rs(kind, part_rows(b, plus, 0), fp_ref.at[b, lo, :], b, plus)
        if kind == 8:
            return rs(kind, part_rows(b, minus, 0), fm_ref.at[b, lo, :], b, minus)
        return rs(kind, part_rows(b, minus, 1), fm_ref.at[b, hi, :], b, minus)

    def add_partner(b, j):
        off = pick(j, SCATTER_ORDER)
        target = dev(off, core)
        rs(j, part_rows(b, target, None), p_ref.at[b, j], b, partner).wait_recv()

        @pl.loop(0, rows, step=LN_ROWS)
        def _(i):
            at = pl.ds(pl.multiple_of(target * rows + i, LN_ROWS), LN_ROWS)
            t_ref[b, at, :] += p_ref[b, j, pl.ds(pl.multiple_of(i, LN_ROWS), LN_ROWS), :]

    def ring_after_partner(b, j):
        @pl.when(j == 0)
        def _():
            ring(4, b).start()
            ring(5, b).start()

        @pl.when(j == 1)
        def _():
            ring(6, b).start()

        @pl.when(j == 2)
        def _():
            ring(8, b).start()

    def add_half(b, device, part, ref):
        @pl.loop(0, half, step=LN_ROWS)
        def _(i):
            at = pl.ds(pl.multiple_of(device * rows + part * half + i, LN_ROWS), LN_ROWS)
            t_ref[b, at, :] += ref[b, pl.ds(pl.multiple_of(i, LN_ROWS), LN_ROWS), :]

    def ring_second(b):
        ring(4, b).wait_recv()
        add_half(b, plus, 0, hp_ref)
        ring(7, b).start()
        ring(5, b).wait_recv()
        add_half(b, minus, 1, hm_ref)
        ring(9, b).start()

    def unit(b, cc):
        r0 = pl.multiple_of(cc * pair, pair)
        at = pl.ds(r0, pair)

        @pl.loop(0, pair, step=LN_ROWS)
        def _(i):
            sub = pl.ds(pl.multiple_of(r0 + i, LN_ROWS), LN_ROWS)
            xs = x_ref[b, sub, :].astype(F32)
            mu = jnp.mean(xs, axis=-1, keepdims=True)
            xc = xs - mu
            rstd = lax.rsqrt(jnp.mean(xc * xc, axis=-1, keepdims=True) + NORM_EPS)
            xh = xc * rstd
            mu_ref[b, sub, :] = mu
            rstd_ref[b, sub, :] = rstd
            a_ref[b, sub, :] = (xh * ln_ref[0:1, :] + ln_ref[1:2, :]).astype(BF16)
            m_ref[b, sub, :] = (xh * ln_ref[2:3, :] + ln_ref[3:4, :]).astype(BF16)

        a = a_ref[b, at, :]
        dy = dy_ref[b, at, :]
        cos = cos_ref[at, :]
        sin = sin_ref[at, :]
        q = dot_nt(a, wq_ref[0:2 * hd, :]).astype(BF16).astype(F32)
        q_ref[b, at, :] = (q * cos + pltpu.roll(q, hd, 1) * sin).astype(BF16)
        k = dot_nt(a, wq_ref[2 * hd:4 * hd, :]).astype(BF16).astype(F32)
        k2 = k * cos + pltpu.roll(k, hd, 1) * sin
        k_ref[b, at, :] = k2.astype(BF16)
        kt_ref[b, :, at] = k2.T.astype(BF16)
        v = dot_nt(a, wq_ref[4 * hd:6 * hd, :])
        v_ref[b, at, :] = v.astype(BF16)
        vt_ref[b, :, at] = v.T.astype(BF16)
        dc_ref[b, at, :] = dot_nt(dy, wo_ref[...]).astype(BF16)
        m = m_ref[b, at, :]
        for f in range(0, ff, BLK):
            h = dot_nn(m, wu_ref[:, f:f + BLK])
            du = dot_nt(dy, wd_ref[f:f + BLK, :])
            cdf = 0.5 * (1.0 + lax.erf(h * SQRT_HALF))
            pdf = jnp.exp2(h * h * (-0.5 * LOG2E)) * INV_SQRT_2PI
            u_ref[b, at, f:f + BLK] = (h * cdf).astype(BF16)
            dh_ref[b, at, f:f + BLK] = (du * (cdf + h * pdf)).astype(BF16)
        dh = dh_ref[b, at, :]
        mu = mu_ref[b, at, :]
        rstd = rstd_ref[b, at, :]
        for d in range(0, width, BLK):
            cols = slice(d, d + BLK)
            dm = dot_nt(dh, wu_ref[cols, :])
            xh = (x_ref[b, at, cols].astype(F32) - mu) * rstd
            t_ref[b, at, cols] = dm * ln_ref[2:3, cols]
            acc_ref[2, :, cols] += fold8(dm * xh)
            acc_ref[3, :, cols] += fold8(dm)

    def attention_head(b, h):
        lane = lax.broadcasted_iota(jnp.int32, (1, 2 * hd), 1)
        q_mask = lax.rem(lane // hh, 2) == h
        v_mask = (lane // hd) == h
        qm_ref[...] = jnp.where(q_mask, q_ref[b], jnp.zeros((), BF16))
        dcm_ref[...] = jnp.where(v_mask, dc_ref[b], jnp.zeros((), BF16))
        v_rows = pl.ds(pl.multiple_of(h * hd, hd), hd)
        k_lo = pl.ds(pl.multiple_of(h * hh, hh), hh)
        k_hi = pl.ds(pl.multiple_of(hd + h * hh, hh), hh)
        for qb in range(seq // BLK):
            qs = slice(qb * BLK, (qb + 1) * BLK)
            kl = (qb + 1) * BLK
            qm = qm_ref[qs, :]
            dcm = dcm_ref[qs, :]
            top = None
            for kb in range(qb + 1):
                ks = slice(kb * BLK, (kb + 1) * BLK)
                s = dot_nt(k_ref[b, ks, :], qm)
                if kb == qb:
                    key = lax.broadcasted_iota(jnp.int32, (BLK, BLK), 0)
                    query = lax.broadcasted_iota(jnp.int32, (BLK, BLK), 1)
                    s = jnp.where(key <= query, s, NEG_BIG)
                s_ref[ks, :] = s
                best = jnp.max(s.reshape(BLK // 8, 8, BLK), axis=0)
                top = best if top is None else jnp.maximum(top, best)
            top = jnp.max(top, axis=0, keepdims=True)
            total = jnp.zeros((8, BLK), F32)
            weighted = jnp.zeros((8, BLK), F32)
            for kb in range(qb + 1):
                ks = slice(kb * BLK, (kb + 1) * BLK)
                e = jnp.exp2((s_ref[ks, :] - top) * (scale * LOG2E))
                dpr = dot_nt(v_ref[b, ks, :], dcm)
                s_ref[ks, :] = e
                dp_ref[ks, :] = dpr
                total += fold8(e)
                weighted += fold8(e * dpr)
            inv = 1.0 / jnp.sum(total, axis=0, keepdims=True)
            mean_dp = jnp.sum(weighted, axis=0, keepdims=True) * inv
            for kb in range(qb + 1):
                ks = slice(kb * BLK, (kb + 1) * BLK)
                p = s_ref[ks, :] * inv
                pt_ref[ks, qs] = p.astype(BF16)
                ds_ref[ks, qs] = (p * (dp_ref[ks, :] - mean_dp) * scale).astype(BF16)
            c = dot_nn(vt_ref[b, v_rows, 0:kl], pt_ref[0:kl, qs])
            ct_ref[b, v_rows, qs] = c.astype(BF16)
            kt = jnp.concatenate([kt_ref[b, k_lo, 0:kl], kt_ref[b, k_hi, 0:kl]], axis=0)
            dq = dot_nn(kt, ds_ref[0:kl, qs])
            dqt_ref[k_lo, qs] = dq[0:hh]
            dqt_ref[k_hi, qs] = dq[hh:hd]
        for kb in range(seq // BLK):
            ks = slice(kb * BLK, (kb + 1) * BLK)
            dva_ref[ks, :] += dot_nn(pt_ref[ks, kb * BLK:], dcm_ref[kb * BLK:, :])
            dka_ref[ks, :] += dot_nn(ds_ref[ks, kb * BLK:], qm_ref[kb * BLK:, :])

    def attention_finish(b):
        @pl.loop(0, seq, step=BLK)
        def _(i):
            at = pl.ds(pl.multiple_of(i, BLK), BLK)
            cos = cos_ref[at, :]
            sin = sin_ref[at, :]
            dq = dqt_ref[:, at].T
            dqkv_ref[b, at, 0:2 * hd] = (dq * cos - pltpu.roll(dq, hd, 1) * sin).astype(BF16)
            dk = dka_ref[at, :]
            dqkv_ref[b, at, 2 * hd:4 * hd] = (dk * cos - pltpu.roll(dk, hd, 1) * sin).astype(BF16)
            dqkv_ref[b, at, 4 * hd:6 * hd] = dva_ref[at, :].astype(BF16)

    def input_grad(b, cc):
        at = pl.ds(pl.multiple_of(cc * pair, pair), pair)
        dqkv = dqkv_ref[b, at, :]
        mu = mu_ref[b, at, :]
        rstd = rstd_ref[b, at, :]
        for d in range(0, width, BLK):
            cols = slice(d, d + BLK)
            da = dot_nn(dqkv, wq_ref[:, cols])
            xh = (x_ref[b, at, cols].astype(F32) - mu) * rstd
            t_ref[b, at, cols] += da * ln_ref[0:1, cols]
            acc_ref[0, :, cols] += fold8(da * xh)
            acc_ref[1, :, cols] += fold8(da)

    def finish(b):
        for kind, ref in ((6, fp_ref), (7, fp_ref), (8, fm_ref), (9, fm_ref)):
            ring(kind, b).wait_recv()

        @pl.loop(0, rows, step=LN_ROWS)
        def _(i):
            at = pl.ds(pl.multiple_of(me * rows + i, LN_ROWS), LN_ROWS)
            sub = pl.ds(pl.multiple_of(i, LN_ROWS), LN_ROWS)
            t = t_ref[b, at, :] + fp_ref[b, sub, :] + fm_ref[b, sub, :]
            rstd = rstd_ref[b, at, :]
            xh = (x_ref[b, at, :].astype(F32) - mu_ref[b, at, :]) * rstd
            n = rstd * (t - jnp.mean(t, axis=-1, keepdims=True) - xh * jnp.mean(t * xh, axis=-1, keepdims=True))
            gi_ref[b, sub, :] = (dy_ref[b, at, :].astype(F32) + n).astype(BF16)

        pltpu.make_async_copy(gi_ref.at[b], gi_out.at[b], store_sem.at[b]).start()

    send_ring(0)
    send_partner(0)
    send_partner(1)
    acc_ref[...] = jnp.zeros_like(acc_ref)
    for copy in loads:
        copy.wait()

    @pl.loop(0, batch)
    def _(b):
        @pl.loop(b * 2, nc + 1)
        def _(i):
            step = i - 1

            @pl.when(i == 0)
            def _():
                arrived(4, 0)
                arrived(5, 0)

            @pl.when((step == 0) & (b == 0))
            def _():
                arrived(4, 1)
                arrived(5, 1)

            @pl.when((step == 1) & (b == 0))
            def _():
                service_first(0)
                send_ring(1)
                service_second(0)

            @pl.when(step == 1)
            def _():
                arrived(10, b)
                arrived(11, b)

            @pl.when(step == 2)
            def _():
                arrived(8, b)
                arrived(9, b)

            @pl.when((step == 2) & (b == 1))
            def _():
                ring_second(0)

            @pl.when(step == 3)
            def _():
                service_far(b)

            unit(jnp.where(step == 0, 1, b), lax.rem(chip + pick(jnp.maximum(step, 0), GATHER_ORDER), nc))

        @pl.when(b == 0)
        def _():
            service_first(1)

        dka_ref[...] = jnp.zeros_like(dka_ref)
        dva_ref[...] = jnp.zeros_like(dva_ref)

        @pl.loop(0, 2)
        def _(h):
            attention_head(b, h)

        @pl.when(b == 0)
        def _():
            service_second(1)

        attention_finish(b)

        @pl.loop(0, nc + 1)
        def _(j):
            @pl.when(j < nc)
            def _():
                input_grad(b, lax.rem(chip + pick(j, SCATTER_ORDER + (0,)), nc))

            for jj in range(nc):
                @pl.when(j == jj)
                def _(jj=jj):
                    to_partner(b, jj, SCATTER_ORDER[jj]).start()

            @pl.when(j > 0)
            def _():
                add_partner(b, j - 1)
                ring_after_partner(b, j - 1)

    for r in range(4):
        gls_ref[r:r + 1, :] = jnp.sum(acc_ref[r], axis=0, keepdims=True)
    gl_ref[me] = gls_ref[...]

    def gl_copy(j, source):
        return pltpu.make_async_remote_copy(
            src_ref=gls_ref, dst_ref=gl_ref.at[source], send_sem=gl_send.at[j], recv_sem=gl_recv.at[j],
            device_id={"tp": lax.rem(me + j, nt)}, device_id_type=MESH_ID)

    for j in range(1, nt):
        gl_copy(j, me).start()

    @pl.loop(0, width, step=BLK)
    def _(i):
        cols = pl.ds(pl.multiple_of(i, BLK), BLK)
        total = dot_tn(m_ref[0, :, cols], dh_ref[0])
        for b in range(1, batch):
            total += dot_tn(m_ref[b, :, cols], dh_ref[b])
        gu_ref[cols, :] = total.astype(BF16)

    ring_second(1)
    stores = [pltpu.make_async_copy(gu_ref, gu_out, store_sem.at[batch])]
    stores[-1].start()

    @pl.loop(0, width, step=BLK)
    def _(i):
        cols = pl.ds(pl.multiple_of(i, BLK), BLK)
        total = dot_tn(u_ref[0], dy_ref[0, :, cols])
        for b in range(1, batch):
            total += dot_tn(u_ref[b], dy_ref[b, :, cols])
        gd_ref[:, cols] = total.astype(BF16)

    stores.append(pltpu.make_async_copy(gd_ref, gd_out, store_sem.at[batch + 1]))
    stores[-1].start()

    @pl.loop(0, width, step=BLK)
    def _(i):
        cols = pl.ds(pl.multiple_of(i, BLK), BLK)
        total = dot_tn(dqkv_ref[0], a_ref[0, :, cols])
        out = dot_nn(ct_ref[0], dy_ref[0, :, cols])
        for b in range(1, batch):
            total += dot_tn(dqkv_ref[b], a_ref[b, :, cols])
            out += dot_nn(ct_ref[b], dy_ref[b, :, cols])
        gq_ref[:, cols] = total.astype(BF16)
        go_ref[:, cols] = out.astype(BF16)

    def store(src, dst):
        stores.append(pltpu.make_async_copy(src, dst, store_sem.at[batch + len(stores)]))
        stores[-1].start()

    store(go_ref, go_out)
    for t, base in ((0, 0), (1, 2 * hd)):
        for part in range(2):
            for g in range(2):
                store(gq_ref.at[pl.ds(base + part * hd + g * hh, hh), :],
                      gq_out.at[pl.ds(g * 3 * hd + t * hd + part * hh, hh), :])
    for g in range(2):
        store(gq_ref.at[pl.ds(4 * hd + g * hd, hd), :], gq_out.at[pl.ds(g * 3 * hd + 2 * hd, hd), :])

    for j in range(1, nt):
        gl_copy(j, lax.rem(me + nt - j, nt)).wait_recv()
    total = gl_ref[0]
    for j in range(1, nt):
        total += gl_ref[j]
    gl_out[...] = total

    finish(0)
    finish(1)

    for b in range(batch):
        pltpu.make_async_copy(gi_ref.at[b], gi_out.at[b], store_sem.at[b]).wait()
        for kind in range(6):
            own(kind, b).wait_send()
        for kind in range(6, 14):
            forward(kind, b).wait_send()
        for j in range(nc):
            to_partner(b, j, SCATTER_ORDER[j]).wait_send()
        for kind in range(4, 10):
            ring(kind, b).wait_send()
    for j in range(1, nt):
        gl_copy(j, me).wait_send()
    for copy in stores:
        copy.wait()


def rope_tables(seq_len, head_dim):
    half_dim = head_dim // 2
    inv_freq = np.float32(ROPE_BASE) ** (np.float32(-2.0) * np.arange(half_dim, dtype=np.float32) / np.float32(head_dim))
    angles = np.arange(seq_len, dtype=np.float32)[:, None] * inv_freq[None, :]
    cos, sin = np.cos(angles), np.sin(angles)
    return jnp.asarray(np.concatenate([cos] * 4, axis=1)), jnp.asarray(np.concatenate([-sin, -sin, sin, sin], axis=1))


def solution(mesh):
    act_spec = P('dp', 'tp', None)
    nt = mesh.shape['tp']
    nc = nt // 2

    def device_step(layer_in, grad_out, w_qkv, w_out, w_up, w_down, ln_params):
        batch, rows, width = layer_in.shape
        seq = rows * nt
        groups, _, hd = w_qkv.shape[1:]
        ff = w_up.shape[1]
        wq = jnp.transpose(w_qkv, (1, 2, 3, 0)).reshape(groups * 3 * hd, width)
        wo = w_out.reshape(groups * hd, width)
        cos, sin = rope_tables(seq, hd)
        lanes = groups * hd
        any_spec = pl.BlockSpec(memory_space=pl.ANY)
        vmem_spec = pl.BlockSpec(memory_space=pltpu.VMEM)
        vm = pltpu.VMEM
        dma = pltpu.SemaphoreType.DMA
        outs = pl.pallas_call(
            functools.partial(layer_kernel, nt),
            out_shape=(
                jax.ShapeDtypeStruct((batch, rows, width), BF16),
                jax.ShapeDtypeStruct((groups * 3 * hd, width), BF16),
                jax.ShapeDtypeStruct((lanes, width), BF16),
                jax.ShapeDtypeStruct((width, ff), BF16),
                jax.ShapeDtypeStruct((ff, width), BF16),
                jax.ShapeDtypeStruct((4, width), F32),
            ),
            in_specs=[any_spec] * 6 + [vmem_spec] + [any_spec] * 2,
            out_specs=(any_spec,) * 5 + (vmem_spec,),
            scratch_shapes=[
                vm((batch, seq, width), BF16), vm((batch, seq, width), BF16),
                vm((batch, seq, width), BF16), vm((batch, seq, width), BF16),
                vm((groups * 3 * hd, width), BF16), vm((lanes, width), BF16), vm((width, ff), BF16), vm((ff, width), BF16),
                vm((seq, lanes), F32), vm((seq, lanes), F32),
                vm((batch, seq, lanes), BF16), vm((batch, seq, lanes), BF16), vm((batch, seq, lanes), BF16), vm((batch, seq, lanes), BF16),
                vm((batch, lanes, seq), BF16), vm((batch, lanes, seq), BF16),
                vm((batch, seq, ff), BF16), vm((batch, seq, ff), BF16),
                vm((batch, seq, width), F32), vm((batch, nc, rows, width), F32),
                vm((batch, rows // 2, width), F32), vm((batch, rows // 2, width), F32),
                vm((batch, rows, width), F32), vm((batch, rows, width), F32),
                vm((batch, seq, 1), F32), vm((batch, seq, 1), F32),
                vm((seq, BLK), F32), vm((seq, BLK), F32), vm((seq, seq), BF16), vm((seq, seq), BF16),
                vm((seq, lanes), BF16), vm((seq, lanes), BF16), vm((seq, lanes), F32), vm((seq, lanes), F32),
                vm((lanes, seq), F32), vm((batch, seq, 3 * lanes), BF16), vm((batch, lanes, seq), BF16),
                vm((4, 8, width), F32), vm((nt, 4, width), F32), vm((4, width), F32),
                vm((batch, rows, width), BF16), vm((3 * lanes, width), BF16), vm((lanes, width), BF16), vm((width, ff), BF16), vm((ff, width), BF16),
                dma((17,)), dma((batch + 13,)), dma((batch, 14)), dma((batch, 14)), dma((batch, 10)), dma((batch, 10)), dma((nt,)), dma((nt,)),
            ],
            compiler_params=pltpu.CompilerParams(collective_id=0, has_side_effects=True, vmem_limit_bytes=66000000),
            name="layer_backward",
        )(layer_in, grad_out, wq, wo, w_up, w_down, ln_params, cos, sin)
        grad_in, gq, go, gu, gd, gl = outs
        gq = jnp.transpose(gq.reshape(groups, 3, hd, width), (3, 0, 1, 2))
        return grad_in, gq, go.reshape(w_out.shape), gu, gd, gl

    return jax.shard_map(
        device_step,
        mesh=mesh,
        in_specs=(act_spec, act_spec, P(None, 'tp', None, None), P('tp', None, None, None), P(None, 'tp'), P('tp', None), P(None, None)),
        out_specs=(act_spec, P('dp', 'tp', None, None), P(('dp', 'tp'), None, None, None), P('dp', 'tp'), P(('dp', 'tp'), None), P('dp', None)),
        check_vma=False,
    )
```

```python
import functools

import jax
import jax.numpy as jnp
import numpy as np
from jax import lax
from jax.experimental import pallas as pl
from jax.experimental.pallas import tpu as pltpu
from jax.sharding import PartitionSpec as P

NORM_EPS = 1e-5
ROPE_BASE = 10000.0
NEG_BIG = -1e30
LOG2E = 1.4426950408889634
SQRT_HALF = 0.7071067811865476
INV_SQRT_2PI = 0.3989422804014327
F32 = jnp.float32
BF16 = jnp.bfloat16
MESH_ID = pl.DeviceIdType.MESH
BLK = 256
LN_ROWS = 32
GATHER_ORDER = (0, 1, 3, 2)
SCATTER_ORDER = (2, 1, 3, 0)


def pick(index, values):
    out = values[-1]
    for i in range(len(values) - 2, -1, -1):
        out = jnp.where(index == i, values[i], out)
    return out


def dot_nn(lhs, rhs):
    return lax.dot_general(lhs, rhs, (((1,), (0,)), ((), ())), preferred_element_type=F32)


def dot_nt(lhs, rhs):
    return lax.dot_general(lhs, rhs, (((1,), (1,)), ((), ())), preferred_element_type=F32)


def dot_tn(lhs, rhs):
    return lax.dot_general(lhs, rhs, (((0,), (0,)), ((), ())), preferred_element_type=F32)


def fold8(value):
    rows, cols = value.shape
    return jnp.sum(value.reshape(rows // 8, 8, cols), axis=0)


def layer_kernel(nt, x_in, dy_in, wq_in, wo_in, wu_in, wd_in, ln_ref, cos_in, sin_in,
                 gi_out, gq_out, go_out, gu_out, gd_out, gl_out,
                 x_ref, dy_ref, a_ref, m_ref, wq_ref, wo_ref, wu_ref, wd_ref, cos_ref, sin_ref,
                 q_ref, k_ref, v_ref, dc_ref, kt_ref, vt_ref, u_ref, dh_ref, t_ref, p_ref,
                 hp_ref, hm_ref, fp_ref, fm_ref, mu_ref, rstd_ref, s_ref, dp_ref, pt_ref, ds_ref,
                 qm_ref, dcm_ref, dka_ref, dva_ref, dqt_ref, dqkv_ref, ct_ref, acc_ref, gl_ref, gls_ref,
                 gi_ref, gq_ref, go_ref, gu_ref, gd_ref,
                 load_sem, store_sem, ag_send, ag_recv, rs_send, rs_recv, gl_send, gl_recv):
    nc = nt // 2
    batch, seq, width = x_ref.shape
    ff = wu_ref.shape[1]
    rows = x_in.shape[1]
    half = rows // 2
    pair = 2 * rows
    hd = wo_in.shape[0] // 2
    hh = hd // 2
    scale = hd ** -0.5

    me = lax.axis_index("tp")
    chip = me // 2
    core = lax.rem(me, 2)
    partner = chip * 2 + (1 - core)

    def dev(off, which):
        return lax.rem(chip + off, nc) * 2 + which

    plus = dev(1, core)
    minus = dev(nc - 1, core)

    def row0(device):
        return pl.multiple_of(device * rows, rows)

    loads = []

    def load(src, dst):
        loads.append(pltpu.make_async_copy(src, dst, load_sem.at[len(loads)]))
        loads[-1].start()

    barrier = pltpu.get_barrier_semaphore()
    for target in (plus, minus, partner):
        pl.semaphore_signal(barrier, inc=1, device_id={"tp": target}, device_id_type=MESH_ID)

    load(x_in, x_ref.at[:, pl.ds(row0(me), rows), :])
    load(dy_in, dy_ref.at[:, pl.ds(row0(me), rows), :])
    for t, base in ((0, 0), (1, 2 * hd)):
        for part in range(2):
            for g in range(2):
                load(wq_in.at[pl.ds(g * 3 * hd + t * hd + part * hh, hh), :],
                     wq_ref.at[pl.ds(base + part * hd + g * hh, hh), :])
    for g in range(2):
        load(wq_in.at[pl.ds(g * 3 * hd + 2 * hd, hd), :], wq_ref.at[pl.ds(4 * hd + g * hd, hd), :])
    load(cos_in, cos_ref)
    load(sin_in, sin_ref)
    load(wo_in, wo_ref)
    load(wu_in, wu_ref)
    load(wd_in, wd_ref)

    loads[0].wait()
    loads[1].wait()
    pl.semaphore_wait(barrier, 3)

    def ag(kind, src, dst, b, target):
        return pltpu.make_async_remote_copy(
            src_ref=src, dst_ref=dst, send_sem=ag_send.at[b, kind], recv_sem=ag_recv.at[b, kind],
            device_id={"tp": target}, device_id_type=MESH_ID)

    def rows_of(ref, b, device):
        return ref.at[b, pl.ds(row0(device), rows), :]

    def own(kind, b):
        ref = (x_ref, dy_ref)[kind % 2]
        target = (plus, minus, partner)[kind // 2]
        return ag(kind, rows_of(ref, b, me), rows_of(ref, b, me), b, target)

    def forward(kind, b):
        if kind == 6:
            return ag(kind, rows_of(x_ref, b, minus), rows_of(x_ref, b, minus), b, plus)
        if kind == 7:
            return ag(kind, rows_of(dy_ref, b, plus), rows_of(dy_ref, b, plus), b, minus)
        ref = (x_ref, dy_ref)[kind % 2]
        source = dev((nc - 1, 1, 2)[(kind - 8) // 2], core)
        return ag(kind, rows_of(ref, b, source), rows_of(ref, b, source), b, partner)

    def arrived(kind, b):
        ref = (x_ref, dy_ref)[kind % 2]
        if kind < 6:
            source = (minus, plus, partner)[kind // 2]
        elif kind < 8:
            source = dev(2, core)
        else:
            source = dev((nc - 1, 1, 2)[(kind - 8) // 2], 1 - core)
        ag(kind, rows_of(ref, b, source), rows_of(ref, b, source), b, partner).wait_recv()

    def send_ring(b):
        for kind in (0, 3, 1, 2):
            own(kind, b).start()

    def send_partner(b):
        for kind in (4, 5):
            own(kind, b).start()

    def service_first(b):
        arrived(0, b)
        forward(6, b).start()
        forward(8, b).start()
        arrived(3, b)
        forward(7, b).start()
        forward(11, b).start()

    def service_second(b):
        arrived(2, b)
        forward(10, b).start()
        arrived(1, b)
        forward(9, b).start()

    def service_far(b):
        arrived(6, b)
        forward(12, b).start()
        arrived(7, b)
        forward(13, b).start()

    def rs(kind, src, dst, b, target):
        return pltpu.make_async_remote_copy(
            src_ref=src, dst_ref=dst, send_sem=rs_send.at[b, kind], recv_sem=rs_recv.at[b, kind],
            device_id={"tp": target}, device_id_type=MESH_ID)

    def part_rows(b, device, part):
        if part is None:
            return t_ref.at[b, pl.ds(row0(device), rows), :]
        return t_ref.at[b, pl.ds(pl.multiple_of(device * rows + part * half, half), half), :]

    def to_partner(b, j, off):
        return rs(j, part_rows(b, dev(off, 1 - core), None), p_ref.at[b, j], b, partner)

    def ring(kind, b):
        lo, hi = pl.ds(0, half), pl.ds(half, half)
        if kind == 4:
            return rs(kind, part_rows(b, dev(2, core), 0), hp_ref.at[b], b, plus)
        if kind == 5:
            return rs(kind, part_rows(b, dev(2, core), 1), hm_ref.at[b], b, minus)
        if kind == 6:
            return rs(kind, part_rows(b, plus, 1), fp_ref.at[b, hi, :], b, plus)
        if kind == 7:
            return rs(kind, part_rows(b, plus, 0), fp_ref.at[b, lo, :], b, plus)
        if kind == 8:
            return rs(kind, part_rows(b, minus, 0), fm_ref.at[b, lo, :], b, minus)
        return rs(kind, part_rows(b, minus, 1), fm_ref.at[b, hi, :], b, minus)

    def add_partner(b, j):
        off = SCATTER_ORDER[j] if isinstance(j, int) else pick(j, SCATTER_ORDER)
        target = dev(off, core)
        rs(j, part_rows(b, target, None), p_ref.at[b, j], b, partner).wait_recv()

        @pl.loop(0, rows, step=LN_ROWS)
        def _(i):
            at = pl.ds(pl.multiple_of(target * rows + i, LN_ROWS), LN_ROWS)
            t_ref[b, at, :] += p_ref[b, j, pl.ds(pl.multiple_of(i, LN_ROWS), LN_ROWS), :]

    def ring_after_partner(b, j):
        @pl.when(j == 0)
        def _():
            ring(4, b).start()
            ring(5, b).start()

        @pl.when(j == 1)
        def _():
            ring(6, b).start()

        @pl.when(j == 2)
        def _():
            ring(8, b).start()

    def add_half(b, device, part, ref):
        @pl.loop(0, half, step=LN_ROWS)
        def _(i):
            at = pl.ds(pl.multiple_of(device * rows + part * half + i, LN_ROWS), LN_ROWS)
            t_ref[b, at, :] += ref[b, pl.ds(pl.multiple_of(i, LN_ROWS), LN_ROWS), :]

    def ring_second(b):
        ring(4, b).wait_recv()
        add_half(b, plus, 0, hp_ref)
        ring(7, b).start()
        ring(5, b).wait_recv()
        add_half(b, minus, 1, hm_ref)
        ring(9, b).start()

    def unit(b, cc):
        r0 = pl.multiple_of(cc * pair, pair)
        at = pl.ds(r0, pair)

        for i in range(0, pair, LN_ROWS):
            sub = pl.ds(pl.multiple_of(r0 + i, LN_ROWS), LN_ROWS)
            xs = x_ref[b, sub, :].astype(F32)
            mu = jnp.mean(xs, axis=-1, keepdims=True)
            xc = xs - mu
            rstd = lax.rsqrt(jnp.mean(xc * xc, axis=-1, keepdims=True) + NORM_EPS)
            xh = xc * rstd
            mu_ref[b, sub, :] = mu
            rstd_ref[b, sub, :] = rstd
            a_ref[b, sub, :] = (xh * ln_ref[0:1, :] + ln_ref[1:2, :]).astype(BF16)
            m_ref[b, sub, :] = (xh * ln_ref[2:3, :] + ln_ref[3:4, :]).astype(BF16)

        a = a_ref[b, at, :]
        dy = dy_ref[b, at, :]
        cos = cos_ref[at, :]
        sin = sin_ref[at, :]
        qk = dot_nt(a, wq_ref[0:4 * hd, :]).astype(BF16).astype(F32)
        q = qk[:, 0:2 * hd]
        q_ref[b, at, :] = (q * cos + pltpu.roll(q, hd, 1) * sin).astype(BF16)
        k = qk[:, 2 * hd:]
        k2 = k * cos + pltpu.roll(k, hd, 1) * sin
        k_ref[b, at, :] = k2.astype(BF16)
        kt_ref[b, :, at] = k2.T.astype(BF16)
        v = dot_nt(a, wq_ref[4 * hd:6 * hd, :])
        v_ref[b, at, :] = v.astype(BF16)
        vt_ref[b, :, at] = v.T.astype(BF16)
        dc_ref[b, at, :] = dot_nt(dy, wo_ref[...]).astype(BF16)
        m = m_ref[b, at, :]
        for f in range(0, ff, BLK):
            h = dot_nn(m, wu_ref[:, f:f + BLK])
            du = dot_nt(dy, wd_ref[f:f + BLK, :])
            cdf = 0.5 * (1.0 + lax.erf(h * SQRT_HALF))
            pdf = jnp.exp2(h * h * (-0.5 * LOG2E)) * INV_SQRT_2PI
            u_ref[b, at, f:f + BLK] = (h * cdf).astype(BF16)
            dh_ref[b, at, f:f + BLK] = (du * (cdf + h * pdf)).astype(BF16)
        dh = dh_ref[b, at, :]
        mu = mu_ref[b, at, :]
        rstd = rstd_ref[b, at, :]
        for d in range(0, width, BLK):
            cols = slice(d, d + BLK)
            dm = dot_nt(dh, wu_ref[cols, :])
            xh = (x_ref[b, at, cols].astype(F32) - mu) * rstd
            t_ref[b, at, cols] = dm * ln_ref[2:3, cols]
            acc_ref[2, :, cols] += fold8(dm * xh)
            acc_ref[3, :, cols] += fold8(dm)

    def attention_head(b, h):
        lane = lax.broadcasted_iota(jnp.int32, (1, 2 * hd), 1)
        q_mask = lax.rem(lane // hh, 2) == h
        v_mask = (lane // hd) == h
        qm_ref[...] = jnp.where(q_mask, q_ref[b], jnp.zeros((), BF16))
        dcm_ref[...] = jnp.where(v_mask, dc_ref[b], jnp.zeros((), BF16))
        v_rows = pl.ds(pl.multiple_of(h * hd, hd), hd)
        k_lo = pl.ds(pl.multiple_of(h * hh, hh), hh)
        k_hi = pl.ds(pl.multiple_of(hd + h * hh, hh), hh)
        for qb in range(seq // BLK):
            qs = slice(qb * BLK, (qb + 1) * BLK)
            kl = (qb + 1) * BLK
            qm = qm_ref[qs, :]
            dcm = dcm_ref[qs, :]
            top = None
            for kb in range(qb + 1):
                ks = slice(kb * BLK, (kb + 1) * BLK)
                s = dot_nt(k_ref[b, ks, :], qm)
                if kb == qb:
                    key = lax.broadcasted_iota(jnp.int32, (BLK, BLK), 0)
                    query = lax.broadcasted_iota(jnp.int32, (BLK, BLK), 1)
                    s = jnp.where(key <= query, s, NEG_BIG)
                s_ref[ks, :] = s
                best = jnp.max(s.reshape(BLK // 8, 8, BLK), axis=0)
                top = best if top is None else jnp.maximum(top, best)
            top = jnp.max(top, axis=0, keepdims=True)
            total = jnp.zeros((8, BLK), F32)
            weighted = jnp.zeros((8, BLK), F32)
            for kb in range(qb + 1):
                ks = slice(kb * BLK, (kb + 1) * BLK)
                e = jnp.exp2((s_ref[ks, :] - top) * (scale * LOG2E))
                dpr = dot_nt(v_ref[b, ks, :], dcm)
                s_ref[ks, :] = e
                dp_ref[ks, :] = dpr
                total += fold8(e)
                weighted += fold8(e * dpr)
            inv = 1.0 / jnp.sum(total, axis=0, keepdims=True)
            mean_dp = jnp.sum(weighted, axis=0, keepdims=True) * inv
            for kb in range(qb + 1):
                ks = slice(kb * BLK, (kb + 1) * BLK)
                p = s_ref[ks, :] * inv
                pt_ref[ks, qs] = p.astype(BF16)
                ds_ref[ks, qs] = (p * (dp_ref[ks, :] - mean_dp) * scale).astype(BF16)
            c = dot_nn(vt_ref[b, v_rows, 0:kl], pt_ref[0:kl, qs])
            ct_ref[b, v_rows, qs] = c.astype(BF16)
            kt = jnp.concatenate([kt_ref[b, k_lo, 0:kl], kt_ref[b, k_hi, 0:kl]], axis=0)
            dq = dot_nn(kt, ds_ref[0:kl, qs])
            dqt_ref[k_lo, qs] = dq[0:hh]
            dqt_ref[k_hi, qs] = dq[hh:hd]
        for kb in range(seq // BLK):
            ks = slice(kb * BLK, (kb + 1) * BLK)
            dva_ref[ks, :] += dot_nn(pt_ref[ks, kb * BLK:], dcm_ref[kb * BLK:, :])
            dka_ref[ks, :] += dot_nn(ds_ref[ks, kb * BLK:], qm_ref[kb * BLK:, :])

    def attention_finish(b):
        @pl.loop(0, seq, step=BLK)
        def _(i):
            at = pl.ds(pl.multiple_of(i, BLK), BLK)
            cos = cos_ref[at, :]
            sin = sin_ref[at, :]
            dq = dqt_ref[:, at].T
            dqkv_ref[b, at, 0:2 * hd] = (dq * cos - pltpu.roll(dq, hd, 1) * sin).astype(BF16)
            dk = dka_ref[at, :]
            dqkv_ref[b, at, 2 * hd:4 * hd] = (dk * cos - pltpu.roll(dk, hd, 1) * sin).astype(BF16)
            dqkv_ref[b, at, 4 * hd:6 * hd] = dva_ref[at, :].astype(BF16)

    def input_grad(b, cc):
        at = pl.ds(pl.multiple_of(cc * pair, pair), pair)
        dqkv = dqkv_ref[b, at, :]
        mu = mu_ref[b, at, :]
        rstd = rstd_ref[b, at, :]
        for d in range(0, width, BLK):
            cols = slice(d, d + BLK)
            da = dot_nn(dqkv, wq_ref[:, cols])
            xh = (x_ref[b, at, cols].astype(F32) - mu) * rstd
            t_ref[b, at, cols] += da * ln_ref[0:1, cols]
            acc_ref[0, :, cols] += fold8(da * xh)
            acc_ref[1, :, cols] += fold8(da)

    def finish(b):
        for kind, ref in ((6, fp_ref), (7, fp_ref), (8, fm_ref), (9, fm_ref)):
            ring(kind, b).wait_recv()

        @pl.loop(0, rows, step=LN_ROWS, unroll=2)
        def _(i):
            at = pl.ds(pl.multiple_of(me * rows + i, LN_ROWS), LN_ROWS)
            sub = pl.ds(pl.multiple_of(i, LN_ROWS), LN_ROWS)
            t = t_ref[b, at, :] + fp_ref[b, sub, :] + fm_ref[b, sub, :]
            rstd = rstd_ref[b, at, :]
            xh = (x_ref[b, at, :].astype(F32) - mu_ref[b, at, :]) * rstd
            n = rstd * (t - jnp.mean(t, axis=-1, keepdims=True) - xh * jnp.mean(t * xh, axis=-1, keepdims=True))
            gi_ref[b, sub, :] = (dy_ref[b, at, :].astype(F32) + n).astype(BF16)

        pltpu.make_async_copy(gi_ref.at[b], gi_out.at[b], store_sem.at[b]).start()

    send_ring(0)
    send_partner(0)
    send_partner(1)
    acc_ref[...] = jnp.zeros_like(acc_ref)
    for copy in loads[2:]:
        copy.wait()

    @pl.loop(0, batch)
    def _(b):
        @pl.loop(b * 2, nc + 1)
        def _(i):
            step = i - 1

            @pl.when(i == 0)
            def _():
                arrived(4, 0)
                arrived(5, 0)

            @pl.when((step == 0) & (b == 0))
            def _():
                arrived(4, 1)
                arrived(5, 1)

            @pl.when((step == 1) & (b == 0))
            def _():
                service_first(0)
                send_ring(1)
                service_second(0)

            @pl.when(step == 1)
            def _():
                arrived(10, b)
                arrived(11, b)

            @pl.when(step == 2)
            def _():
                arrived(8, b)
                arrived(9, b)

            @pl.when((step == 2) & (b == 1))
            def _():
                for j in range(1, nc):
                    add_partner(0, j)
                    ring_after_partner(0, j)

            @pl.when(step == 3)
            def _():
                service_far(b)
                arrived(12, b)
                arrived(13, b)

            unit(jnp.where(step == 0, 1, b), lax.rem(chip + pick(jnp.maximum(step, 0), GATHER_ORDER), nc))

        @pl.when(b == 0)
        def _():
            service_first(1)

        dka_ref[...] = jnp.zeros_like(dka_ref)
        dva_ref[...] = jnp.zeros_like(dva_ref)

        @pl.loop(0, 2)
        def _(h):
            attention_head(b, h)

            @pl.when((b == 1) & (h == 0))
            def _():
                ring_second(0)

        @pl.when(b == 0)
        def _():
            service_second(1)

        attention_finish(b)

        @pl.loop(0, nc + 1)
        def _(j):
            @pl.when(j < nc)
            def _():
                input_grad(b, lax.rem(chip + pick(j, SCATTER_ORDER + (0,)), nc))

            for jj in range(nc):
                @pl.when(j == jj)
                def _(jj=jj):
                    to_partner(b, jj, SCATTER_ORDER[jj]).start()

            @pl.when(((j > 0) & (b == 1)) | (j == nc))
            def _():
                which = jnp.where(b == 1, j - 1, 0)
                add_partner(b, which)
                ring_after_partner(b, which)

    for r in range(4):
        gls_ref[0, r:r + 1, :] = jnp.sum(acc_ref[r], axis=0, keepdims=True)

    def gl_copy(kind, src, dst, target):
        return pltpu.make_async_remote_copy(
            src_ref=src, dst_ref=dst, send_sem=gl_send.at[kind], recv_sem=gl_recv.at[kind],
            device_id={"tp": target}, device_id_type=MESH_ID)

    def from_chip(off):
        return gl_ref.at[lax.rem(chip + off, nc)]

    gl_pair = gl_copy(0, gls_ref.at[0], gls_ref.at[1], partner)
    gl_plus = gl_copy(1, from_chip(0), from_chip(0), plus)
    gl_minus = gl_copy(2, from_chip(0), from_chip(0), minus)
    gl_far = gl_copy(3, from_chip(nc - 1), from_chip(nc - 1), plus)
    gl_pair.start()

    @pl.loop(0, width, step=BLK)
    def _(i):
        cols = pl.ds(pl.multiple_of(i, BLK), BLK)
        total = dot_tn(m_ref[0, :, cols], dh_ref[0])
        for b in range(1, batch):
            total += dot_tn(m_ref[b, :, cols], dh_ref[b])
        gu_ref[cols, :] = total.astype(BF16)

    gl_pair.wait_recv()
    gl_ref[chip] = gls_ref[0] + gls_ref[1]
    gl_plus.start()
    gl_minus.start()
    stores = [pltpu.make_async_copy(gu_ref, gu_out, store_sem.at[batch])]
    stores[-1].start()

    @pl.loop(0, width, step=BLK)
    def _(i):
        cols = pl.ds(pl.multiple_of(i, BLK), BLK)
        total = dot_tn(u_ref[0], dy_ref[0, :, cols])
        for b in range(1, batch):
            total += dot_tn(u_ref[b], dy_ref[b, :, cols])
        gd_ref[:, cols] = total.astype(BF16)

    stores.append(pltpu.make_async_copy(gd_ref, gd_out, store_sem.at[batch + 1]))
    stores[-1].start()

    @pl.loop(0, width, step=BLK)
    def _(i):
        cols = pl.ds(pl.multiple_of(i, BLK), BLK)
        total = dot_tn(dqkv_ref[0], a_ref[0, :, cols])
        out = dot_nn(ct_ref[0], dy_ref[0, :, cols])
        for b in range(1, batch):
            total += dot_tn(dqkv_ref[b], a_ref[b, :, cols])
            out += dot_nn(ct_ref[b], dy_ref[b, :, cols])
        gq_ref[:, cols] = total.astype(BF16)
        go_ref[:, cols] = out.astype(BF16)

    def store(src, dst):
        stores.append(pltpu.make_async_copy(src, dst, store_sem.at[batch + len(stores)]))
        stores[-1].start()

    store(go_ref, go_out)
    for t, base in ((0, 0), (1, 2 * hd)):
        for part in range(2):
            for g in range(2):
                store(gq_ref.at[pl.ds(base + part * hd + g * hh, hh), :],
                      gq_out.at[pl.ds(g * 3 * hd + t * hd + part * hh, hh), :])
    for g in range(2):
        store(gq_ref.at[pl.ds(4 * hd + g * hd, hd), :], gq_out.at[pl.ds(g * 3 * hd + 2 * hd, hd), :])

    finish(0)
    ring_second(1)
    gl_copy(1, from_chip(nc - 1), from_chip(nc - 1), plus).wait_recv()
    gl_far.start()
    finish(1)

    gl_copy(2, from_chip(1), from_chip(1), minus).wait_recv()
    gl_copy(3, from_chip(2), from_chip(2), plus).wait_recv()
    total = gl_ref[0]
    for j in range(1, nc):
        total += gl_ref[j]
    gl_out[...] = total

    for b in range(batch):
        pltpu.make_async_copy(gi_ref.at[b], gi_out.at[b], store_sem.at[b]).wait()
        for kind in range(6):
            own(kind, b).wait_send()
        for kind in range(6, 14):
            forward(kind, b).wait_send()
        for j in range(nc):
            to_partner(b, j, SCATTER_ORDER[j]).wait_send()
        for kind in range(4, 10):
            ring(kind, b).wait_send()
    for copy in (gl_pair, gl_plus, gl_minus, gl_far):
        copy.wait_send()
    for copy in stores:
        copy.wait()


def rope_tables(seq_len, head_dim):
    half_dim = head_dim // 2
    inv_freq = np.float32(ROPE_BASE) ** (np.float32(-2.0) * np.arange(half_dim, dtype=np.float32) / np.float32(head_dim))
    angles = np.arange(seq_len, dtype=np.float32)[:, None] * inv_freq[None, :]
    cos, sin = np.cos(angles), np.sin(angles)
    return jnp.asarray(np.concatenate([cos] * 4, axis=1)), jnp.asarray(np.concatenate([-sin, -sin, sin, sin], axis=1))


def solution(mesh):
    act_spec = P('dp', 'tp', None)
    nt = mesh.shape['tp']
    nc = nt // 2

    def device_step(layer_in, grad_out, w_qkv, w_out, w_up, w_down, ln_params):
        batch, rows, width = layer_in.shape
        seq = rows * nt
        groups, _, hd = w_qkv.shape[1:]
        ff = w_up.shape[1]
        wq = jnp.transpose(w_qkv, (1, 2, 3, 0)).reshape(groups * 3 * hd, width)
        wo = w_out.reshape(groups * hd, width)
        cos, sin = rope_tables(seq, hd)
        lanes = groups * hd
        any_spec = pl.BlockSpec(memory_space=pl.ANY)
        vmem_spec = pl.BlockSpec(memory_space=pltpu.VMEM)
        vm = pltpu.VMEM
        dma = pltpu.SemaphoreType.DMA
        outs = pl.pallas_call(
            functools.partial(layer_kernel, nt),
            out_shape=(
                jax.ShapeDtypeStruct((batch, rows, width), BF16),
                jax.ShapeDtypeStruct((groups * 3 * hd, width), BF16),
                jax.ShapeDtypeStruct((lanes, width), BF16),
                jax.ShapeDtypeStruct((width, ff), BF16),
                jax.ShapeDtypeStruct((ff, width), BF16),
                jax.ShapeDtypeStruct((4, width), F32),
            ),
            in_specs=[any_spec] * 6 + [vmem_spec] + [any_spec] * 2,
            out_specs=(any_spec,) * 5 + (vmem_spec,),
            scratch_shapes=[
                vm((batch, seq, width), BF16), vm((batch, seq, width), BF16),
                vm((batch, seq, width), BF16), vm((batch, seq, width), BF16),
                vm((groups * 3 * hd, width), BF16), vm((lanes, width), BF16), vm((width, ff), BF16), vm((ff, width), BF16),
                vm((seq, lanes), F32), vm((seq, lanes), F32),
                vm((batch, seq, lanes), BF16), vm((batch, seq, lanes), BF16), vm((batch, seq, lanes), BF16), vm((batch, seq, lanes), BF16),
                vm((batch, lanes, seq), BF16), vm((batch, lanes, seq), BF16),
                vm((batch, seq, ff), BF16), vm((batch, seq, ff), BF16),
                vm((batch, seq, width), F32), vm((batch, nc, rows, width), F32),
                vm((batch, rows // 2, width), F32), vm((batch, rows // 2, width), F32),
                vm((batch, rows, width), F32), vm((batch, rows, width), F32),
                vm((batch, seq, 1), F32), vm((batch, seq, 1), F32),
                vm((seq, BLK), F32), vm((seq, BLK), F32), vm((seq, seq), BF16), vm((seq, seq), BF16),
                vm((seq, lanes), BF16), vm((seq, lanes), BF16), vm((seq, lanes), F32), vm((seq, lanes), F32),
                vm((lanes, seq), F32), vm((batch, seq, 3 * lanes), BF16), vm((batch, lanes, seq), BF16),
                vm((4, 8, width), F32), vm((nc, 4, width), F32), vm((2, 4, width), F32),
                vm((batch, rows, width), BF16), vm((3 * lanes, width), BF16), vm((lanes, width), BF16), vm((width, ff), BF16), vm((ff, width), BF16),
                dma((17,)), dma((batch + 13,)), dma((batch, 14)), dma((batch, 14)), dma((batch, 10)), dma((batch, 10)), dma((4,)), dma((4,)),
            ],
            compiler_params=pltpu.CompilerParams(collective_id=0, has_side_effects=True, vmem_limit_bytes=66000000),
            name="layer_backward",
        )(layer_in, grad_out, wq, wo, w_up, w_down, ln_params, cos, sin)
        grad_in, gq, go, gu, gd, gl = outs
        gq = jnp.transpose(gq.reshape(groups, 3, hd, width), (3, 0, 1, 2))
        return grad_in, gq, go.reshape(w_out.shape), gu, gd, gl

    return jax.shard_map(
        device_step,
        mesh=mesh,
        in_specs=(act_spec, act_spec, P(None, 'tp', None, None), P('tp', None, None, None), P(None, 'tp'), P('tp', None), P(None, None)),
        out_specs=(act_spec, P('dp', 'tp', None, None), P(('dp', 'tp'), None, None, None), P('dp', 'tp'), P(('dp', 'tp'), None), P('dp', None)),
        check_vma=False,
    )
```

```python
import functools

import jax
import jax.numpy as jnp
import numpy as np
from jax import lax
from jax.experimental import pallas as pl
from jax.experimental.pallas import tpu as pltpu
from jax.sharding import PartitionSpec as P

NORM_EPS = 1e-5
ROPE_BASE = 10000.0
NEG_BIG = -1e30
LOG2E = 1.4426950408889634
SQRT_HALF = 0.7071067811865476
INV_SQRT_2PI = 0.3989422804014327
F32 = jnp.float32
BF16 = jnp.bfloat16
MESH_ID = pl.DeviceIdType.MESH
BLK = 256
LN_ROWS = 32
VMEM_LIMIT = 62000000
GATHER_ORDER = (0, 1, 3, 2)
SCATTER_ORDER = (2, 1, 3, 0)


def pick(index, values):
    out = values[-1]
    for i in range(len(values) - 2, -1, -1):
        out = jnp.where(index == i, values[i], out)
    return out


def dot_nn(lhs, rhs):
    return lax.dot_general(lhs, rhs, (((1,), (0,)), ((), ())), preferred_element_type=F32)


def dot_nt(lhs, rhs):
    return lax.dot_general(lhs, rhs, (((1,), (1,)), ((), ())), preferred_element_type=F32)


def dot_tn(lhs, rhs):
    return lax.dot_general(lhs, rhs, (((0,), (0,)), ((), ())), preferred_element_type=F32)


def fold8(value):
    rows, cols = value.shape
    return jnp.sum(value.reshape(rows // 8, 8, cols), axis=0)


def layer_kernel(nt, x_in, dy_in, wq_in, wo_in, wu_in, wd_in, ln_ref, cos_in, sin_in,
                 gi_ref, gq_ref, go_ref, gu_ref, gd_ref, gl_out,
                 x_ref, dy_ref, a_ref, m_ref, wq_ref, wo_ref, wu_ref, wd_ref, cos_ref, sin_ref,
                 q_ref, k_ref, v_ref, dc_ref, kt_ref, vt_ref, u_ref, dh_ref, t_ref, p_ref,
                 hp_ref, hm_ref, fp_ref, fm_ref, mu_ref, rstd_ref, s_ref, dp_ref, pt_ref, ds_ref,
                 qm_ref, dcm_ref, dka_ref, dva_ref, dqt_ref, dqkv_ref, ct_ref, acc_ref, gl_ref, gls_ref,
                 load_sem, ag_send, ag_recv, rs_send, rs_recv, gl_send, gl_recv):
    nc = nt // 2
    batch, seq, width = x_ref.shape
    ff = wu_ref.shape[1]
    rows = x_in.shape[1]
    half = rows // 2
    pair = 2 * rows
    hd = wo_in.shape[0] // 2
    hh = hd // 2
    scale = hd ** -0.5

    me = lax.axis_index("tp")
    chip = me // 2
    core = lax.rem(me, 2)
    partner = chip * 2 + (1 - core)

    def dev(off, which):
        return lax.rem(chip + off, nc) * 2 + which

    plus = dev(1, core)
    minus = dev(nc - 1, core)

    def row0(device):
        return pl.multiple_of(device * rows, rows)

    loads = []

    def load(src, dst):
        loads.append(pltpu.make_async_copy(src, dst, load_sem.at[len(loads)]))
        loads[-1].start()

    barrier = pltpu.get_barrier_semaphore()
    for target in (plus, minus, partner):
        pl.semaphore_signal(barrier, inc=1, device_id={"tp": target}, device_id_type=MESH_ID)

    load(x_in, x_ref.at[:, pl.ds(row0(me), rows), :])
    load(dy_in, dy_ref.at[:, pl.ds(row0(me), rows), :])
    for t, base in ((0, 0), (1, 2 * hd)):
        for part in range(2):
            for g in range(2):
                load(wq_in.at[pl.ds(g * 3 * hd + t * hd + part * hh, hh), :],
                     wq_ref.at[pl.ds(base + part * hd + g * hh, hh), :])
    for g in range(2):
        load(wq_in.at[pl.ds(g * 3 * hd + 2 * hd, hd), :], wq_ref.at[pl.ds(4 * hd + g * hd, hd), :])
    load(cos_in, cos_ref)
    load(sin_in, sin_ref)
    load(wo_in, wo_ref)
    load(wu_in, wu_ref)
    load(wd_in, wd_ref)

    loads[0].wait()
    loads[1].wait()
    pl.semaphore_wait(barrier, 3)

    def ag(kind, src, dst, b, target):
        return pltpu.make_async_remote_copy(
            src_ref=src, dst_ref=dst, send_sem=ag_send.at[b, kind], recv_sem=ag_recv.at[b, kind],
            device_id={"tp": target}, device_id_type=MESH_ID)

    def rows_of(ref, b, device):
        return ref.at[b, pl.ds(row0(device), rows), :]

    def own(kind, b):
        ref = (x_ref, dy_ref)[kind % 2]
        target = (plus, minus, partner)[kind // 2]
        return ag(kind, rows_of(ref, b, me), rows_of(ref, b, me), b, target)

    def forward(kind, b):
        if kind == 6:
            return ag(kind, rows_of(x_ref, b, minus), rows_of(x_ref, b, minus), b, plus)
        if kind == 7:
            return ag(kind, rows_of(dy_ref, b, plus), rows_of(dy_ref, b, plus), b, minus)
        ref = (x_ref, dy_ref)[kind % 2]
        source = dev((nc - 1, 1, 2)[(kind - 8) // 2], core)
        return ag(kind, rows_of(ref, b, source), rows_of(ref, b, source), b, partner)

    def arrived(kind, b):
        ref = (x_ref, dy_ref)[kind % 2]
        if kind < 6:
            source = (minus, plus, partner)[kind // 2]
        elif kind < 8:
            source = dev(2, core)
        else:
            source = dev((nc - 1, 1, 2)[(kind - 8) // 2], 1 - core)
        ag(kind, rows_of(ref, b, source), rows_of(ref, b, source), b, partner).wait_recv()

    def send_ring(b):
        for kind in (0, 3, 1, 2):
            own(kind, b).start()

    def send_partner(b):
        for kind in (4, 5):
            own(kind, b).start()

    def service_first(b):
        arrived(0, b)
        forward(6, b).start()
        forward(8, b).start()
        arrived(3, b)
        forward(7, b).start()
        forward(11, b).start()

    def service_second(b):
        arrived(2, b)
        forward(10, b).start()
        arrived(1, b)
        forward(9, b).start()

    def service_far(b):
        arrived(6, b)
        forward(12, b).start()
        arrived(7, b)
        forward(13, b).start()

    def rs(kind, src, dst, b, target):
        return pltpu.make_async_remote_copy(
            src_ref=src, dst_ref=dst, send_sem=rs_send.at[b, kind], recv_sem=rs_recv.at[b, kind],
            device_id={"tp": target}, device_id_type=MESH_ID)

    def part_rows(b, device, part):
        if part is None:
            return t_ref.at[b, pl.ds(row0(device), rows), :]
        return t_ref.at[b, pl.ds(pl.multiple_of(device * rows + part * half, half), half), :]

    def to_partner(b, j, off):
        return rs(j, part_rows(b, dev(off, 1 - core), None), p_ref.at[b, j], b, partner)

    def ring(kind, b):
        lo, hi = pl.ds(0, half), pl.ds(half, half)
        if kind == 4:
            return rs(kind, part_rows(b, dev(2, core), 0), hp_ref.at[b], b, plus)
        if kind == 5:
            return rs(kind, part_rows(b, dev(2, core), 1), hm_ref.at[b], b, minus)
        if kind == 6:
            return rs(kind, part_rows(b, plus, 1), fp_ref.at[b, hi, :], b, plus)
        if kind == 7:
            return rs(kind, part_rows(b, plus, 0), fp_ref.at[b, lo, :], b, plus)
        if kind == 8:
            return rs(kind, part_rows(b, minus, 0), fm_ref.at[b, lo, :], b, minus)
        return rs(kind, part_rows(b, minus, 1), fm_ref.at[b, hi, :], b, minus)

    def add_partner(b, j):
        off = SCATTER_ORDER[j] if isinstance(j, int) else pick(j, SCATTER_ORDER)
        target = dev(off, core)
        rs(j, part_rows(b, target, None), p_ref.at[b, j], b, partner).wait_recv()

        @pl.loop(0, rows, step=LN_ROWS)
        def _(i):
            at = pl.ds(pl.multiple_of(target * rows + i, LN_ROWS), LN_ROWS)
            t_ref[b, at, :] += p_ref[b, j, pl.ds(pl.multiple_of(i, LN_ROWS), LN_ROWS), :]

    def ring_after_partner(b, j):
        @pl.when(j == 0)
        def _():
            ring(4, b).start()
            ring(5, b).start()

        @pl.when(j == 1)
        def _():
            ring(6, b).start()

        @pl.when(j == 2)
        def _():
            ring(8, b).start()

    def add_half(b, device, part, ref):
        @pl.loop(0, half, step=LN_ROWS)
        def _(i):
            at = pl.ds(pl.multiple_of(device * rows + part * half + i, LN_ROWS), LN_ROWS)
            t_ref[b, at, :] += ref[b, pl.ds(pl.multiple_of(i, LN_ROWS), LN_ROWS), :]

    def ring_second(b):
        ring(4, b).wait_recv()
        add_half(b, plus, 0, hp_ref)
        ring(7, b).start()
        ring(5, b).wait_recv()
        add_half(b, minus, 1, hm_ref)
        ring(9, b).start()

    def unit(b, cc):
        r0 = pl.multiple_of(cc * pair, pair)
        at = pl.ds(r0, pair)

        for i in range(0, pair, LN_ROWS):
            sub = pl.ds(pl.multiple_of(r0 + i, LN_ROWS), LN_ROWS)
            xs = x_ref[b, sub, :].astype(F32)
            mu = jnp.mean(xs, axis=-1, keepdims=True)
            xc = xs - mu
            rstd = lax.rsqrt(jnp.mean(xc * xc, axis=-1, keepdims=True) + NORM_EPS)
            xh = xc * rstd
            mu_ref[b, sub, :] = mu
            rstd_ref[b, sub, :] = rstd
            a_ref[b, sub, :] = (xh * ln_ref[0:1, :] + ln_ref[1:2, :]).astype(BF16)
            m_ref[b, sub, :] = (xh * ln_ref[2:3, :] + ln_ref[3:4, :]).astype(BF16)

        a = a_ref[b, at, :]
        dy = dy_ref[b, at, :]
        cos = cos_ref[at, :]
        sin = sin_ref[at, :]
        qk = dot_nt(a, wq_ref[0:4 * hd, :]).astype(BF16).astype(F32)
        q = qk[:, 0:2 * hd]
        q_ref[b, at, :] = (q * cos + pltpu.roll(q, hd, 1) * sin).astype(BF16)
        k = qk[:, 2 * hd:]
        k2 = k * cos + pltpu.roll(k, hd, 1) * sin
        k_ref[b, at, :] = k2.astype(BF16)
        kt_ref[b, :, at] = k2.T.astype(BF16)
        v = dot_nt(a, wq_ref[4 * hd:6 * hd, :])
        v_ref[b, at, :] = v.astype(BF16)
        vt_ref[b, :, at] = v.T.astype(BF16)
        dc_ref[b, at, :] = dot_nt(dy, wo_ref[...]).astype(BF16)
        m = m_ref[b, at, :]
        for f in range(0, ff, BLK):
            h = dot_nn(m, wu_ref[:, f:f + BLK])
            du = dot_nt(dy, wd_ref[f:f + BLK, :])
            cdf = 0.5 * (1.0 + lax.erf(h * SQRT_HALF))
            pdf = jnp.exp2(h * h * (-0.5 * LOG2E)) * INV_SQRT_2PI
            u_ref[b, at, f:f + BLK] = (h * cdf).astype(BF16)
            dh_ref[b, at, f:f + BLK] = (du * (cdf + h * pdf)).astype(BF16)
        dh = dh_ref[b, at, :]
        mu = mu_ref[b, at, :]
        rstd = rstd_ref[b, at, :]
        for d in range(0, width, BLK):
            cols = slice(d, d + BLK)
            dm = dot_nt(dh, wu_ref[cols, :])
            xh = (x_ref[b, at, cols].astype(F32) - mu) * rstd
            t_ref[b, at, cols] = dm * ln_ref[2:3, cols]
            acc_ref[2, :, cols] += fold8(dm * xh)
            acc_ref[3, :, cols] += fold8(dm)

    def attention_head(b, h):
        lane = lax.broadcasted_iota(jnp.int32, (1, 2 * hd), 1)
        q_mask = lax.rem(lane // hh, 2) == h
        v_mask = (lane // hd) == h
        qm_ref[...] = jnp.where(q_mask, q_ref[b], jnp.zeros((), BF16))
        dcm_ref[...] = jnp.where(v_mask, dc_ref[b], jnp.zeros((), BF16))
        v_rows = pl.ds(pl.multiple_of(h * hd, hd), hd)
        k_lo = pl.ds(pl.multiple_of(h * hh, hh), hh)
        k_hi = pl.ds(pl.multiple_of(hd + h * hh, hh), hh)
        for qb in range(seq // BLK):
            qs = slice(qb * BLK, (qb + 1) * BLK)
            kl = (qb + 1) * BLK
            qm = qm_ref[qs, :]
            dcm = dcm_ref[qs, :]
            top = None
            for kb in range(qb + 1):
                ks = slice(kb * BLK, (kb + 1) * BLK)
                s = dot_nt(k_ref[b, ks, :], qm)
                if kb == qb:
                    key = lax.broadcasted_iota(jnp.int32, (BLK, BLK), 0)
                    query = lax.broadcasted_iota(jnp.int32, (BLK, BLK), 1)
                    s = jnp.where(key <= query, s, NEG_BIG)
                s_ref[ks, :] = s
                best = jnp.max(s.reshape(BLK // 8, 8, BLK), axis=0)
                top = best if top is None else jnp.maximum(top, best)
            top = jnp.max(top, axis=0, keepdims=True)
            total = jnp.zeros((8, BLK), F32)
            weighted = jnp.zeros((8, BLK), F32)
            for kb in range(qb + 1):
                ks = slice(kb * BLK, (kb + 1) * BLK)
                e = jnp.exp2((s_ref[ks, :] - top) * (scale * LOG2E))
                dpr = dot_nt(v_ref[b, ks, :], dcm)
                s_ref[ks, :] = e
                dp_ref[ks, :] = dpr
                total += fold8(e)
                weighted += fold8(e * dpr)
            inv = 1.0 / jnp.sum(total, axis=0, keepdims=True)
            mean_dp = jnp.sum(weighted, axis=0, keepdims=True) * inv
            for kb in range(qb + 1):
                ks = slice(kb * BLK, (kb + 1) * BLK)
                p = s_ref[ks, :] * inv
                pt_ref[ks, qs] = p.astype(BF16)
                ds_ref[ks, qs] = (p * (dp_ref[ks, :] - mean_dp) * scale).astype(BF16)
            c = dot_nn(vt_ref[b, v_rows, 0:kl], pt_ref[0:kl, qs])
            ct_ref[b, v_rows, qs] = c.astype(BF16)
            kt = jnp.concatenate([kt_ref[b, k_lo, 0:kl], kt_ref[b, k_hi, 0:kl]], axis=0)
            dq = dot_nn(kt, ds_ref[0:kl, qs])
            dqt_ref[k_lo, qs] = dq[0:hh]
            dqt_ref[k_hi, qs] = dq[hh:hd]
        for kb in range(seq // BLK):
            ks = slice(kb * BLK, (kb + 1) * BLK)
            dva_ref[ks, :] += dot_nn(pt_ref[ks, kb * BLK:], dcm_ref[kb * BLK:, :])
            dka_ref[ks, :] += dot_nn(ds_ref[ks, kb * BLK:], qm_ref[kb * BLK:, :])

    def attention_finish(b):
        @pl.loop(0, seq, step=BLK)
        def _(i):
            at = pl.ds(pl.multiple_of(i, BLK), BLK)
            cos = cos_ref[at, :]
            sin = sin_ref[at, :]
            dq = dqt_ref[:, at].T
            dqkv_ref[b, at, 0:2 * hd] = (dq * cos - pltpu.roll(dq, hd, 1) * sin).astype(BF16)
            dk = dka_ref[at, :]
            dqkv_ref[b, at, 2 * hd:4 * hd] = (dk * cos - pltpu.roll(dk, hd, 1) * sin).astype(BF16)
            dqkv_ref[b, at, 4 * hd:6 * hd] = dva_ref[at, :].astype(BF16)

    def input_grad(b, cc):
        at = pl.ds(pl.multiple_of(cc * pair, pair), pair)
        dqkv = dqkv_ref[b, at, :]
        mu = mu_ref[b, at, :]
        rstd = rstd_ref[b, at, :]
        for d in range(0, width, BLK):
            cols = slice(d, d + BLK)
            da = dot_nn(dqkv, wq_ref[:, cols])
            xh = (x_ref[b, at, cols].astype(F32) - mu) * rstd
            t_ref[b, at, cols] += da * ln_ref[0:1, cols]
            acc_ref[0, :, cols] += fold8(da * xh)
            acc_ref[1, :, cols] += fold8(da)

    def finish(b):
        for kind, ref in ((6, fp_ref), (7, fp_ref), (8, fm_ref), (9, fm_ref)):
            ring(kind, b).wait_recv()

        @pl.loop(0, rows, step=LN_ROWS, unroll=2)
        def _(i):
            at = pl.ds(pl.multiple_of(me * rows + i, LN_ROWS), LN_ROWS)
            sub = pl.ds(pl.multiple_of(i, LN_ROWS), LN_ROWS)
            t = t_ref[b, at, :] + fp_ref[b, sub, :] + fm_ref[b, sub, :]
            rstd = rstd_ref[b, at, :]
            xh = (x_ref[b, at, :].astype(F32) - mu_ref[b, at, :]) * rstd
            n = rstd * (t - jnp.mean(t, axis=-1, keepdims=True) - xh * jnp.mean(t * xh, axis=-1, keepdims=True))
            gi_ref[b, sub, :] = (dy_ref[b, at, :].astype(F32) + n).astype(BF16)

    send_ring(0)
    send_partner(0)
    send_partner(1)
    acc_ref[...] = jnp.zeros_like(acc_ref)
    for copy in loads[2:]:
        copy.wait()

    @pl.loop(0, batch)
    def _(b):
        @pl.loop(b * 2, nc + 1)
        def _(i):
            step = i - 1

            @pl.when(i == 0)
            def _():
                arrived(4, 0)
                arrived(5, 0)

            @pl.when((step == 0) & (b == 0))
            def _():
                arrived(4, 1)
                arrived(5, 1)

            @pl.when((step == 1) & (b == 0))
            def _():
                service_first(0)
                send_ring(1)
                service_second(0)

            @pl.when(step == 1)
            def _():
                arrived(10, b)
                arrived(11, b)

            @pl.when(step == 2)
            def _():
                arrived(8, b)
                arrived(9, b)

            @pl.when((step == 2) & (b == 1))
            def _():
                for j in range(1, nc):
                    add_partner(0, j)
                    ring_after_partner(0, j)

            @pl.when(step == 3)
            def _():
                service_far(b)
                arrived(12, b)
                arrived(13, b)

            unit(jnp.where(step == 0, 1, b), lax.rem(chip + pick(jnp.maximum(step, 0), GATHER_ORDER), nc))

        @pl.when(b == 0)
        def _():
            service_first(1)

        dka_ref[...] = jnp.zeros_like(dka_ref)
        dva_ref[...] = jnp.zeros_like(dva_ref)

        @pl.loop(0, 2)
        def _(h):
            attention_head(b, h)

            @pl.when((b == 1) & (h == 0))
            def _():
                ring_second(0)

        @pl.when(b == 0)
        def _():
            service_second(1)

        attention_finish(b)

        @pl.loop(0, nc + 1)
        def _(j):
            @pl.when(j < nc)
            def _():
                input_grad(b, lax.rem(chip + pick(j, SCATTER_ORDER + (0,)), nc))

            for jj in range(nc):
                @pl.when(j == jj)
                def _(jj=jj):
                    to_partner(b, jj, SCATTER_ORDER[jj]).start()

            @pl.when(((j > 0) & (b == 1)) | (j == nc))
            def _():
                which = jnp.where(b == 1, j - 1, 0)
                add_partner(b, which)
                ring_after_partner(b, which)

    for r in range(4):
        gls_ref[0, r:r + 1, :] = jnp.sum(acc_ref[r], axis=0, keepdims=True)

    def gl_copy(kind, src, dst, target):
        return pltpu.make_async_remote_copy(
            src_ref=src, dst_ref=dst, send_sem=gl_send.at[kind], recv_sem=gl_recv.at[kind],
            device_id={"tp": target}, device_id_type=MESH_ID)

    def from_chip(off):
        return gl_ref.at[lax.rem(chip + off, nc)]

    gl_pair = gl_copy(0, gls_ref.at[0], gls_ref.at[1], partner)
    gl_plus = gl_copy(1, from_chip(0), from_chip(0), plus)
    gl_minus = gl_copy(2, from_chip(0), from_chip(0), minus)
    gl_far = gl_copy(3, from_chip(nc - 1), from_chip(nc - 1), plus)
    gl_pair.start()

    @pl.loop(0, width, step=BLK)
    def _(i):
        cols = pl.ds(pl.multiple_of(i, BLK), BLK)
        total = dot_tn(m_ref[0, :, cols], dh_ref[0])
        for b in range(1, batch):
            total += dot_tn(m_ref[b, :, cols], dh_ref[b])
        gu_ref[cols, :] = total.astype(BF16)

    gl_pair.wait_recv()
    gl_ref[chip] = gls_ref[0] + gls_ref[1]
    gl_plus.start()
    gl_minus.start()

    @pl.loop(0, width, step=BLK)
    def _(i):
        cols = pl.ds(pl.multiple_of(i, BLK), BLK)
        total = dot_tn(u_ref[0], dy_ref[0, :, cols])
        for b in range(1, batch):
            total += dot_tn(u_ref[b], dy_ref[b, :, cols])
        gd_ref[:, cols] = total.astype(BF16)

    @pl.loop(0, width, step=BLK)
    def _(i):
        cols = pl.ds(pl.multiple_of(i, BLK), BLK)
        total = dot_tn(dqkv_ref[0], a_ref[0, :, cols])
        out = dot_nn(ct_ref[0], dy_ref[0, :, cols])
        for b in range(1, batch):
            total += dot_tn(dqkv_ref[b], a_ref[b, :, cols])
            out += dot_nn(ct_ref[b], dy_ref[b, :, cols])
        total = total.astype(BF16)
        for t, base in ((0, 0), (1, 2 * hd)):
            for part in range(2):
                for g in range(2):
                    row, to = base + part * hd + g * hh, g * 3 * hd + t * hd + part * hh
                    gq_ref[to:to + hh, cols] = total[row:row + hh]
        for g in range(2):
            row, to = 4 * hd + g * hd, g * 3 * hd + 2 * hd
            gq_ref[to:to + hd, cols] = total[row:row + hd]
        go_ref[:, cols] = out.astype(BF16)

    finish(0)
    ring_second(1)
    gl_copy(1, from_chip(nc - 1), from_chip(nc - 1), plus).wait_recv()
    gl_far.start()
    finish(1)

    gl_copy(2, from_chip(1), from_chip(1), minus).wait_recv()
    gl_copy(3, from_chip(2), from_chip(2), plus).wait_recv()
    total = gl_ref[0]
    for j in range(1, nc):
        total += gl_ref[j]
    gl_out[...] = total

    for b in range(batch):
        for kind in range(6):
            own(kind, b).wait_send()
        for kind in range(6, 14):
            forward(kind, b).wait_send()
        for j in range(nc):
            to_partner(b, j, SCATTER_ORDER[j]).wait_send()
        for kind in range(4, 10):
            ring(kind, b).wait_send()
    for copy in (gl_pair, gl_plus, gl_minus, gl_far):
        copy.wait_send()


def store_kernel(*refs):
    n = len(refs) // 2
    copies = [pltpu.make_async_copy(refs[i], refs[n + i], refs[2 * n].at[i]) for i in range(n)]
    for copy in copies:
        copy.start()
    for copy in copies:
        copy.wait()


def rope_tables(seq_len, head_dim):
    half_dim = head_dim // 2
    inv_freq = np.float32(ROPE_BASE) ** (np.float32(-2.0) * np.arange(half_dim, dtype=np.float32) / np.float32(head_dim))
    angles = np.arange(seq_len, dtype=np.float32)[:, None] * inv_freq[None, :]
    cos, sin = np.cos(angles), np.sin(angles)
    return jnp.asarray(np.concatenate([cos] * 4, axis=1)), jnp.asarray(np.concatenate([-sin, -sin, sin, sin], axis=1))


def solution(mesh):
    act_spec = P('dp', 'tp', None)
    nt = mesh.shape['tp']
    nc = nt // 2

    def device_step(layer_in, grad_out, w_qkv, w_out, w_up, w_down, ln_params):
        batch, rows, width = layer_in.shape
        seq = rows * nt
        groups, _, hd = w_qkv.shape[1:]
        ff = w_up.shape[1]
        wq = jnp.transpose(w_qkv, (1, 2, 3, 0)).reshape(groups * 3 * hd, width)
        wo = w_out.reshape(groups * hd, width)
        cos, sin = rope_tables(seq, hd)
        lanes = groups * hd
        any_spec = pl.BlockSpec(memory_space=pl.ANY)
        vmem_spec = pl.BlockSpec(memory_space=pltpu.VMEM)
        vm = pltpu.VMEM
        dma = pltpu.SemaphoreType.DMA
        shapes = (
            jax.ShapeDtypeStruct((batch, rows, width), BF16),
            jax.ShapeDtypeStruct((groups * 3 * hd, width), BF16),
            jax.ShapeDtypeStruct((lanes, width), BF16),
            jax.ShapeDtypeStruct((width, ff), BF16),
            jax.ShapeDtypeStruct((ff, width), BF16),
            jax.ShapeDtypeStruct((4, width), F32),
        )
        outs = pl.pallas_call(
            functools.partial(layer_kernel, nt),
            out_shape=tuple(vm(shape.shape, shape.dtype) for shape in shapes),
            in_specs=[any_spec] * 6 + [vmem_spec] + [any_spec] * 2,
            out_specs=(vmem_spec,) * 6,
            scratch_shapes=[
                vm((batch, seq, width), BF16), vm((batch, seq, width), BF16),
                vm((batch, seq, width), BF16), vm((batch, seq, width), BF16),
                vm((groups * 3 * hd, width), BF16), vm((lanes, width), BF16), vm((width, ff), BF16), vm((ff, width), BF16),
                vm((seq, lanes), F32), vm((seq, lanes), F32),
                vm((batch, seq, lanes), BF16), vm((batch, seq, lanes), BF16), vm((batch, seq, lanes), BF16), vm((batch, seq, lanes), BF16),
                vm((batch, lanes, seq), BF16), vm((batch, lanes, seq), BF16),
                vm((batch, seq, ff), BF16), vm((batch, seq, ff), BF16),
                vm((batch, seq, width), F32), vm((batch, nc, rows, width), F32),
                vm((batch, rows // 2, width), F32), vm((batch, rows // 2, width), F32),
                vm((batch, rows, width), F32), vm((batch, rows, width), F32),
                vm((batch, seq, 1), F32), vm((batch, seq, 1), F32),
                vm((seq, BLK), F32), vm((seq, BLK), F32), vm((seq, seq), BF16), vm((seq, seq), BF16),
                vm((seq, lanes), BF16), vm((seq, lanes), BF16), vm((seq, lanes), F32), vm((seq, lanes), F32),
                vm((lanes, seq), F32), vm((batch, seq, 3 * lanes), BF16), vm((batch, lanes, seq), BF16),
                vm((4, 8, width), F32), vm((nc, 4, width), F32), vm((2, 4, width), F32),
                dma((17,)), dma((batch, 14)), dma((batch, 14)), dma((batch, 10)), dma((batch, 10)), dma((4,)), dma((4,)),
            ],
            compiler_params=pltpu.CompilerParams(collective_id=0, has_side_effects=True, vmem_limit_bytes=VMEM_LIMIT),
            name="layer_backward",
        )(layer_in, grad_out, wq, wo, w_up, w_down, ln_params, cos, sin)
        outs = pl.pallas_call(
            store_kernel,
            out_shape=shapes,
            in_specs=[vmem_spec] * 6,
            out_specs=(any_spec,) * 6,
            scratch_shapes=[dma((6,))],
            compiler_params=pltpu.CompilerParams(vmem_limit_bytes=1 << 20),
            name="store_outputs",
        )(*(pltpu.with_memory_space_constraint(out, pltpu.VMEM) for out in outs))
        grad_in, gq, go, gu, gd, gl = outs
        gq = jnp.transpose(gq.reshape(groups, 3, hd, width), (3, 0, 1, 2))
        return grad_in, gq, go.reshape(w_out.shape), gu, gd, gl

    return jax.shard_map(
        device_step,
        mesh=mesh,
        in_specs=(act_spec, act_spec, P(None, 'tp', None, None), P('tp', None, None, None), P(None, 'tp'), P('tp', None), P(None, None)),
        out_specs=(act_spec, P('dp', 'tp', None, None), P(('dp', 'tp'), None, None, None), P('dp', 'tp'), P(('dp', 'tp'), None), P('dp', None)),
        check_vma=False,
    )
```

```python
import functools

import jax
import jax.numpy as jnp
import numpy as np
from jax import lax
from jax.experimental import pallas as pl
from jax.experimental.pallas import tpu as pltpu
from jax.sharding import PartitionSpec as P

NORM_EPS = 1e-5
ROPE_BASE = 10000.0
NEG_BIG = -1e30
LOG2E = 1.4426950408889634
SQRT_HALF = 0.7071067811865476
INV_SQRT_2PI = 0.3989422804014327
F32 = jnp.float32
BF16 = jnp.bfloat16
MESH_ID = pl.DeviceIdType.MESH
BLK = 256
LN_ROWS = 32
VMEM_LIMIT = 62000000
GATHER_ORDER = (0, 1, 3, 2)
SCATTER_ORDER = (2, 1, 3, 0)


def pick(index, values):
    out = values[-1]
    for i in range(len(values) - 2, -1, -1):
        out = jnp.where(index == i, values[i], out)
    return out


def dot_nn(lhs, rhs):
    return lax.dot_general(lhs, rhs, (((1,), (0,)), ((), ())), preferred_element_type=F32)


def dot_nt(lhs, rhs):
    return lax.dot_general(lhs, rhs, (((1,), (1,)), ((), ())), preferred_element_type=F32)


def dot_tn(lhs, rhs):
    return lax.dot_general(lhs, rhs, (((0,), (0,)), ((), ())), preferred_element_type=F32)


def fold8(value):
    rows, cols = value.shape
    return jnp.sum(value.reshape(rows // 8, 8, cols), axis=0)


def layer_kernel(nt, x_in, dy_in, wq_in, wo_in, wu_in, wd_in, ln_ref, cos_in, sin_in,
                 gi_ref, gq_ref, go_ref, gu_ref, gd_ref, gl_out,
                 x_ref, dy_ref, a_ref, m_ref, wq_ref, wo_ref, wu_ref, wd_ref, cos_ref, sin_ref,
                 q_ref, k_ref, v_ref, dc_ref, kt_ref, vt_ref, u_ref, dh_ref, t_ref, p_ref,
                 hp_ref, hm_ref, fp_ref, fm_ref, mu_ref, rstd_ref, s_ref, dp_ref, pt_ref, ds_ref,
                 qm_ref, dcm_ref, dka_ref, dva_ref, dqt_ref, dqkv_ref, ct_ref, acc_ref, gl_ref, gls_ref,
                 load_sem, ag_send, ag_recv, rs_send, rs_recv, gl_send, gl_recv):
    nc = nt // 2
    batch, seq, width = x_ref.shape
    ff = wu_ref.shape[1]
    rows = x_in.shape[1]
    half = rows // 2
    quarter = rows // 4
    pair = 2 * rows
    hd = wo_in.shape[0] // 2
    hh = hd // 2
    scale = hd ** -0.5

    me = lax.axis_index("tp")
    chip = me // 2
    core = lax.rem(me, 2)
    partner = chip * 2 + (1 - core)

    def dev(off, which):
        return lax.rem(chip + off, nc) * 2 + which

    plus = dev(1, core)
    minus = dev(nc - 1, core)

    def row0(device):
        return pl.multiple_of(device * rows, rows)

    loads = []

    def load(src, dst):
        loads.append(pltpu.make_async_copy(src, dst, load_sem.at[len(loads)]))
        loads[-1].start()

    barrier = pltpu.get_barrier_semaphore()
    for target in (plus, minus, partner):
        pl.semaphore_signal(barrier, inc=1, device_id={"tp": target}, device_id_type=MESH_ID)

    load(x_in, x_ref.at[:, pl.ds(row0(me), rows), :])
    load(dy_in, dy_ref.at[:, pl.ds(row0(me), rows), :])
    loads[0].wait()
    loads[1].wait()
    pl.semaphore_wait(barrier, 3)

    def ag(kind, src, dst, b, target):
        return pltpu.make_async_remote_copy(
            src_ref=src, dst_ref=dst, send_sem=ag_send.at[b, kind], recv_sem=ag_recv.at[b, kind],
            device_id={"tp": target}, device_id_type=MESH_ID)

    def rows_of(ref, b, device):
        return ref.at[b, pl.ds(row0(device), rows), :]

    def own(kind, b):
        ref = (x_ref, dy_ref)[kind % 2]
        target = (plus, minus, partner)[kind // 2]
        return ag(kind, rows_of(ref, b, me), rows_of(ref, b, me), b, target)

    def forward(kind, b):
        if kind == 6:
            return ag(kind, rows_of(x_ref, b, minus), rows_of(x_ref, b, minus), b, plus)
        if kind == 7:
            return ag(kind, rows_of(dy_ref, b, plus), rows_of(dy_ref, b, plus), b, minus)
        ref = (x_ref, dy_ref)[kind % 2]
        source = dev((nc - 1, 1, 2)[(kind - 8) // 2], core)
        return ag(kind, rows_of(ref, b, source), rows_of(ref, b, source), b, partner)

    def arrived(kind, b):
        ref = (x_ref, dy_ref)[kind % 2]
        if kind < 6:
            source = (minus, plus, partner)[kind // 2]
        elif kind < 8:
            source = dev(2, core)
        else:
            source = dev((nc - 1, 1, 2)[(kind - 8) // 2], 1 - core)
        ag(kind, rows_of(ref, b, source), rows_of(ref, b, source), b, partner).wait_recv()

    def send_ring(b):
        for kind in (0, 3, 1, 2):
            own(kind, b).start()

    def send_partner(b):
        for kind in (4, 5):
            own(kind, b).start()

    def service_first(b):
        arrived(0, b)
        forward(6, b).start()
        forward(8, b).start()
        arrived(3, b)
        forward(7, b).start()
        forward(11, b).start()

    def service_second(b):
        arrived(2, b)
        forward(10, b).start()
        arrived(1, b)
        forward(9, b).start()

    def service_far(b):
        arrived(6, b)
        forward(12, b).start()
        arrived(7, b)
        forward(13, b).start()

    def rs(kind, src, dst, b, target):
        return pltpu.make_async_remote_copy(
            src_ref=src, dst_ref=dst, send_sem=rs_send.at[b, kind], recv_sem=rs_recv.at[b, kind],
            device_id={"tp": target}, device_id_type=MESH_ID)

    def part_rows(b, device, first, count):
        return t_ref.at[b, pl.ds(pl.multiple_of(device * rows + first, quarter), count), :]

    def to_partner(b, j, off):
        return rs(j, part_rows(b, dev(off, 1 - core), 0, rows), p_ref.at[b, j], b, partner)

    def ring(kind, b):
        if kind < 6:
            to, ref = ((plus, hp_ref), (minus, hm_ref))[kind - 4]
            return rs(kind, part_rows(b, dev(2, core), (kind - 4) * half, half), ref.at[b], b, to)
        to, ref, first, count = {
            6: (plus, fp_ref, half, half), 7: (plus, fp_ref, 0, quarter), 10: (plus, fp_ref, quarter, quarter),
            8: (minus, fm_ref, 0, half), 9: (minus, fm_ref, half, quarter), 11: (minus, fm_ref, half + quarter, quarter),
        }[kind]
        return rs(kind, part_rows(b, to, first, count), ref.at[b, pl.ds(first, count), :], b, to)

    def add_partner(b, j):
        target = dev(SCATTER_ORDER[j], core)
        rs(j, part_rows(b, target, 0, rows), p_ref.at[b, j], b, partner).wait_recv()

        @pl.loop(0, rows, step=LN_ROWS)
        def _(i):
            at = pl.ds(pl.multiple_of(target * rows + i, LN_ROWS), LN_ROWS)
            t_ref[b, at, :] += p_ref[b, j, pl.ds(pl.multiple_of(i, LN_ROWS), LN_ROWS), :]

    def add_quarter(b, device, first, ref, at):
        t_ref[b, pl.ds(pl.multiple_of(device * rows + first, quarter), quarter), :] += ref[b, pl.ds(at, quarter), :]

    def ring_second(b):
        ring(4, b).wait_recv()
        add_quarter(b, plus, 0, hp_ref, 0)
        ring(7, b).start()
        ring(5, b).wait_recv()
        add_quarter(b, minus, half, hm_ref, 0)
        ring(9, b).start()
        add_quarter(b, plus, quarter, hp_ref, quarter)
        ring(10, b).start()
        add_quarter(b, minus, half + quarter, hm_ref, quarter)
        ring(11, b).start()

    def unit(b, cc):
        r0 = pl.multiple_of(cc * pair, pair)
        at = pl.ds(r0, pair)

        for i in range(0, pair, LN_ROWS):
            sub = pl.ds(pl.multiple_of(r0 + i, LN_ROWS), LN_ROWS)
            xs = x_ref[b, sub, :].astype(F32)
            mu = jnp.mean(xs, axis=-1, keepdims=True)
            xc = xs - mu
            rstd = lax.rsqrt(jnp.mean(xc * xc, axis=-1, keepdims=True) + NORM_EPS)
            xh = xc * rstd
            mu_ref[b, sub, :] = mu
            rstd_ref[b, sub, :] = rstd
            a_ref[b, sub, :] = (xh * ln_ref[0:1, :] + ln_ref[1:2, :]).astype(BF16)
            m_ref[b, sub, :] = (xh * ln_ref[2:3, :] + ln_ref[3:4, :]).astype(BF16)

        a = a_ref[b, at, :]
        dy = dy_ref[b, at, :]
        cos = cos_ref[at, :]
        sin = sin_ref[at, :]
        qk = dot_nt(a, wq_ref[0:4 * hd, :]).astype(BF16).astype(F32)
        q = qk[:, 0:2 * hd]
        q_ref[b, at, :] = (q * cos + pltpu.roll(q, hd, 1) * sin).astype(BF16)
        k = qk[:, 2 * hd:]
        k2 = k * cos + pltpu.roll(k, hd, 1) * sin
        k_ref[b, at, :] = k2.astype(BF16)
        kt_ref[b, :, at] = k2.T.astype(BF16)
        v = dot_nt(a, wq_ref[4 * hd:6 * hd, :])
        v_ref[b, at, :] = v.astype(BF16)
        vt_ref[b, :, at] = v.T.astype(BF16)
        dc_ref[b, at, :] = dot_nt(dy, wo_ref[...]).astype(BF16)
        m = m_ref[b, at, :]
        for f in range(0, ff, BLK):
            h = dot_nn(m, wu_ref[:, f:f + BLK])
            du = dot_nt(dy, wd_ref[f:f + BLK, :])
            cdf = 0.5 * (1.0 + lax.erf(h * SQRT_HALF))
            pdf = jnp.exp2(h * h * (-0.5 * LOG2E)) * INV_SQRT_2PI
            u_ref[b, at, f:f + BLK] = (h * cdf).astype(BF16)
            dh_ref[b, at, f:f + BLK] = (du * (cdf + h * pdf)).astype(BF16)
        dh = dh_ref[b, at, :]
        mu = mu_ref[b, at, :]
        rstd = rstd_ref[b, at, :]
        for d in range(0, width, BLK):
            cols = slice(d, d + BLK)
            dm = dot_nt(dh, wu_ref[cols, :])
            xh = (x_ref[b, at, cols].astype(F32) - mu) * rstd
            t_ref[b, at, cols] = dm * ln_ref[2:3, cols]
            acc_ref[2, :, cols] += fold8(dm * xh)
            acc_ref[3, :, cols] += fold8(dm)

    def attention_head(b, h):
        lane = lax.broadcasted_iota(jnp.int32, (1, 2 * hd), 1)
        q_mask = lax.rem(lane // hh, 2) == h
        v_mask = (lane // hd) == h
        qm_ref[...] = jnp.where(q_mask, q_ref[b], jnp.zeros((), BF16))
        dcm_ref[...] = jnp.where(v_mask, dc_ref[b], jnp.zeros((), BF16))
        v_rows = pl.ds(pl.multiple_of(h * hd, hd), hd)
        k_lo = pl.ds(pl.multiple_of(h * hh, hh), hh)
        k_hi = pl.ds(pl.multiple_of(hd + h * hh, hh), hh)
        for qb in range(seq // BLK):
            qs = slice(qb * BLK, (qb + 1) * BLK)
            kl = (qb + 1) * BLK
            qm = qm_ref[qs, :]
            dcm = dcm_ref[qs, :]
            top = None
            for kb in range(qb + 1):
                ks = slice(kb * BLK, (kb + 1) * BLK)
                s = dot_nt(k_ref[b, ks, :], qm)
                if kb == qb:
                    key = lax.broadcasted_iota(jnp.int32, (BLK, BLK), 0)
                    query = lax.broadcasted_iota(jnp.int32, (BLK, BLK), 1)
                    s = jnp.where(key <= query, s, NEG_BIG)
                s_ref[ks, :] = s
                best = jnp.max(s.reshape(BLK // 8, 8, BLK), axis=0)
                top = best if top is None else jnp.maximum(top, best)
            top = jnp.max(top, axis=0, keepdims=True)
            total = jnp.zeros((8, BLK), F32)
            weighted = jnp.zeros((8, BLK), F32)
            for kb in range(qb + 1):
                ks = slice(kb * BLK, (kb + 1) * BLK)
                e = jnp.exp2((s_ref[ks, :] - top) * (scale * LOG2E))
                dpr = dot_nt(v_ref[b, ks, :], dcm)
                s_ref[ks, :] = e
                dp_ref[ks, :] = dpr
                total += fold8(e)
                weighted += fold8(e * dpr)
            inv = 1.0 / jnp.sum(total, axis=0, keepdims=True)
            mean_dp = jnp.sum(weighted, axis=0, keepdims=True) * inv
            for kb in range(qb + 1):
                ks = slice(kb * BLK, (kb + 1) * BLK)
                p = s_ref[ks, :] * inv
                pt_ref[ks, qs] = p.astype(BF16)
                ds_ref[ks, qs] = (p * (dp_ref[ks, :] - mean_dp) * scale).astype(BF16)
            c = dot_nn(vt_ref[b, v_rows, 0:kl], pt_ref[0:kl, qs])
            ct_ref[b, v_rows, qs] = c.astype(BF16)
            kt = jnp.concatenate([kt_ref[b, k_lo, 0:kl], kt_ref[b, k_hi, 0:kl]], axis=0)
            dq = dot_nn(kt, ds_ref[0:kl, qs])
            dqt_ref[k_lo, qs] = dq[0:hh]
            dqt_ref[k_hi, qs] = dq[hh:hd]
        for kb in range(seq // BLK):
            ks = slice(kb * BLK, (kb + 1) * BLK)
            dva_ref[ks, :] += dot_nn(pt_ref[ks, kb * BLK:], dcm_ref[kb * BLK:, :])
            dka_ref[ks, :] += dot_nn(ds_ref[ks, kb * BLK:], qm_ref[kb * BLK:, :])

    def input_grad(b, cc):
        at = pl.ds(pl.multiple_of(cc * pair, pair), pair)
        cos = cos_ref[at, :]
        sin = sin_ref[at, :]
        dq = dqt_ref[:, at].T
        dqkv_ref[b, at, 0:2 * hd] = (dq * cos - pltpu.roll(dq, hd, 1) * sin).astype(BF16)
        dk = dka_ref[at, :]
        dqkv_ref[b, at, 2 * hd:4 * hd] = (dk * cos - pltpu.roll(dk, hd, 1) * sin).astype(BF16)
        dqkv_ref[b, at, 4 * hd:6 * hd] = dva_ref[at, :].astype(BF16)
        dqkv = dqkv_ref[b, at, :]
        mu = mu_ref[b, at, :]
        rstd = rstd_ref[b, at, :]
        for d in range(0, width, BLK):
            cols = slice(d, d + BLK)
            da = dot_nn(dqkv, wq_ref[:, cols])
            xh = (x_ref[b, at, cols].astype(F32) - mu) * rstd
            t_ref[b, at, cols] += da * ln_ref[0:1, cols]
            acc_ref[0, :, cols] += fold8(da * xh)
            acc_ref[1, :, cols] += fold8(da)

    def finish_rows(b, first):
        at = pl.ds(pl.multiple_of(me * rows + first, quarter), quarter)
        sub = pl.ds(first, quarter)
        t = t_ref[b, at, :] + fp_ref[b, sub, :] + fm_ref[b, sub, :]
        rstd = rstd_ref[b, at, :]
        xh = (x_ref[b, at, :].astype(F32) - mu_ref[b, at, :]) * rstd
        n = rstd * (t - jnp.mean(t, axis=-1, keepdims=True) - xh * jnp.mean(t * xh, axis=-1, keepdims=True))
        gi_ref[b, sub, :] = (dy_ref[b, at, :].astype(F32) + n).astype(BF16)

    def finish(b):
        for kind in (6, 8, 7, 9):
            ring(kind, b).wait_recv()
        finish_rows(b, 0)
        finish_rows(b, half)
        for kind in (10, 11):
            ring(kind, b).wait_recv()
        finish_rows(b, quarter)
        finish_rows(b, half + quarter)

    def gl_copy(kind, src, dst, target):
        return pltpu.make_async_remote_copy(
            src_ref=src, dst_ref=dst, send_sem=gl_send.at[kind], recv_sem=gl_recv.at[kind],
            device_id={"tp": target}, device_id_type=MESH_ID)

    def from_chip(off):
        return gl_ref.at[lax.rem(chip + off, nc)]

    gl_pair = gl_copy(0, gls_ref.at[0], gls_ref.at[1], partner)
    gl_plus = gl_copy(1, from_chip(0), from_chip(0), plus)
    gl_minus = gl_copy(2, from_chip(0), from_chip(0), minus)
    gl_far = gl_copy(3, from_chip(nc - 1), from_chip(nc - 1), plus)

    send_ring(0)
    send_partner(0)
    send_partner(1)

    for t, base in ((0, 0), (1, 2 * hd)):
        for part in range(2):
            for g in range(2):
                load(wq_in.at[pl.ds(g * 3 * hd + t * hd + part * hh, hh), :],
                     wq_ref.at[pl.ds(base + part * hd + g * hh, hh), :])
    for g in range(2):
        load(wq_in.at[pl.ds(g * 3 * hd + 2 * hd, hd), :], wq_ref.at[pl.ds(4 * hd + g * hd, hd), :])
    load(cos_in, cos_ref)
    load(sin_in, sin_ref)
    load(wo_in, wo_ref)
    load(wu_in, wu_ref)
    load(wd_in, wd_ref)

    acc_ref[...] = jnp.zeros_like(acc_ref)
    for copy in loads[2:]:
        copy.wait()

    @pl.loop(0, batch)
    def _(b):
        @pl.loop(b * 2, nc + 1)
        def _(i):
            step = i - 1

            @pl.when(i == 0)
            def _():
                arrived(4, 0)
                arrived(5, 0)

            @pl.when((step == 0) & (b == 0))
            def _():
                arrived(4, 1)
                arrived(5, 1)

            @pl.when((step == 1) & (b == 0))
            def _():
                service_first(0)
                send_ring(1)
                service_second(0)

            @pl.when(step == 1)
            def _():
                arrived(10, b)
                arrived(11, b)

            @pl.when(step == 2)
            def _():
                arrived(8, b)
                arrived(9, b)

            @pl.when((step == 2) & (b == 1))
            def _():
                add_partner(0, 1)
                ring(6, 0).start()
                add_partner(0, 2)
                ring(8, 0).start()
                add_partner(0, 3)

            @pl.when(step == 3)
            def _():
                service_far(b)
                arrived(12, b)
                arrived(13, b)

            unit(jnp.where(step == 0, 1, b), lax.rem(chip + pick(jnp.maximum(step, 0), GATHER_ORDER), nc))

        @pl.when(b == 0)
        def _():
            service_first(1)

        @pl.when(b == 1)
        def _():
            ring_second(0)

        dka_ref[...] = jnp.zeros_like(dka_ref)
        dva_ref[...] = jnp.zeros_like(dva_ref)

        @pl.loop(0, 2)
        def _(h):
            attention_head(b, h)

        @pl.when(b == 0)
        def _():
            service_second(1)

        @pl.loop(0, nc)
        def _(j):
            input_grad(b, lax.rem(chip + pick(j, SCATTER_ORDER), nc))
            for jj in range(nc):
                @pl.when(j == jj)
                def _(jj=jj):
                    to_partner(b, jj, SCATTER_ORDER[jj]).start()

            @pl.when(j == 3 - b)
            def _():
                add_partner(b, 0)
                ring(4, b).start()
                ring(5, b).start()

    for r in range(4):
        gls_ref[0, r:r + 1, :] = jnp.sum(acc_ref[r], axis=0, keepdims=True)
    gl_pair.start()
    add_partner(1, 1)
    add_partner(1, 2)
    gl_pair.wait_recv()
    gl_ref[chip] = gls_ref[0] + gls_ref[1]
    gl_plus.start()
    gl_minus.start()
    ring(6, 1).start()
    ring(8, 1).start()
    add_partner(1, 3)

    @pl.loop(0, width, step=BLK)
    def _(i):
        cols = pl.ds(pl.multiple_of(i, BLK), BLK)
        total = dot_tn(m_ref[0, :, cols], dh_ref[0])
        for b in range(1, batch):
            total += dot_tn(m_ref[b, :, cols], dh_ref[b])
        gu_ref[cols, :] = total.astype(BF16)


    @pl.loop(0, width, step=BLK)
    def _(i):
        cols = pl.ds(pl.multiple_of(i, BLK), BLK)
        total = dot_tn(u_ref[0], dy_ref[0, :, cols])
        for b in range(1, batch):
            total += dot_tn(u_ref[b], dy_ref[b, :, cols])
        gd_ref[:, cols] = total.astype(BF16)

    gl_copy(1, from_chip(nc - 1), from_chip(nc - 1), plus).wait_recv()
    gl_far.start()
    ring_second(1)

    @pl.loop(0, width, step=BLK)
    def _(i):
        cols = pl.ds(pl.multiple_of(i, BLK), BLK)
        total = dot_tn(dqkv_ref[0], a_ref[0, :, cols])
        out = dot_nn(ct_ref[0], dy_ref[0, :, cols])
        for b in range(1, batch):
            total += dot_tn(dqkv_ref[b], a_ref[b, :, cols])
            out += dot_nn(ct_ref[b], dy_ref[b, :, cols])
        total = total.astype(BF16)
        for t, base in ((0, 0), (1, 2 * hd)):
            for part in range(2):
                for g in range(2):
                    row, to = base + part * hd + g * hh, g * 3 * hd + t * hd + part * hh
                    gq_ref[to:to + hh, cols] = total[row:row + hh]
        for g in range(2):
            row, to = 4 * hd + g * hd, g * 3 * hd + 2 * hd
            gq_ref[to:to + hd, cols] = total[row:row + hd]
        go_ref[:, cols] = out.astype(BF16)

    finish(0)
    gl_copy(2, from_chip(1), from_chip(1), minus).wait_recv()
    gl_copy(3, from_chip(2), from_chip(2), plus).wait_recv()
    total = gl_ref[0]
    for j in range(1, nc):
        total += gl_ref[j]
    gl_out[...] = total

    for b in range(batch):
        for kind in range(6):
            own(kind, b).wait_send()
        for kind in range(6, 14):
            forward(kind, b).wait_send()
        for j in range(nc):
            to_partner(b, j, SCATTER_ORDER[j]).wait_send()
    for kind in range(4, 12):
        ring(kind, 0).wait_send()
    for kind in (4, 5, 6, 8):
        ring(kind, 1).wait_send()
    for copy in (gl_pair, gl_plus, gl_minus, gl_far):
        copy.wait_send()
    finish(1)
    for kind in (7, 9, 10, 11):
        ring(kind, 1).wait_send()


def store_kernel(*refs):
    n = len(refs) // 2
    copies = [pltpu.make_async_copy(refs[i], refs[n + i], refs[2 * n].at[i]) for i in range(n)]
    for copy in copies:
        copy.start()
    for copy in copies:
        copy.wait()


def rope_tables(seq_len, head_dim):
    half_dim = head_dim // 2
    inv_freq = np.float32(ROPE_BASE) ** (np.float32(-2.0) * np.arange(half_dim, dtype=np.float32) / np.float32(head_dim))
    angles = np.arange(seq_len, dtype=np.float32)[:, None] * inv_freq[None, :]
    cos, sin = np.cos(angles), np.sin(angles)
    return jnp.asarray(np.concatenate([cos] * 4, axis=1)), jnp.asarray(np.concatenate([-sin, -sin, sin, sin], axis=1))


def solution(mesh):
    act_spec = P('dp', 'tp', None)
    nt = mesh.shape['tp']
    nc = nt // 2

    def device_step(layer_in, grad_out, w_qkv, w_out, w_up, w_down, ln_params):
        batch, rows, width = layer_in.shape
        seq = rows * nt
        groups, _, hd = w_qkv.shape[1:]
        ff = w_up.shape[1]
        wq = jnp.transpose(w_qkv, (1, 2, 3, 0)).reshape(groups * 3 * hd, width)
        wo = w_out.reshape(groups * hd, width)
        cos, sin = rope_tables(seq, hd)
        lanes = groups * hd
        any_spec = pl.BlockSpec(memory_space=pl.ANY)
        vmem_spec = pl.BlockSpec(memory_space=pltpu.VMEM)
        vm = pltpu.VMEM
        dma = pltpu.SemaphoreType.DMA
        shapes = (
            jax.ShapeDtypeStruct((batch, rows, width), BF16),
            jax.ShapeDtypeStruct((groups * 3 * hd, width), BF16),
            jax.ShapeDtypeStruct((lanes, width), BF16),
            jax.ShapeDtypeStruct((width, ff), BF16),
            jax.ShapeDtypeStruct((ff, width), BF16),
            jax.ShapeDtypeStruct((4, width), F32),
        )
        outs = pl.pallas_call(
            functools.partial(layer_kernel, nt),
            out_shape=tuple(vm(shape.shape, shape.dtype) for shape in shapes),
            in_specs=[any_spec] * 6 + [vmem_spec] + [any_spec] * 2,
            out_specs=(vmem_spec,) * 6,
            scratch_shapes=[
                vm((batch, seq, width), BF16), vm((batch, seq, width), BF16),
                vm((batch, seq, width), BF16), vm((batch, seq, width), BF16),
                vm((groups * 3 * hd, width), BF16), vm((lanes, width), BF16), vm((width, ff), BF16), vm((ff, width), BF16),
                vm((seq, lanes), F32), vm((seq, lanes), F32),
                vm((batch, seq, lanes), BF16), vm((batch, seq, lanes), BF16), vm((batch, seq, lanes), BF16), vm((batch, seq, lanes), BF16),
                vm((batch, lanes, seq), BF16), vm((batch, lanes, seq), BF16),
                vm((batch, seq, ff), BF16), vm((batch, seq, ff), BF16),
                vm((batch, seq, width), F32), vm((batch, nc, rows, width), F32),
                vm((batch, rows // 2, width), F32), vm((batch, rows // 2, width), F32),
                vm((batch, rows, width), F32), vm((batch, rows, width), F32),
                vm((batch, seq, 1), F32), vm((batch, seq, 1), F32),
                vm((seq, BLK), F32), vm((seq, BLK), F32), vm((seq, seq), BF16), vm((seq, seq), BF16),
                vm((seq, lanes), BF16), vm((seq, lanes), BF16), vm((seq, lanes), F32), vm((seq, lanes), F32),
                vm((lanes, seq), F32), vm((batch, seq, 3 * lanes), BF16), vm((batch, lanes, seq), BF16),
                vm((4, 8, width), F32), vm((nc, 4, width), F32), vm((2, 4, width), F32),
                dma((17,)), dma((batch, 14)), dma((batch, 14)), dma((batch, 12)), dma((batch, 12)), dma((4,)), dma((4,)),
            ],
            compiler_params=pltpu.CompilerParams(collective_id=0, has_side_effects=True, vmem_limit_bytes=VMEM_LIMIT),
            name="layer_backward",
        )(layer_in, grad_out, wq, wo, w_up, w_down, ln_params, cos, sin)
        outs = pl.pallas_call(
            store_kernel,
            out_shape=shapes,
            in_specs=[vmem_spec] * 6,
            out_specs=(any_spec,) * 6,
            scratch_shapes=[dma((6,))],
            compiler_params=pltpu.CompilerParams(vmem_limit_bytes=1 << 20),
            name="store_outputs",
        )(*(pltpu.with_memory_space_constraint(out, pltpu.VMEM) for out in outs))
        grad_in, gq, go, gu, gd, gl = outs
        gq = jnp.transpose(gq.reshape(groups, 3, hd, width), (3, 0, 1, 2))
        return grad_in, gq, go.reshape(w_out.shape), gu, gd, gl

    return jax.shard_map(
        device_step,
        mesh=mesh,
        in_specs=(act_spec, act_spec, P(None, 'tp', None, None), P('tp', None, None, None), P(None, 'tp'), P('tp', None), P(None, None)),
        out_specs=(act_spec, P('dp', 'tp', None, None), P(('dp', 'tp'), None, None, None), P('dp', 'tp'), P(('dp', 'tp'), None), P('dp', None)),
        check_vma=False,
    )
```

```python
import functools

import jax
import jax.numpy as jnp
import numpy as np
from jax import lax
from jax.experimental import pallas as pl
from jax.experimental.pallas import tpu as pltpu
from jax.sharding import PartitionSpec as P

NORM_EPS = 1e-5
ROPE_BASE = 10000.0
NEG_BIG = -1e30
LOG2E = 1.4426950408889634
SQRT_HALF = 0.7071067811865476
INV_SQRT_2PI = 0.3989422804014327
F32 = jnp.float32
BF16 = jnp.bfloat16
MESH_ID = pl.DeviceIdType.MESH
BLK = 256
LN_ROWS = 32
VMEM_LIMIT = 62000000
GATHER_ORDER = (0, 1, 3, 2)
SCATTER_ORDER = (2, 1, 3, 0)


def pick(index, values):
    out = values[-1]
    for i in range(len(values) - 2, -1, -1):
        out = jnp.where(index == i, values[i], out)
    return out


def dot_nn(lhs, rhs):
    return lax.dot_general(lhs, rhs, (((1,), (0,)), ((), ())), preferred_element_type=F32)


def dot_nt(lhs, rhs):
    return lax.dot_general(lhs, rhs, (((1,), (1,)), ((), ())), preferred_element_type=F32)


def dot_tn(lhs, rhs):
    return lax.dot_general(lhs, rhs, (((0,), (0,)), ((), ())), preferred_element_type=F32)


def fold8(value):
    rows, cols = value.shape
    return jnp.sum(value.reshape(rows // 8, 8, cols), axis=0)


def layer_kernel(nt, x_in, dy_in, wq_in, wo_in, wu_in, wd_in, ln_ref, cos_in, sin_in,
                 gi_ref, gq_ref, go_ref, gu_ref, gd_ref, gl_out,
                 x_ref, dy_ref, a_ref, m_ref, wq_ref, wo_ref, wu_ref, wd_ref, cos_ref, sin_ref,
                 q_ref, k_ref, v_ref, dc_ref, kt_ref, vt_ref, u_ref, dh_ref, t_ref, p_ref,
                 hp_ref, hm_ref, fp_ref, fm_ref, mu_ref, rstd_ref, s_ref, dp_ref, pt_ref, ds_ref,
                 qm_ref, dcm_ref, dka_ref, dva_ref, dqt_ref, dqkv_ref, ct_ref, acc_ref, gl_ref, gls_ref,
                 load_sem, ag_send, ag_recv, rs_send, rs_recv, gl_send, gl_recv):
    nc = nt // 2
    batch, seq, width = x_ref.shape
    ff = wu_ref.shape[1]
    rows = x_in.shape[1]
    half = rows // 2
    quarter = rows // 4
    pair = 2 * rows
    hd = wo_in.shape[0] // 2
    hh = hd // 2
    scale = hd ** -0.5

    me = lax.axis_index("tp")
    chip = me // 2
    core = lax.rem(me, 2)
    partner = chip * 2 + (1 - core)

    def dev(off, which):
        return lax.rem(chip + off, nc) * 2 + which

    plus = dev(1, core)
    minus = dev(nc - 1, core)

    def row0(device):
        return pl.multiple_of(device * rows, rows)

    loads = []

    def load(src, dst):
        loads.append(pltpu.make_async_copy(src, dst, load_sem.at[len(loads)]))
        loads[-1].start()

    def load_piece(first, count, to):
        pltpu.make_async_copy(wq_in.at[pl.ds(first, count), :], wq_ref.at[pl.ds(to, count), :], load_sem.at[2]).start()

    barrier = pltpu.get_barrier_semaphore()
    for target in (plus, minus, partner):
        pl.semaphore_signal(barrier, inc=1, device_id={"tp": target}, device_id_type=MESH_ID)

    load(x_in, x_ref.at[:, pl.ds(row0(me), rows), :])
    load(dy_in, dy_ref.at[:, pl.ds(row0(me), rows), :])
    loads[0].wait()
    loads[1].wait()
    pl.semaphore_wait(barrier, 3)

    def ag(kind, src, dst, b, target):
        return pltpu.make_async_remote_copy(
            src_ref=src, dst_ref=dst, send_sem=ag_send.at[b, kind], recv_sem=ag_recv.at[b, kind],
            device_id={"tp": target}, device_id_type=MESH_ID)

    def rows_of(ref, b, device):
        return ref.at[b, pl.ds(row0(device), rows), :]

    def own(kind, b):
        ref = (x_ref, dy_ref)[kind % 2]
        target = (plus, minus, partner)[kind // 2]
        return ag(kind, rows_of(ref, b, me), rows_of(ref, b, me), b, target)

    def forward(kind, b):
        if kind == 6:
            return ag(kind, rows_of(x_ref, b, minus), rows_of(x_ref, b, minus), b, plus)
        if kind == 7:
            return ag(kind, rows_of(dy_ref, b, plus), rows_of(dy_ref, b, plus), b, minus)
        ref = (x_ref, dy_ref)[kind % 2]
        source = dev((nc - 1, 1, 2)[(kind - 8) // 2], core)
        return ag(kind, rows_of(ref, b, source), rows_of(ref, b, source), b, partner)

    def arrived(kind, b):
        ref = (x_ref, dy_ref)[kind % 2]
        if kind < 6:
            source = (minus, plus, partner)[kind // 2]
        elif kind < 8:
            source = dev(2, core)
        else:
            source = dev((nc - 1, 1, 2)[(kind - 8) // 2], 1 - core)
        ag(kind, rows_of(ref, b, source), rows_of(ref, b, source), b, partner).wait_recv()

    def send_ring(b):
        for kind in (0, 3, 1, 2):
            own(kind, b).start()

    def send_partner(b):
        for kind in (4, 5):
            own(kind, b).start()

    def service_first(b):
        arrived(0, b)
        forward(6, b).start()
        forward(8, b).start()
        arrived(3, b)
        forward(7, b).start()
        forward(11, b).start()

    def service_second(b):
        arrived(2, b)
        forward(10, b).start()
        arrived(1, b)
        forward(9, b).start()

    def service_far(b):
        arrived(6, b)
        forward(12, b).start()
        arrived(7, b)
        forward(13, b).start()

    def rs(kind, src, dst, b, target):
        return pltpu.make_async_remote_copy(
            src_ref=src, dst_ref=dst, send_sem=rs_send.at[b, kind], recv_sem=rs_recv.at[b, kind],
            device_id={"tp": target}, device_id_type=MESH_ID)

    def part_rows(b, device, first, count):
        return t_ref.at[b, pl.ds(pl.multiple_of(device * rows + first, quarter), count), :]

    def to_partner(b, j, off):
        return rs(j, part_rows(b, dev(off, 1 - core), 0, rows), p_ref.at[b, j], b, partner)

    def ring(kind, b):
        if kind < 6:
            to, ref = ((plus, hp_ref), (minus, hm_ref))[kind - 4]
            return rs(kind, part_rows(b, dev(2, core), (kind - 4) * half, half), ref.at[b], b, to)
        to, ref, first, count = {
            6: (plus, fp_ref, half, half), 7: (plus, fp_ref, 0, quarter), 10: (plus, fp_ref, quarter, quarter),
            8: (minus, fm_ref, 0, half), 9: (minus, fm_ref, half, quarter), 11: (minus, fm_ref, half + quarter, quarter),
        }[kind]
        return rs(kind, part_rows(b, to, first, count), ref.at[b, pl.ds(first, count), :], b, to)

    def add_partner(b, j):
        target = dev(SCATTER_ORDER[j], core)
        rs(j, part_rows(b, target, 0, rows), p_ref.at[b, j], b, partner).wait_recv()

        @pl.loop(0, rows, step=LN_ROWS)
        def _(i):
            at = pl.ds(pl.multiple_of(target * rows + i, LN_ROWS), LN_ROWS)
            t_ref[b, at, :] += p_ref[b, j, pl.ds(pl.multiple_of(i, LN_ROWS), LN_ROWS), :]

    def add_quarter(b, device, first, ref, at):
        t_ref[b, pl.ds(pl.multiple_of(device * rows + first, quarter), quarter), :] += ref[b, pl.ds(at, quarter), :]

    def ring_second(b):
        ring(4, b).wait_recv()
        add_quarter(b, plus, 0, hp_ref, 0)
        ring(7, b).start()
        ring(5, b).wait_recv()
        add_quarter(b, minus, half, hm_ref, 0)
        ring(9, b).start()
        add_quarter(b, plus, quarter, hp_ref, quarter)
        ring(10, b).start()
        add_quarter(b, minus, half + quarter, hm_ref, quarter)
        ring(11, b).start()

    def unit(b, cc):
        r0 = pl.multiple_of(cc * pair, pair)
        at = pl.ds(r0, pair)

        for i in range(0, pair, LN_ROWS):
            sub = pl.ds(pl.multiple_of(r0 + i, LN_ROWS), LN_ROWS)
            xs = x_ref[b, sub, :].astype(F32)
            mu = jnp.mean(xs, axis=-1, keepdims=True)
            xc = xs - mu
            rstd = lax.rsqrt(jnp.mean(xc * xc, axis=-1, keepdims=True) + NORM_EPS)
            xh = xc * rstd
            mu_ref[b, sub, :] = mu
            rstd_ref[b, sub, :] = rstd
            a_ref[b, sub, :] = (xh * ln_ref[0:1, :] + ln_ref[1:2, :]).astype(BF16)
            m_ref[b, sub, :] = (xh * ln_ref[2:3, :] + ln_ref[3:4, :]).astype(BF16)

        a = a_ref[b, at, :]
        dy = dy_ref[b, at, :]
        cos = cos_ref[at, :]
        sin = sin_ref[at, :]
        qk = dot_nt(a, wq_ref[0:4 * hd, :]).astype(BF16).astype(F32)
        q = qk[:, 0:2 * hd]
        q_ref[b, at, :] = (q * cos + pltpu.roll(q, hd, 1) * sin).astype(BF16)
        k = qk[:, 2 * hd:]
        k2 = k * cos + pltpu.roll(k, hd, 1) * sin
        k_ref[b, at, :] = k2.astype(BF16)
        kt_ref[b, :, at] = k2.T.astype(BF16)
        v = dot_nt(a, wq_ref[4 * hd:6 * hd, :])
        v_ref[b, at, :] = v.astype(BF16)
        vt_ref[b, :, at] = v.T.astype(BF16)
        dc_ref[b, at, :] = dot_nt(dy, wo_ref[...]).astype(BF16)
        m = m_ref[b, at, :]
        for f in range(0, ff, BLK):
            h = dot_nn(m, wu_ref[:, f:f + BLK])
            du = dot_nt(dy, wd_ref[f:f + BLK, :])
            cdf = 0.5 * (1.0 + lax.erf(h * SQRT_HALF))
            pdf = jnp.exp2(h * h * (-0.5 * LOG2E)) * INV_SQRT_2PI
            u_ref[b, at, f:f + BLK] = (h * cdf).astype(BF16)
            dh_ref[b, at, f:f + BLK] = (du * (cdf + h * pdf)).astype(BF16)
        dh = dh_ref[b, at, :]
        mu = mu_ref[b, at, :]
        rstd = rstd_ref[b, at, :]
        for d in range(0, width, BLK):
            cols = slice(d, d + BLK)
            dm = dot_nt(dh, wu_ref[cols, :])
            xh = (x_ref[b, at, cols].astype(F32) - mu) * rstd
            t_ref[b, at, cols] = dm * ln_ref[2:3, cols]
            acc_ref[2, :, cols] += fold8(dm * xh)
            acc_ref[3, :, cols] += fold8(dm)

    def attention_head(b, h):
        lane = lax.broadcasted_iota(jnp.int32, (1, 2 * hd), 1)
        q_mask = lax.rem(lane // hh, 2) == h
        v_mask = (lane // hd) == h
        qm_ref[...] = jnp.where(q_mask, q_ref[b], jnp.zeros((), BF16))
        dcm_ref[...] = jnp.where(v_mask, dc_ref[b], jnp.zeros((), BF16))
        v_rows = pl.ds(pl.multiple_of(h * hd, hd), hd)
        k_lo = pl.ds(pl.multiple_of(h * hh, hh), hh)
        k_hi = pl.ds(pl.multiple_of(hd + h * hh, hh), hh)
        for qb in range(seq // BLK):
            qs = slice(qb * BLK, (qb + 1) * BLK)
            kl = (qb + 1) * BLK
            qm = qm_ref[qs, :]
            dcm = dcm_ref[qs, :]
            top = None
            for kb in range(qb + 1):
                ks = slice(kb * BLK, (kb + 1) * BLK)
                s = dot_nt(k_ref[b, ks, :], qm)
                if kb == qb:
                    key = lax.broadcasted_iota(jnp.int32, (BLK, BLK), 0)
                    query = lax.broadcasted_iota(jnp.int32, (BLK, BLK), 1)
                    s = jnp.where(key <= query, s, NEG_BIG)
                s_ref[ks, :] = s
                best = jnp.max(s.reshape(BLK // 8, 8, BLK), axis=0)
                top = best if top is None else jnp.maximum(top, best)
            top = jnp.max(top, axis=0, keepdims=True)
            total = jnp.zeros((8, BLK), F32)
            weighted = jnp.zeros((8, BLK), F32)
            for kb in range(qb + 1):
                ks = slice(kb * BLK, (kb + 1) * BLK)
                e = jnp.exp2((s_ref[ks, :] - top) * (scale * LOG2E))
                dpr = dot_nt(v_ref[b, ks, :], dcm)
                s_ref[ks, :] = e
                dp_ref[ks, :] = dpr
                total += fold8(e)
                weighted += fold8(e * dpr)
            inv = 1.0 / jnp.sum(total, axis=0, keepdims=True)
            mean_dp = jnp.sum(weighted, axis=0, keepdims=True) * inv
            for kb in range(qb + 1):
                ks = slice(kb * BLK, (kb + 1) * BLK)
                p = s_ref[ks, :] * inv
                pt_ref[ks, qs] = p.astype(BF16)
                ds_ref[ks, qs] = (p * (dp_ref[ks, :] - mean_dp) * scale).astype(BF16)
            c = dot_nn(vt_ref[b, v_rows, 0:kl], pt_ref[0:kl, qs])
            ct_ref[b, v_rows, qs] = c.astype(BF16)
            kt = jnp.concatenate([kt_ref[b, k_lo, 0:kl], kt_ref[b, k_hi, 0:kl]], axis=0)
            dq = dot_nn(kt, ds_ref[0:kl, qs])
            dqt_ref[k_lo, qs] = dq[0:hh]
            dqt_ref[k_hi, qs] = dq[hh:hd]
        for kb in range(seq // BLK):
            ks = slice(kb * BLK, (kb + 1) * BLK)
            dva_ref[ks, :] += dot_nn(pt_ref[ks, kb * BLK:], dcm_ref[kb * BLK:, :])
            dka_ref[ks, :] += dot_nn(ds_ref[ks, kb * BLK:], qm_ref[kb * BLK:, :])

    def input_grad(b, cc):
        at = pl.ds(pl.multiple_of(cc * pair, pair), pair)
        cos = cos_ref[at, :]
        sin = sin_ref[at, :]
        dq = dqt_ref[:, at].T
        dqkv_ref[b, at, 0:2 * hd] = (dq * cos - pltpu.roll(dq, hd, 1) * sin).astype(BF16)
        dk = dka_ref[at, :]
        dqkv_ref[b, at, 2 * hd:4 * hd] = (dk * cos - pltpu.roll(dk, hd, 1) * sin).astype(BF16)
        dqkv_ref[b, at, 4 * hd:6 * hd] = dva_ref[at, :].astype(BF16)
        dqkv = dqkv_ref[b, at, :]
        mu = mu_ref[b, at, :]
        rstd = rstd_ref[b, at, :]
        for d in range(0, width, BLK):
            cols = slice(d, d + BLK)
            da = dot_nn(dqkv, wq_ref[:, cols])
            xh = (x_ref[b, at, cols].astype(F32) - mu) * rstd
            t_ref[b, at, cols] += da * ln_ref[0:1, cols]
            acc_ref[0, :, cols] += fold8(da * xh)
            acc_ref[1, :, cols] += fold8(da)

    def finish_rows(b, first):
        at = pl.ds(pl.multiple_of(me * rows + first, quarter), quarter)
        sub = pl.ds(first, quarter)
        t = t_ref[b, at, :] + fp_ref[b, sub, :] + fm_ref[b, sub, :]
        rstd = rstd_ref[b, at, :]
        xh = (x_ref[b, at, :].astype(F32) - mu_ref[b, at, :]) * rstd
        n = rstd * (t - jnp.mean(t, axis=-1, keepdims=True) - xh * jnp.mean(t * xh, axis=-1, keepdims=True))
        gi_ref[b, sub, :] = (dy_ref[b, at, :].astype(F32) + n).astype(BF16)

    def finish(b):
        for kind in (6, 8, 7, 9):
            ring(kind, b).wait_recv()
        finish_rows(b, 0)
        finish_rows(b, half)
        for kind in (10, 11):
            ring(kind, b).wait_recv()
        finish_rows(b, quarter)
        finish_rows(b, half + quarter)

    def gl_copy(kind, src, dst, target):
        return pltpu.make_async_remote_copy(
            src_ref=src, dst_ref=dst, send_sem=gl_send.at[kind], recv_sem=gl_recv.at[kind],
            device_id={"tp": target}, device_id_type=MESH_ID)

    def from_chip(off):
        return gl_ref.at[lax.rem(chip + off, nc)]

    gl_pair = gl_copy(0, gls_ref.at[0], gls_ref.at[1], partner)
    gl_plus = gl_copy(1, from_chip(0), from_chip(0), plus)
    gl_minus = gl_copy(2, from_chip(0), from_chip(0), minus)
    gl_far = gl_copy(3, from_chip(nc - 1), from_chip(nc - 1), plus)

    send_ring(0)
    send_partner(0)
    send_partner(1)

    for t, base in ((0, 0), (1, 2 * hd)):
        for part in range(2):
            for g in range(2):
                load_piece(g * 3 * hd + t * hd + part * hh, hh, base + part * hd + g * hh)
    for g in range(2):
        load_piece(g * 3 * hd + 2 * hd, hd, 4 * hd + g * hd)
    loads.append(pltpu.make_async_copy(wq_in, wq_ref, load_sem.at[2]))
    load(cos_in, cos_ref)
    load(sin_in, sin_ref)
    load(wo_in, wo_ref)
    load(wu_in, wu_ref)
    load(wd_in, wd_ref)

    acc_ref[...] = jnp.zeros_like(acc_ref)
    for copy in loads[2:]:
        copy.wait()

    @pl.loop(0, batch)
    def _(b):
        @pl.loop(b * 2, nc + 1)
        def _(i):
            step = i - 1

            @pl.when(i == 0)
            def _():
                arrived(4, 0)
                arrived(5, 0)

            @pl.when((step == 0) & (b == 0))
            def _():
                arrived(4, 1)
                arrived(5, 1)

            @pl.when((step == 1) & (b == 0))
            def _():
                service_first(0)
                send_ring(1)
                service_second(0)

            @pl.when((step == 2) & (b == 1))
            def _():
                add_partner(0, 1)
                ring(6, 0).start()
                add_partner(0, 2)
                ring(8, 0).start()

            @pl.when(step == 1)
            def _():
                arrived(10, b)
                arrived(11, b)

            @pl.when(step == 2)
            def _():
                arrived(8, b)
                arrived(9, b)

            @pl.when(step == 3 - b)
            def _():
                service_far(b)

            @pl.when(step == 3)
            def _():
                arrived(12, b)
                arrived(13, b)

            unit(jnp.where(step == 0, 1, b), lax.rem(chip + pick(jnp.maximum(step, 0), GATHER_ORDER), nc))

        @pl.when(b == 1)
        def _():
            ring_second(0)

        dka_ref[...] = jnp.zeros_like(dka_ref)
        dva_ref[...] = jnp.zeros_like(dva_ref)

        @pl.loop(0, 2)
        def _(h):
            attention_head(b, h)

            @pl.when((b == 0) & (h == 0))
            def _():
                service_first(1)

        @pl.loop(0, nc)
        def _(j):
            input_grad(b, lax.rem(chip + pick(j, SCATTER_ORDER), nc))
            for jj in range(nc):
                @pl.when(j == jj)
                def _(jj=jj):
                    to_partner(b, jj, SCATTER_ORDER[jj]).start()

            @pl.when((b == 0) & (j == 1))
            def _():
                service_second(1)

            @pl.when(j == 3 - b)
            def _():
                add_partner(b, 0)
                ring(4, b).start()
                ring(5, b).start()

    for r in range(4):
        gls_ref[0, r:r + 1, :] = jnp.sum(acc_ref[r], axis=0, keepdims=True)
    gl_pair.start()
    add_partner(1, 1)
    add_partner(1, 2)
    gl_pair.wait_recv()
    gl_ref[chip] = gls_ref[0] + gls_ref[1]
    gl_plus.start()
    gl_minus.start()
    ring(6, 1).start()
    ring(8, 1).start()
    @pl.loop(0, width, step=BLK)
    def _(i):
        cols = pl.ds(pl.multiple_of(i, BLK), BLK)
        total = dot_tn(m_ref[0, :, cols], dh_ref[0])
        for b in range(1, batch):
            total += dot_tn(m_ref[b, :, cols], dh_ref[b])
        gu_ref[cols, :] = total.astype(BF16)


    @pl.loop(0, width, step=BLK)
    def _(i):
        cols = pl.ds(pl.multiple_of(i, BLK), BLK)
        total = dot_tn(u_ref[0], dy_ref[0, :, cols])
        for b in range(1, batch):
            total += dot_tn(u_ref[b], dy_ref[b, :, cols])
        gd_ref[:, cols] = total.astype(BF16)

    gl_copy(1, from_chip(nc - 1), from_chip(nc - 1), plus).wait_recv()
    gl_far.start()
    ring_second(1)

    @pl.loop(0, width, step=BLK)
    def _(i):
        cols = pl.ds(pl.multiple_of(i, BLK), BLK)
        total = dot_tn(dqkv_ref[0], a_ref[0, :, cols])
        out = dot_nn(ct_ref[0], dy_ref[0, :, cols])
        for b in range(1, batch):
            total += dot_tn(dqkv_ref[b], a_ref[b, :, cols])
            out += dot_nn(ct_ref[b], dy_ref[b, :, cols])
        total = total.astype(BF16)
        for t, base in ((0, 0), (1, 2 * hd)):
            for part in range(2):
                for g in range(2):
                    row, to = base + part * hd + g * hh, g * 3 * hd + t * hd + part * hh
                    gq_ref[to:to + hh, cols] = total[row:row + hh]
        for g in range(2):
            row, to = 4 * hd + g * hd, g * 3 * hd + 2 * hd
            gq_ref[to:to + hd, cols] = total[row:row + hd]
        go_ref[:, cols] = out.astype(BF16)

    add_partner(0, 3)
    add_partner(1, 3)
    finish(0)
    gl_copy(2, from_chip(1), from_chip(1), minus).wait_recv()
    gl_copy(3, from_chip(2), from_chip(2), plus).wait_recv()
    total = gl_ref[0]
    for j in range(1, nc):
        total += gl_ref[j]
    gl_out[...] = total

    for b in range(batch):
        for kind in range(6):
            own(kind, b).wait_send()
        for kind in range(6, 14):
            forward(kind, b).wait_send()
        for j in range(nc):
            to_partner(b, j, SCATTER_ORDER[j]).wait_send()
    for kind in range(4, 12):
        ring(kind, 0).wait_send()
    for kind in (4, 5, 6, 8):
        ring(kind, 1).wait_send()
    for copy in (gl_pair, gl_plus, gl_minus, gl_far):
        copy.wait_send()
    finish(1)
    for kind in (7, 9, 10, 11):
        ring(kind, 1).wait_send()


def store_kernel(*refs):
    n = len(refs) // 2
    copies = [pltpu.make_async_copy(refs[i], refs[n + i], refs[2 * n].at[i]) for i in range(n)]
    for copy in copies:
        copy.start()
    for copy in copies:
        copy.wait()


def rope_tables(seq_len, head_dim):
    half_dim = head_dim // 2
    inv_freq = np.float32(ROPE_BASE) ** (np.float32(-2.0) * np.arange(half_dim, dtype=np.float32) / np.float32(head_dim))
    angles = np.arange(seq_len, dtype=np.float32)[:, None] * inv_freq[None, :]
    cos, sin = np.cos(angles), np.sin(angles)
    return jnp.asarray(np.concatenate([cos] * 4, axis=1)), jnp.asarray(np.concatenate([-sin, -sin, sin, sin], axis=1))


def solution(mesh):
    act_spec = P('dp', 'tp', None)
    nt = mesh.shape['tp']
    nc = nt // 2

    def device_step(layer_in, grad_out, w_qkv, w_out, w_up, w_down, ln_params):
        batch, rows, width = layer_in.shape
        seq = rows * nt
        groups, _, hd = w_qkv.shape[1:]
        ff = w_up.shape[1]
        wq = jnp.transpose(w_qkv, (1, 2, 3, 0)).reshape(groups * 3 * hd, width)
        wo = w_out.reshape(groups * hd, width)
        cos, sin = rope_tables(seq, hd)
        lanes = groups * hd
        any_spec = pl.BlockSpec(memory_space=pl.ANY)
        vmem_spec = pl.BlockSpec(memory_space=pltpu.VMEM)
        vm = pltpu.VMEM
        dma = pltpu.SemaphoreType.DMA
        shapes = (
            jax.ShapeDtypeStruct((batch, rows, width), BF16),
            jax.ShapeDtypeStruct((groups * 3 * hd, width), BF16),
            jax.ShapeDtypeStruct((lanes, width), BF16),
            jax.ShapeDtypeStruct((width, ff), BF16),
            jax.ShapeDtypeStruct((ff, width), BF16),
            jax.ShapeDtypeStruct((4, width), F32),
        )
        outs = pl.pallas_call(
            functools.partial(layer_kernel, nt),
            out_shape=tuple(vm(shape.shape, shape.dtype) for shape in shapes),
            in_specs=[any_spec] * 6 + [vmem_spec] + [any_spec] * 2,
            out_specs=(vmem_spec,) * 6,
            scratch_shapes=[
                vm((batch, seq, width), BF16), vm((batch, seq, width), BF16),
                vm((batch, seq, width), BF16), vm((batch, seq, width), BF16),
                vm((groups * 3 * hd, width), BF16), vm((lanes, width), BF16), vm((width, ff), BF16), vm((ff, width), BF16),
                vm((seq, lanes), F32), vm((seq, lanes), F32),
                vm((batch, seq, lanes), BF16), vm((batch, seq, lanes), BF16), vm((batch, seq, lanes), BF16), vm((batch, seq, lanes), BF16),
                vm((batch, lanes, seq), BF16), vm((batch, lanes, seq), BF16),
                vm((batch, seq, ff), BF16), vm((batch, seq, ff), BF16),
                vm((batch, seq, width), F32), vm((batch, nc, rows, width), F32),
                vm((batch, rows // 2, width), F32), vm((batch, rows // 2, width), F32),
                vm((batch, rows, width), F32), vm((batch, rows, width), F32),
                vm((batch, seq, 1), F32), vm((batch, seq, 1), F32),
                vm((seq, BLK), F32), vm((seq, BLK), F32), vm((seq, seq), BF16), vm((seq, seq), BF16),
                vm((seq, lanes), BF16), vm((seq, lanes), BF16), vm((seq, lanes), F32), vm((seq, lanes), F32),
                vm((lanes, seq), F32), vm((batch, seq, 3 * lanes), BF16), vm((batch, lanes, seq), BF16),
                vm((4, 8, width), F32), vm((nc, 4, width), F32), vm((2, 4, width), F32),
                dma((8,)), dma((batch, 14)), dma((batch, 14)), dma((batch, 12)), dma((batch, 12)), dma((4,)), dma((4,)),
            ],
            compiler_params=pltpu.CompilerParams(collective_id=0, has_side_effects=True, vmem_limit_bytes=VMEM_LIMIT),
            name="layer_backward",
        )(layer_in, grad_out, wq, wo, w_up, w_down, ln_params, cos, sin)
        outs = pl.pallas_call(
            store_kernel,
            out_shape=shapes,
            in_specs=[vmem_spec] * 6,
            out_specs=(any_spec,) * 6,
            scratch_shapes=[dma((6,))],
            compiler_params=pltpu.CompilerParams(vmem_limit_bytes=1 << 20),
            name="store_outputs",
        )(*(pltpu.with_memory_space_constraint(out, pltpu.VMEM) for out in outs))
        grad_in, gq, go, gu, gd, gl = outs
        gq = jnp.transpose(gq.reshape(groups, 3, hd, width), (3, 0, 1, 2))
        return grad_in, gq, go.reshape(w_out.shape), gu, gd, gl

    return jax.shard_map(
        device_step,
        mesh=mesh,
        in_specs=(act_spec, act_spec, P(None, 'tp', None, None), P('tp', None, None, None), P(None, 'tp'), P('tp', None), P(None, None)),
        out_specs=(act_spec, P('dp', 'tp', None, None), P(('dp', 'tp'), None, None, None), P('dp', 'tp'), P(('dp', 'tp'), None), P('dp', None)),
        check_vma=False,
    )
```

```python
import functools

import jax
import jax.numpy as jnp
import numpy as np
from jax import lax
from jax.experimental import pallas as pl
from jax.experimental.pallas import tpu as pltpu
from jax.sharding import PartitionSpec as P

NORM_EPS = 1e-5
ROPE_BASE = 10000.0
NEG_BIG = -1e30
LOG2E = 1.4426950408889634
SQRT_HALF = 0.7071067811865476
INV_SQRT_2PI = 0.3989422804014327
F32 = jnp.float32
BF16 = jnp.bfloat16
MESH_ID = pl.DeviceIdType.MESH
BLK = 256
LN_ROWS = 32
STORE_PARTS = 1
KEY_BLK = 128
VMEM_LIMIT = 62000000
GATHER_ORDER = (0, 1, 3, 2)
SCATTER_ORDER = (2, 1, 3, 0)


def pick(index, values):
    out = values[-1]
    for i in range(len(values) - 2, -1, -1):
        out = jnp.where(index == i, values[i], out)
    return out


def dot_nn(lhs, rhs):
    return lax.dot_general(lhs, rhs, (((1,), (0,)), ((), ())), preferred_element_type=F32)


def dot_nt(lhs, rhs):
    return lax.dot_general(lhs, rhs, (((1,), (1,)), ((), ())), preferred_element_type=F32)


def dot_tn(lhs, rhs):
    return lax.dot_general(lhs, rhs, (((0,), (0,)), ((), ())), preferred_element_type=F32)


def fold8(value):
    rows, cols = value.shape
    return jnp.sum(value.reshape(rows // 8, 8, cols), axis=0)


def layer_kernel(nt, x_in, dy_in, wq_in, wo_in, wu_in, wd_in, ln_in, cos_in, sin_in,
                 gi_ref, gq_ref, go_ref, gu_ref, gd_ref, gl_out,
                 x_ref, dy_ref, a_ref, m_ref, wq_ref, wo_ref, wu_ref, wd_ref, cos_ref, sin_ref,
                 q_ref, k_ref, v_ref, dc_ref, kt_ref, vt_ref, u_ref, dh_ref, t_ref, p_ref,
                 hp_ref, hm_ref, fp_ref, fm_ref, mu_ref, rstd_ref, s_ref, dp_ref, pt_ref, ds_ref,
                 qm_ref, dcm_ref, dka_ref, dva_ref, dqt_ref, dqkv_ref, ct_ref, acc_ref, gl_ref, gls_ref,
                 ln_ref, load_sem, ag_send, ag_recv, rs_send, rs_recv, gl_send, gl_recv):
    nc = nt // 2
    batch, seq, width = x_ref.shape
    ff = wu_ref.shape[1]
    rows = x_in.shape[1]
    half = rows // 2
    quarter = rows // 4
    pair = 2 * rows
    hd = wo_in.shape[0] // 2
    hh = hd // 2
    scale = hd ** -0.5

    me = lax.axis_index("tp")
    chip = me // 2
    core = lax.rem(me, 2)
    partner = chip * 2 + (1 - core)

    def dev(off, which):
        return lax.rem(chip + off, nc) * 2 + which

    plus = dev(1, core)
    minus = dev(nc - 1, core)

    def row0(device):
        return pl.multiple_of(device * rows, rows)

    loads = []

    def load(src, dst):
        loads.append(pltpu.make_async_copy(src, dst, load_sem.at[len(loads)]))
        loads[-1].start()

    def load_piece(first, count, to):
        pltpu.make_async_copy(wq_in.at[pl.ds(first, count), :], wq_ref.at[pl.ds(to, count), :], load_sem.at[2]).start()

    load(x_in, x_ref.at[:, pl.ds(row0(me), rows), :])
    load(dy_in, dy_ref.at[:, pl.ds(row0(me), rows), :])

    barrier = pltpu.get_barrier_semaphore()
    for target in (plus, minus, partner):
        pl.semaphore_signal(barrier, inc=1, device_id={"tp": target}, device_id_type=MESH_ID)

    loads[0].wait()
    loads[1].wait()
    pl.semaphore_wait(barrier, 3)

    def ag(kind, src, dst, b, target):
        send = ag_send.at[b * 6 + kind] if kind < 6 else ag_send.at[6 + kind]
        return pltpu.make_async_remote_copy(
            src_ref=src, dst_ref=dst, send_sem=send, recv_sem=ag_recv.at[b, kind],
            device_id={"tp": target}, device_id_type=MESH_ID)

    def rows_of(ref, b, device):
        return ref.at[b, pl.ds(row0(device), rows), :]

    def own(kind, b):
        ref = (x_ref, dy_ref)[kind % 2]
        target = (plus, minus, partner)[kind // 2]
        return ag(kind, rows_of(ref, b, me), rows_of(ref, b, me), b, target)

    def forward(kind, b):
        if kind == 6:
            return ag(kind, rows_of(x_ref, b, minus), rows_of(x_ref, b, minus), b, plus)
        if kind == 7:
            return ag(kind, rows_of(dy_ref, b, plus), rows_of(dy_ref, b, plus), b, minus)
        ref = (x_ref, dy_ref)[kind % 2]
        source = dev((nc - 1, 1, 2)[(kind - 8) // 2], core)
        return ag(kind, rows_of(ref, b, source), rows_of(ref, b, source), b, partner)

    def arrived(kind, b):
        ref = (x_ref, dy_ref)[kind % 2]
        if kind < 6:
            source = (minus, plus, partner)[kind // 2]
        elif kind < 8:
            source = dev(2, core)
        else:
            source = dev((nc - 1, 1, 2)[(kind - 8) // 2], 1 - core)
        ag(kind, rows_of(ref, b, source), rows_of(ref, b, source), b, partner).wait_recv()

    def send_ring(b):
        for kind in (0, 3, 1, 2):
            own(kind, b).start()

    def send_partner(b):
        for kind in (4, 5):
            own(kind, b).start()

    def service_first(b):
        if b == 1:
            for kind in range(6, 14):
                forward(kind, 0).wait_send()
        arrived(0, b)
        forward(6, b).start()
        forward(8, b).start()
        arrived(3, b)
        forward(7, b).start()
        forward(11, b).start()

    def service_second(b):
        arrived(2, b)
        forward(10, b).start()
        arrived(1, b)
        forward(9, b).start()

    def service_far(b):
        arrived(6, b)
        forward(12, b).start()
        arrived(7, b)
        forward(13, b).start()

    def rs(kind, src, dst, b, target):
        return pltpu.make_async_remote_copy(
            src_ref=src, dst_ref=dst, send_sem=rs_send.at[kind], recv_sem=rs_recv.at[b, kind],
            device_id={"tp": target}, device_id_type=MESH_ID)

    def part_rows(b, device, first, count):
        return t_ref.at[b, pl.ds(pl.multiple_of(device * rows + first, quarter), count), :]

    def to_partner(b, j, off):
        return rs(j, part_rows(b, dev(off, 1 - core), 0, rows), p_ref.at[b, j], b, partner)

    def ring(kind, b):
        if kind < 6:
            to, ref = ((plus, hp_ref), (minus, hm_ref))[kind - 4]
            return rs(kind, part_rows(b, dev(2, core), (kind - 4) * half, half), ref.at[b], b, to)
        to, ref, first, count = {
            6: (plus, fp_ref, half, half), 7: (plus, fp_ref, 0, quarter), 10: (plus, fp_ref, quarter, quarter),
            8: (minus, fm_ref, 0, half), 9: (minus, fm_ref, half, quarter), 11: (minus, fm_ref, half + quarter, quarter),
        }[kind]
        return rs(kind, part_rows(b, to, first, count), ref.at[b, pl.ds(first, count), :], b, to)

    def add_partner(b, j):
        target = dev(SCATTER_ORDER[j], core)
        rs(j, part_rows(b, target, 0, rows), p_ref.at[b, j], b, partner).wait_recv()

        @pl.loop(0, rows, step=LN_ROWS)
        def _(i):
            at = pl.ds(pl.multiple_of(target * rows + i, LN_ROWS), LN_ROWS)
            t_ref[b, at, :] += p_ref[b, j, pl.ds(pl.multiple_of(i, LN_ROWS), LN_ROWS), :]

    def add_quarter(b, device, first, ref, at):
        t_ref[b, pl.ds(pl.multiple_of(device * rows + first, quarter), quarter), :] += ref[b, pl.ds(at, quarter), :]

    def ring_second(b):
        ring(4, b).wait_recv()
        add_quarter(b, plus, 0, hp_ref, 0)
        ring(7, b).start()
        ring(5, b).wait_recv()
        add_quarter(b, minus, half, hm_ref, 0)
        ring(9, b).start()
        add_quarter(b, plus, quarter, hp_ref, quarter)
        ring(10, b).start()
        add_quarter(b, minus, half + quarter, hm_ref, quarter)
        ring(11, b).start()

    def unit(b, cc):
        r0 = pl.multiple_of(cc * pair, pair)
        at = pl.ds(r0, pair)

        for i in range(0, pair, LN_ROWS):
            sub = pl.ds(pl.multiple_of(r0 + i, LN_ROWS), LN_ROWS)
            xs = x_ref[b, sub, :].astype(F32)
            mu = jnp.mean(xs, axis=-1, keepdims=True)
            xc = xs - mu
            rstd = lax.rsqrt(jnp.mean(xc * xc, axis=-1, keepdims=True) + NORM_EPS)
            xh = xc * rstd
            mu_ref[b, sub, :] = mu
            rstd_ref[b, sub, :] = rstd
            a_ref[b, sub, :] = (xh * ln_ref[0:1, :] + ln_ref[1:2, :]).astype(BF16)
            m_ref[b, sub, :] = (xh * ln_ref[2:3, :] + ln_ref[3:4, :]).astype(BF16)

        a = a_ref[b, at, :]
        dy = dy_ref[b, at, :]
        cos = cos_ref[at, :]
        sin = sin_ref[at, :]
        qk = dot_nt(a, wq_ref[0:4 * hd, :]).astype(BF16).astype(F32)
        q = qk[:, 0:2 * hd]
        q_ref[b, at, :] = (q * cos + pltpu.roll(q, hd, 1) * sin).astype(BF16)
        k = qk[:, 2 * hd:]
        k2 = k * cos + pltpu.roll(k, hd, 1) * sin
        k_ref[b, at, :] = k2.astype(BF16)
        kt_ref[b, :, at] = k2.T.astype(BF16)
        v = dot_nt(a, wq_ref[4 * hd:6 * hd, :])
        v_ref[b, at, :] = v.astype(BF16)
        vt_ref[b, :, at] = v.T.astype(BF16)
        dc_ref[b, at, :] = dot_nt(dy, wo_ref[...]).astype(BF16)
        m = m_ref[b, at, :]
        for f in range(0, ff, BLK):
            h = dot_nn(m, wu_ref[:, f:f + BLK])
            du = dot_nt(dy, wd_ref[f:f + BLK, :])
            cdf = 0.5 * (1.0 + lax.erf(h * SQRT_HALF))
            pdf = jnp.exp2(h * h * (-0.5 * LOG2E)) * INV_SQRT_2PI
            u_ref[b, at, f:f + BLK] = (h * cdf).astype(BF16)
            dh_ref[b, at, f:f + BLK] = (du * (cdf + h * pdf)).astype(BF16)
        dh = dh_ref[b, at, :]
        mu = mu_ref[b, at, :]
        rstd = rstd_ref[b, at, :]
        for d in range(0, width, BLK):
            cols = slice(d, d + BLK)
            dm = dot_nt(dh, wu_ref[cols, :])
            xh = (x_ref[b, at, cols].astype(F32) - mu) * rstd
            t_ref[b, at, cols] = dm * ln_ref[2:3, cols]
            acc_ref[2, :, cols] += fold8(dm * xh)
            acc_ref[3, :, cols] += fold8(dm)

    def attention_head(b, h):
        lane = lax.broadcasted_iota(jnp.int32, (1, 2 * hd), 1)
        q_mask = lax.rem(lane // hh, 2) == h
        v_mask = (lane // hd) == h
        qm_ref[...] = jnp.where(q_mask, q_ref[b], jnp.zeros((), BF16))
        dcm_ref[...] = jnp.where(v_mask, dc_ref[b], jnp.zeros((), BF16))
        v_rows = pl.ds(pl.multiple_of(h * hd, hd), hd)
        k_lo = pl.ds(pl.multiple_of(h * hh, hh), hh)
        k_hi = pl.ds(pl.multiple_of(hd + h * hh, hh), hh)
        for qb in range(seq // BLK):
            qs = slice(qb * BLK, (qb + 1) * BLK)
            kl = (qb + 1) * BLK
            qm = qm_ref[qs, :]
            dcm = dcm_ref[qs, :]
            top = None
            for kb in range(0, kl, KEY_BLK):
                ks = slice(kb, kb + KEY_BLK)
                s = dot_nt(k_ref[b, ks, :], qm)
                if kb >= qb * BLK:
                    key = lax.broadcasted_iota(jnp.int32, (KEY_BLK, BLK), 0) + (kb - qb * BLK)
                    query = lax.broadcasted_iota(jnp.int32, (KEY_BLK, BLK), 1)
                    s = jnp.where(key <= query, s, NEG_BIG / scale)
                s_ref[ks, :] = s
                best = jnp.max(s.reshape(KEY_BLK // 8, 8, BLK), axis=0)
                top = best if top is None else jnp.maximum(top, best)
            top = jnp.max(top, axis=0, keepdims=True)
            total = jnp.zeros((8, BLK), F32)
            weighted = jnp.zeros((8, BLK), F32)
            for kb in range(0, kl, KEY_BLK):
                ks = slice(kb, kb + KEY_BLK)
                e = jnp.exp2((s_ref[ks, :] - top) * (scale * LOG2E))
                dpr = dot_nt(v_ref[b, ks, :], dcm)
                s_ref[ks, :] = e
                dp_ref[ks, :] = dpr
                total += fold8(e)
                weighted += fold8(e * dpr)
            inv = 1.0 / jnp.sum(total, axis=0, keepdims=True)
            mean_dp = jnp.sum(weighted, axis=0, keepdims=True) * inv
            for kb in range(0, kl, KEY_BLK):
                ks = slice(kb, kb + KEY_BLK)
                p = s_ref[ks, :] * inv
                pt_ref[ks, qs] = p.astype(BF16)
                ds_ref[ks, qs] = (p * (dp_ref[ks, :] - mean_dp) * scale).astype(BF16)
            c = dot_nn(vt_ref[b, v_rows, 0:kl], pt_ref[0:kl, qs])
            ct_ref[b, v_rows, qs] = c.astype(BF16)
            kt = jnp.concatenate([kt_ref[b, k_lo, 0:kl], kt_ref[b, k_hi, 0:kl]], axis=0)
            dq = dot_nn(kt, ds_ref[0:kl, qs])
            dqt_ref[k_lo, qs] = dq[0:hh]
            dqt_ref[k_hi, qs] = dq[hh:hd]
        for kb in range(seq // BLK):
            ks = slice(kb * BLK, (kb + 1) * BLK)
            dva_ref[ks, :] += dot_nn(pt_ref[ks, kb * BLK:], dcm_ref[kb * BLK:, :])
            dka_ref[ks, :] += dot_nn(ds_ref[ks, kb * BLK:], qm_ref[kb * BLK:, :])

    def input_grad(b, cc):
        at = pl.ds(pl.multiple_of(cc * pair, pair), pair)
        cos = cos_ref[at, :]
        sin = sin_ref[at, :]
        dq = dqt_ref[:, at].T
        dqkv_ref[b, at, 0:2 * hd] = (dq * cos - pltpu.roll(dq, hd, 1) * sin).astype(BF16)
        dk = dka_ref[at, :]
        dqkv_ref[b, at, 2 * hd:4 * hd] = (dk * cos - pltpu.roll(dk, hd, 1) * sin).astype(BF16)
        dqkv_ref[b, at, 4 * hd:6 * hd] = dva_ref[at, :].astype(BF16)
        dqkv = dqkv_ref[b, at, :]
        mu = mu_ref[b, at, :]
        rstd = rstd_ref[b, at, :]
        for d in range(0, width, BLK):
            cols = slice(d, d + BLK)
            da = dot_nn(dqkv, wq_ref[:, cols])
            xh = (x_ref[b, at, cols].astype(F32) - mu) * rstd
            t_ref[b, at, cols] += da * ln_ref[0:1, cols]
            acc_ref[0, :, cols] += fold8(da * xh)
            acc_ref[1, :, cols] += fold8(da)

    def finish_rows(b, first):
        at = pl.ds(pl.multiple_of(me * rows + first, quarter), quarter)
        sub = pl.ds(first, quarter)
        t = t_ref[b, at, :] + fp_ref[b, sub, :] + fm_ref[b, sub, :]
        rstd = rstd_ref[b, at, :]
        xh = (x_ref[b, at, :].astype(F32) - mu_ref[b, at, :]) * rstd
        n = rstd * (t - jnp.mean(t, axis=-1, keepdims=True) - xh * jnp.mean(t * xh, axis=-1, keepdims=True))
        gi_ref[b, sub, :] = (dy_ref[b, at, :].astype(F32) + n).astype(BF16)

    def finish(b):
        for kind in (6, 8, 7, 9):
            ring(kind, b).wait_recv()
        finish_rows(b, 0)
        finish_rows(b, half)
        for kind in (10, 11):
            ring(kind, b).wait_recv()
        finish_rows(b, quarter)
        finish_rows(b, half + quarter)

    def gl_copy(kind, src, dst, target):
        return pltpu.make_async_remote_copy(
            src_ref=src, dst_ref=dst, send_sem=gl_send.at[kind], recv_sem=gl_recv.at[kind],
            device_id={"tp": target}, device_id_type=MESH_ID)

    def from_chip(off):
        return gl_ref.at[lax.rem(chip + off, nc)]

    gl_pair = gl_copy(0, gls_ref.at[0], gls_ref.at[1], partner)
    gl_plus = gl_copy(1, from_chip(0), from_chip(0), plus)
    gl_minus = gl_copy(2, from_chip(0), from_chip(0), minus)
    gl_far = gl_copy(3, from_chip(nc - 1), from_chip(nc - 1), plus)

    send_ring(0)
    send_partner(0)
    send_partner(1)

    for t, base in ((0, 0), (1, 2 * hd)):
        for part in range(2):
            for g in range(2):
                load_piece(g * 3 * hd + t * hd + part * hh, hh, base + part * hd + g * hh)
    for g in range(2):
        load_piece(g * 3 * hd + 2 * hd, hd, 4 * hd + g * hd)
    loads.append(pltpu.make_async_copy(wq_in, wq_ref, load_sem.at[2]))
    load(ln_in, ln_ref)
    load(cos_in, cos_ref)
    load(sin_in, sin_ref)
    load(wo_in, wo_ref)
    load(wu_in, wu_ref)
    load(wd_in, wd_ref)

    acc_ref[...] = jnp.zeros_like(acc_ref)
    for copy in loads[2:]:
        copy.wait()

    @pl.loop(0, batch)
    def _(b):
        @pl.loop(b * 2, nc + 1)
        def _(i):
            step = i - 1

            @pl.when(i == 0)
            def _():
                arrived(4, 0)
                arrived(5, 0)

            @pl.when((step == 0) & (b == 0))
            def _():
                arrived(4, 1)
                arrived(5, 1)

            @pl.when((step == 1) & (b == 0))
            def _():
                service_first(0)
                send_ring(1)
                service_second(0)

            @pl.when((step == 2) & (b == 1))
            def _():
                add_partner(0, 1)
                ring(6, 0).start()
                add_partner(0, 2)
                ring(8, 0).start()

            @pl.when(step == 1)
            def _():
                arrived(10, b)
                arrived(11, b)

            @pl.when(step == 2)
            def _():
                arrived(8, b)
                arrived(9, b)

            @pl.when(step == 3 - b)
            def _():
                service_far(b)

            @pl.when(step == 3)
            def _():
                arrived(12, b)
                arrived(13, b)

            unit(jnp.where(step == 0, 1, b), lax.rem(chip + pick(jnp.maximum(step, 0), GATHER_ORDER), nc))

        @pl.when(b == 1)
        def _():
            ring_second(0)

        dka_ref[...] = jnp.zeros_like(dka_ref)
        dva_ref[...] = jnp.zeros_like(dva_ref)

        @pl.when(b == 1)
        def _():
            for j in range(nc):
                to_partner(0, j, SCATTER_ORDER[j]).wait_send()

        @pl.loop(0, 2)
        def _(h):
            attention_head(b, h)

            @pl.when((b == 0) & (h == 0))
            def _():
                service_first(1)

        @pl.loop(0, nc)
        def _(j):
            input_grad(b, lax.rem(chip + pick(j, SCATTER_ORDER), nc))
            for jj in range(nc):
                @pl.when(j == jj)
                def _(jj=jj):
                    to_partner(b, jj, SCATTER_ORDER[jj]).start()

            @pl.when((b == 0) & (j == 1))
            def _():
                service_second(1)

            @pl.when((j == 2) & (b == 1))
            def _():
                for kind in (4, 5, 6, 8):
                    ring(kind, 0).wait_send()

            @pl.when(j == 3 - b)
            def _():
                add_partner(b, 0)
                ring(4, b).start()
                ring(5, b).start()

    for r in range(4):
        gls_ref[0, r:r + 1, :] = jnp.sum(acc_ref[r], axis=0, keepdims=True)
    gl_pair.start()
    add_partner(1, 1)
    add_partner(1, 2)
    gl_pair.wait_recv()
    gl_ref[chip] = gls_ref[0] + gls_ref[1]
    gl_plus.start()
    gl_minus.start()
    ring(6, 1).start()
    ring(8, 1).start()
    @pl.loop(0, width, step=BLK)
    def _(i):
        cols = pl.ds(pl.multiple_of(i, BLK), BLK)
        total = dot_tn(m_ref[0, :, cols], dh_ref[0])
        for b in range(1, batch):
            total += dot_tn(m_ref[b, :, cols], dh_ref[b])
        gu_ref[cols, :] = total.astype(BF16)


    @pl.loop(0, width, step=BLK)
    def _(i):
        cols = pl.ds(pl.multiple_of(i, BLK), BLK)
        total = dot_tn(u_ref[0], dy_ref[0, :, cols])
        for b in range(1, batch):
            total += dot_tn(u_ref[b], dy_ref[b, :, cols])
        gd_ref[:, cols] = total.astype(BF16)

    gl_copy(1, from_chip(nc - 1), from_chip(nc - 1), plus).wait_recv()
    gl_far.start()
    for kind in (7, 9, 10, 11):
        ring(kind, 0).wait_send()
    ring_second(1)

    @pl.loop(0, width, step=BLK)
    def _(i):
        cols = pl.ds(pl.multiple_of(i, BLK), BLK)
        total = dot_tn(dqkv_ref[0], a_ref[0, :, cols])
        out = dot_nn(ct_ref[0], dy_ref[0, :, cols])
        for b in range(1, batch):
            total += dot_tn(dqkv_ref[b], a_ref[b, :, cols])
            out += dot_nn(ct_ref[b], dy_ref[b, :, cols])
        total = total.astype(BF16)
        for t, base in ((0, 0), (1, 2 * hd)):
            for part in range(2):
                for g in range(2):
                    row, to = base + part * hd + g * hh, g * 3 * hd + t * hd + part * hh
                    gq_ref[to:to + hh, cols] = total[row:row + hh]
        for g in range(2):
            row, to = 4 * hd + g * hd, g * 3 * hd + 2 * hd
            gq_ref[to:to + hd, cols] = total[row:row + hd]
        go_ref[:, cols] = out.astype(BF16)

    add_partner(0, 3)
    add_partner(1, 3)
    finish(0)
    gl_copy(2, from_chip(1), from_chip(1), minus).wait_recv()
    gl_copy(3, from_chip(2), from_chip(2), plus).wait_recv()
    total = gl_ref[0]
    for j in range(1, nc):
        total += gl_ref[j]
    gl_out[...] = total

    for b in range(batch):
        for kind in range(6):
            own(kind, b).wait_send()
    for kind in range(6, 14):
        forward(kind, 1).wait_send()
    for j in range(nc):
        to_partner(1, j, SCATTER_ORDER[j]).wait_send()
    for kind in (4, 5, 6, 8):
        ring(kind, 1).wait_send()
    for copy in (gl_pair, gl_plus, gl_minus, gl_far):
        copy.wait_send()
    finish(1)
    for kind in (7, 9, 10, 11):
        ring(kind, 1).wait_send()


def store_kernel(*refs):
    n = len(refs) // 2
    copies = []
    for src, dst in zip(refs[:n], refs[n:2 * n]):
        parts = STORE_PARTS if src.shape[-2] % (16 * STORE_PARTS) == 0 else 1
        step = src.shape[-2] // parts
        for i in range(parts):
            at = (slice(None),) * (len(src.shape) - 2) + (pl.ds(i * step, step), slice(None))
            copies.append(pltpu.make_async_copy(src.at[at], dst.at[at], refs[2 * n].at[len(copies)]))
    for copy in copies:
        copy.start()
    for copy in copies:
        copy.wait()


def rope_tables(seq_len, head_dim):
    half_dim = head_dim // 2
    inv_freq = np.float32(ROPE_BASE) ** (np.float32(-2.0) * np.arange(half_dim, dtype=np.float32) / np.float32(head_dim))
    angles = np.arange(seq_len, dtype=np.float32)[:, None] * inv_freq[None, :]
    cos, sin = np.cos(angles), np.sin(angles)
    return jnp.asarray(np.concatenate([cos] * 4, axis=1)), jnp.asarray(np.concatenate([-sin, -sin, sin, sin], axis=1))


def solution(mesh):
    act_spec = P('dp', 'tp', None)
    nt = mesh.shape['tp']
    nc = nt // 2

    def device_step(layer_in, grad_out, w_qkv, w_out, w_up, w_down, ln_params):
        batch, rows, width = layer_in.shape
        seq = rows * nt
        groups, _, hd = w_qkv.shape[1:]
        ff = w_up.shape[1]
        wq = jnp.transpose(w_qkv, (1, 2, 3, 0)).reshape(groups * 3 * hd, width)
        wo = w_out.reshape(groups * hd, width)
        cos, sin = rope_tables(seq, hd)
        lanes = groups * hd
        any_spec = pl.BlockSpec(memory_space=pl.ANY)
        vmem_spec = pl.BlockSpec(memory_space=pltpu.VMEM)
        vm = pltpu.VMEM
        dma = pltpu.SemaphoreType.DMA
        shapes = (
            jax.ShapeDtypeStruct((batch, rows, width), BF16),
            jax.ShapeDtypeStruct((groups * 3 * hd, width), BF16),
            jax.ShapeDtypeStruct((lanes, width), BF16),
            jax.ShapeDtypeStruct((width, ff), BF16),
            jax.ShapeDtypeStruct((ff, width), BF16),
            jax.ShapeDtypeStruct((4, width), F32),
        )
        outs = pl.pallas_call(
            functools.partial(layer_kernel, nt),
            out_shape=tuple(vm(shape.shape, shape.dtype) for shape in shapes),
            in_specs=[any_spec] * 9,
            out_specs=(vmem_spec,) * 6,
            scratch_shapes=[
                vm((batch, seq, width), BF16), vm((batch, seq, width), BF16),
                vm((batch, seq, width), BF16), vm((batch, seq, width), BF16),
                vm((groups * 3 * hd, width), BF16), vm((lanes, width), BF16), vm((width, ff), BF16), vm((ff, width), BF16),
                vm((seq, lanes), F32), vm((seq, lanes), F32),
                vm((batch, seq, lanes), BF16), vm((batch, seq, lanes), BF16), vm((batch, seq, lanes), BF16), vm((batch, seq, lanes), BF16),
                vm((batch, lanes, seq), BF16), vm((batch, lanes, seq), BF16),
                vm((batch, seq, ff), BF16), vm((batch, seq, ff), BF16),
                vm((batch, seq, width), F32), vm((batch, nc, rows, width), F32),
                vm((batch, rows // 2, width), F32), vm((batch, rows // 2, width), F32),
                vm((batch, rows, width), F32), vm((batch, rows, width), F32),
                vm((batch, seq, 1), F32), vm((batch, seq, 1), F32),
                vm((seq, BLK), F32), vm((seq, BLK), F32), vm((seq, seq), BF16), vm((seq, seq), BF16),
                vm((seq, lanes), BF16), vm((seq, lanes), BF16), vm((seq, lanes), F32), vm((seq, lanes), F32),
                vm((lanes, seq), F32), vm((batch, seq, 3 * lanes), BF16), vm((batch, lanes, seq), BF16),
                vm((4, 8, width), F32), vm((nc, 4, width), F32), vm((2, 4, width), F32),
                vm((4, width), F32), dma((9,)), dma((20,)), dma((batch, 14)), dma((12,)), dma((batch, 12)), dma((4,)), dma((4,)),
            ],
            compiler_params=pltpu.CompilerParams(collective_id=0, has_side_effects=True, vmem_limit_bytes=VMEM_LIMIT),
            name="layer_backward",
        )(layer_in, grad_out, wq, wo, w_up, w_down, ln_params, cos, sin)
        outs = pl.pallas_call(
            store_kernel,
            out_shape=shapes,
            in_specs=[vmem_spec] * 6,
            out_specs=(any_spec,) * 6,
            scratch_shapes=[dma((6 * STORE_PARTS,))],
            compiler_params=pltpu.CompilerParams(vmem_limit_bytes=1 << 20),
            name="store_outputs",
        )(*(pltpu.with_memory_space_constraint(out, pltpu.VMEM) for out in outs))
        grad_in, gq, go, gu, gd, gl = outs
        gq = jnp.transpose(gq.reshape(groups, 3, hd, width), (3, 0, 1, 2))
        return grad_in, gq, go.reshape(w_out.shape), gu, gd, gl

    return jax.shard_map(
        device_step,
        mesh=mesh,
        in_specs=(act_spec, act_spec, P(None, 'tp', None, None), P('tp', None, None, None), P(None, 'tp'), P('tp', None), P(None, None)),
        out_specs=(act_spec, P('dp', 'tp', None, None), P(('dp', 'tp'), None, None, None), P('dp', 'tp'), P(('dp', 'tp'), None), P('dp', None)),
        check_vma=False,
    )
```

```python
import functools

import jax
import jax.numpy as jnp
import numpy as np
from jax import lax
from jax.experimental import pallas as pl
from jax.experimental.pallas import tpu as pltpu
from jax.sharding import PartitionSpec as P

NORM_EPS = 1e-5
ROPE_BASE = 10000.0
NEG_BIG = -1e30
LOG2E = 1.4426950408889634
SQRT_HALF = 0.7071067811865476
INV_SQRT_2PI = 0.3989422804014327
F32 = jnp.float32
BF16 = jnp.bfloat16
MESH_ID = pl.DeviceIdType.MESH
BLK = 256
LN_ROWS = 32
STORE_PARTS = 1
KEY_BLK = 128
VMEM_LIMIT = 62000000
GATHER_ORDER = (0, 1, 3, 2)
SCATTER_ORDER = (2, 1, 3, 0)


def pick(index, values):
    out = values[-1]
    for i in range(len(values) - 2, -1, -1):
        out = jnp.where(index == i, values[i], out)
    return out


def dot_nn(lhs, rhs):
    return lax.dot_general(lhs, rhs, (((1,), (0,)), ((), ())), preferred_element_type=F32)


def dot_nt(lhs, rhs):
    return lax.dot_general(lhs, rhs, (((1,), (1,)), ((), ())), preferred_element_type=F32)


def dot_tn(lhs, rhs):
    return lax.dot_general(lhs, rhs, (((0,), (0,)), ((), ())), preferred_element_type=F32)


def fold8(value):
    rows, cols = value.shape
    return jnp.sum(value.reshape(rows // 8, 8, cols), axis=0)


def layer_kernel(nt, x_in, dy_in, wq_in, wo_in, wu_in, wd_in, ln_in, cos_in, sin_in,
                 gi_ref, gq_ref, go_ref, gu_ref, gd_ref, gl_out,
                 x_ref, dy_ref, a_ref, m_ref, wq_ref, wo_ref, wu_ref, wd_ref, cos_ref, sin_ref,
                 q_ref, k_ref, v_ref, dc_ref, kt_ref, vt_ref, u_ref, dh_ref, t_ref, p_ref,
                 hp_ref, hm_ref, fp_ref, fm_ref, mu_ref, rstd_ref, s_ref, dp_ref, pt_ref, ds_ref,
                 qm_ref, dcm_ref, dka_ref, dva_ref, dqt_ref, dqkv_ref, ct_ref, acc_ref, gl_ref, gls_ref,
                 ln_ref, load_sem, ag_send, ag_recv, rs_send, rs_recv, gl_send, gl_recv):
    nc = nt // 2
    batch, seq, width = x_ref.shape
    ff = wu_ref.shape[1]
    rows = x_in.shape[1]
    half = rows // 2
    quarter = rows // 4
    pair = 2 * rows
    hd = wo_in.shape[0] // 2
    hh = hd // 2
    scale = hd ** -0.5

    me = lax.axis_index("tp")
    chip = me // 2
    core = lax.rem(me, 2)
    partner = chip * 2 + (1 - core)

    def dev(off, which):
        return lax.rem(chip + off, nc) * 2 + which

    plus = dev(1, core)
    minus = dev(nc - 1, core)

    def row0(device):
        return pl.multiple_of(device * rows, rows)

    loads = []

    def load(src, dst):
        loads.append(pltpu.make_async_copy(src, dst, load_sem.at[len(loads)]))
        loads[-1].start()

    def load_piece(first, count, to):
        pltpu.make_async_copy(wq_in.at[pl.ds(first, count), :], wq_ref.at[pl.ds(to, count), :], load_sem.at[2]).start()

    load(x_in, x_ref.at[:, pl.ds(row0(me), rows), :])
    load(dy_in, dy_ref.at[:, pl.ds(row0(me), rows), :])

    barrier = pltpu.get_barrier_semaphore()
    for target in (plus, minus, partner):
        pl.semaphore_signal(barrier, inc=1, device_id={"tp": target}, device_id_type=MESH_ID)

    loads[0].wait()
    loads[1].wait()
    pl.semaphore_wait(barrier, 3)

    def ag(kind, src, dst, b, target):
        send = ag_send.at[b * 6 + kind] if kind < 6 else ag_send.at[6 + kind]
        return pltpu.make_async_remote_copy(
            src_ref=src, dst_ref=dst, send_sem=send, recv_sem=ag_recv.at[b, kind],
            device_id={"tp": target}, device_id_type=MESH_ID)

    def rows_of(ref, b, device):
        return ref.at[b, pl.ds(row0(device), rows), :]

    def own(kind, b):
        ref = (x_ref, dy_ref)[kind % 2]
        target = (plus, minus, partner)[kind // 2]
        return ag(kind, rows_of(ref, b, me), rows_of(ref, b, me), b, target)

    def forward(kind, b):
        if kind == 6:
            return ag(kind, rows_of(x_ref, b, minus), rows_of(x_ref, b, minus), b, plus)
        if kind == 7:
            return ag(kind, rows_of(dy_ref, b, plus), rows_of(dy_ref, b, plus), b, minus)
        ref = (x_ref, dy_ref)[kind % 2]
        source = dev((nc - 1, 1, 2)[(kind - 8) // 2], core)
        return ag(kind, rows_of(ref, b, source), rows_of(ref, b, source), b, partner)

    def arrived(kind, b):
        ref = (x_ref, dy_ref)[kind % 2]
        if kind < 6:
            source = (minus, plus, partner)[kind // 2]
        elif kind < 8:
            source = dev(2, core)
        else:
            source = dev((nc - 1, 1, 2)[(kind - 8) // 2], 1 - core)
        ag(kind, rows_of(ref, b, source), rows_of(ref, b, source), b, partner).wait_recv()

    def send_ring(b):
        for kind in (0, 3, 1, 2):
            own(kind, b).start()

    def send_partner(b):
        for kind in (4, 5):
            own(kind, b).start()

    def service_first(b):
        if b == 1:
            for kind in range(6, 14):
                forward(kind, 0).wait_send()
        arrived(0, b)
        forward(6, b).start()
        forward(8, b).start()
        arrived(3, b)
        forward(7, b).start()
        forward(11, b).start()

    def service_second(b):
        arrived(2, b)
        forward(10, b).start()
        arrived(1, b)
        forward(9, b).start()

    def service_far(b):
        arrived(6, b)
        forward(12, b).start()
        arrived(7, b)
        forward(13, b).start()

    def rs(kind, src, dst, b, target):
        return pltpu.make_async_remote_copy(
            src_ref=src, dst_ref=dst, send_sem=rs_send.at[kind], recv_sem=rs_recv.at[b, kind],
            device_id={"tp": target}, device_id_type=MESH_ID)

    def part_rows(b, device, first, count):
        return t_ref.at[b, pl.ds(pl.multiple_of(device * rows + first, quarter), count), :]

    def to_partner(b, j, off):
        return rs(j, part_rows(b, dev(off, 1 - core), 0, rows), p_ref.at[b, j], b, partner)

    def ring(kind, b):
        if kind < 6:
            to, ref = ((plus, hp_ref), (minus, hm_ref))[kind - 4]
            return rs(kind, part_rows(b, dev(2, core), (kind - 4) * half, half), ref.at[b], b, to)
        to, ref, first, count = {
            6: (plus, fp_ref, half, half), 7: (plus, fp_ref, 0, quarter), 10: (plus, fp_ref, quarter, quarter),
            8: (minus, fm_ref, 0, half), 9: (minus, fm_ref, half, quarter), 11: (minus, fm_ref, half + quarter, quarter),
        }[kind]
        return rs(kind, part_rows(b, to, first, count), ref.at[b, pl.ds(first, count), :], b, to)

    def add_partner(b, j):
        target = dev(SCATTER_ORDER[j], core)
        rs(j, part_rows(b, target, 0, rows), p_ref.at[b, j], b, partner).wait_recv()

        @pl.loop(0, rows, step=LN_ROWS)
        def _(i):
            at = pl.ds(pl.multiple_of(target * rows + i, LN_ROWS), LN_ROWS)
            t_ref[b, at, :] += p_ref[b, j, pl.ds(pl.multiple_of(i, LN_ROWS), LN_ROWS), :]

    def add_quarter(b, device, first, ref, at):
        t_ref[b, pl.ds(pl.multiple_of(device * rows + first, quarter), quarter), :] += ref[b, pl.ds(at, quarter), :]

    def ring_second(b):
        ring(4, b).wait_recv()
        add_quarter(b, plus, 0, hp_ref, 0)
        ring(7, b).start()
        ring(5, b).wait_recv()
        add_quarter(b, minus, half, hm_ref, 0)
        ring(9, b).start()
        add_quarter(b, plus, quarter, hp_ref, quarter)
        ring(10, b).start()
        add_quarter(b, minus, half + quarter, hm_ref, quarter)
        ring(11, b).start()

    def unit(b, cc):
        r0 = pl.multiple_of(cc * pair, pair)
        at = pl.ds(r0, pair)

        for i in range(0, pair, LN_ROWS):
            sub = pl.ds(pl.multiple_of(r0 + i, LN_ROWS), LN_ROWS)
            xs = x_ref[b, sub, :].astype(F32)
            mu = jnp.mean(xs, axis=-1, keepdims=True)
            xc = xs - mu
            rstd = lax.rsqrt(jnp.mean(xc * xc, axis=-1, keepdims=True) + NORM_EPS)
            xh = xc * rstd
            mu_ref[b, sub, :] = mu
            rstd_ref[b, sub, :] = rstd
            a_ref[b, sub, :] = (xh * ln_ref[0:1, :] + ln_ref[1:2, :]).astype(BF16)
            m_ref[b, sub, :] = (xh * ln_ref[2:3, :] + ln_ref[3:4, :]).astype(BF16)

        a = a_ref[b, at, :]
        dy = dy_ref[b, at, :]
        cos = cos_ref[at, :]
        sin = sin_ref[at, :]
        qk = dot_nt(a, wq_ref[0:4 * hd, :]).astype(BF16).astype(F32)
        q = qk[:, 0:2 * hd]
        q_ref[b, at, :] = (q * cos + pltpu.roll(q, hd, 1) * sin).astype(BF16)
        k = qk[:, 2 * hd:]
        k2 = k * cos + pltpu.roll(k, hd, 1) * sin
        k_ref[b, at, :] = k2.astype(BF16)
        kt_ref[b, :, at] = k2.T.astype(BF16)
        v = dot_nt(a, wq_ref[4 * hd:6 * hd, :])
        v_ref[b, at, :] = v.astype(BF16)
        vt_ref[b, :, at] = v.T.astype(BF16)
        dc_ref[b, at, :] = dot_nt(dy, wo_ref[...]).astype(BF16)

    def unit_mlp(b, cc):
        at = pl.ds(pl.multiple_of(cc * pair, pair), pair)
        dy = dy_ref[b, at, :]
        m = m_ref[b, at, :]
        for f in range(0, ff, BLK):
            h = dot_nn(m, wu_ref[:, f:f + BLK])
            du = dot_nt(dy, wd_ref[f:f + BLK, :])
            cdf = 0.5 * (1.0 + lax.erf(h * SQRT_HALF))
            pdf = jnp.exp2(h * h * (-0.5 * LOG2E)) * INV_SQRT_2PI
            u_ref[b, at, f:f + BLK] = (h * cdf).astype(BF16)
            dh_ref[b, at, f:f + BLK] = (du * (cdf + h * pdf)).astype(BF16)
        dh = dh_ref[b, at, :]
        mu = mu_ref[b, at, :]
        rstd = rstd_ref[b, at, :]
        for d in range(0, width, BLK):
            cols = slice(d, d + BLK)
            dm = dot_nt(dh, wu_ref[cols, :])
            xh = (x_ref[b, at, cols].astype(F32) - mu) * rstd
            t_ref[b, at, cols] = dm * ln_ref[2:3, cols]
            acc_ref[2, :, cols] += fold8(dm * xh)
            acc_ref[3, :, cols] += fold8(dm)

    def attention_head(b, h):
        lane = lax.broadcasted_iota(jnp.int32, (1, 2 * hd), 1)
        q_mask = lax.rem(lane // hh, 2) == h
        v_mask = (lane // hd) == h
        qm_ref[...] = jnp.where(q_mask, q_ref[b], jnp.zeros((), BF16))
        dcm_ref[...] = jnp.where(v_mask, dc_ref[b], jnp.zeros((), BF16))
        v_rows = pl.ds(pl.multiple_of(h * hd, hd), hd)
        k_lo = pl.ds(pl.multiple_of(h * hh, hh), hh)
        k_hi = pl.ds(pl.multiple_of(hd + h * hh, hh), hh)
        for qb in range(seq // BLK):
            qs = slice(qb * BLK, (qb + 1) * BLK)
            kl = (qb + 1) * BLK
            qm = qm_ref[qs, :]
            dcm = dcm_ref[qs, :]
            top = None
            for kb in range(0, kl, KEY_BLK):
                ks = slice(kb, kb + KEY_BLK)
                s = dot_nt(k_ref[b, ks, :], qm)
                if kb >= qb * BLK:
                    key = lax.broadcasted_iota(jnp.int32, (KEY_BLK, BLK), 0) + (kb - qb * BLK)
                    query = lax.broadcasted_iota(jnp.int32, (KEY_BLK, BLK), 1)
                    s = jnp.where(key <= query, s, NEG_BIG / scale)
                s_ref[ks, :] = s
                best = jnp.max(s.reshape(KEY_BLK // 8, 8, BLK), axis=0)
                top = best if top is None else jnp.maximum(top, best)
            top = jnp.max(top, axis=0, keepdims=True)
            total = jnp.zeros((8, BLK), F32)
            weighted = jnp.zeros((8, BLK), F32)
            for kb in range(0, kl, KEY_BLK):
                ks = slice(kb, kb + KEY_BLK)
                e = jnp.exp2((s_ref[ks, :] - top) * (scale * LOG2E))
                dpr = dot_nt(v_ref[b, ks, :], dcm)
                s_ref[ks, :] = e
                dp_ref[ks, :] = dpr
                total += fold8(e)
                weighted += fold8(e * dpr)
            inv = 1.0 / jnp.sum(total, axis=0, keepdims=True)
            mean_dp = jnp.sum(weighted, axis=0, keepdims=True) * inv
            for kb in range(0, kl, KEY_BLK):
                ks = slice(kb, kb + KEY_BLK)
                p = s_ref[ks, :] * inv
                pt_ref[ks, qs] = p.astype(BF16)
                ds_ref[ks, qs] = (p * (dp_ref[ks, :] - mean_dp) * scale).astype(BF16)
            c = dot_nn(vt_ref[b, v_rows, 0:kl], pt_ref[0:kl, qs])
            ct_ref[b, v_rows, qs] = c.astype(BF16)
            kt = jnp.concatenate([kt_ref[b, k_lo, 0:kl], kt_ref[b, k_hi, 0:kl]], axis=0)
            dq = dot_nn(kt, ds_ref[0:kl, qs])
            dqt_ref[k_lo, qs] = dq[0:hh]
            dqt_ref[k_hi, qs] = dq[hh:hd]
        for kb in range(seq // BLK):
            ks = slice(kb * BLK, (kb + 1) * BLK)
            dva_ref[ks, :] += dot_nn(pt_ref[ks, kb * BLK:], dcm_ref[kb * BLK:, :])
            dka_ref[ks, :] += dot_nn(ds_ref[ks, kb * BLK:], qm_ref[kb * BLK:, :])

    def input_grad(b, cc):
        at = pl.ds(pl.multiple_of(cc * pair, pair), pair)
        cos = cos_ref[at, :]
        sin = sin_ref[at, :]
        dq = dqt_ref[:, at].T
        dqkv_ref[b, at, 0:2 * hd] = (dq * cos - pltpu.roll(dq, hd, 1) * sin).astype(BF16)
        dk = dka_ref[at, :]
        dqkv_ref[b, at, 2 * hd:4 * hd] = (dk * cos - pltpu.roll(dk, hd, 1) * sin).astype(BF16)
        dqkv_ref[b, at, 4 * hd:6 * hd] = dva_ref[at, :].astype(BF16)
        dqkv = dqkv_ref[b, at, :]
        mu = mu_ref[b, at, :]
        rstd = rstd_ref[b, at, :]
        for d in range(0, width, BLK):
            cols = slice(d, d + BLK)
            da = dot_nn(dqkv, wq_ref[:, cols])
            xh = (x_ref[b, at, cols].astype(F32) - mu) * rstd
            t_ref[b, at, cols] += da * ln_ref[0:1, cols]
            acc_ref[0, :, cols] += fold8(da * xh)
            acc_ref[1, :, cols] += fold8(da)

    def finish_rows(b, first):
        at = pl.ds(pl.multiple_of(me * rows + first, quarter), quarter)
        sub = pl.ds(first, quarter)
        t = t_ref[b, at, :] + fp_ref[b, sub, :] + fm_ref[b, sub, :]
        rstd = rstd_ref[b, at, :]
        xh = (x_ref[b, at, :].astype(F32) - mu_ref[b, at, :]) * rstd
        n = rstd * (t - jnp.mean(t, axis=-1, keepdims=True) - xh * jnp.mean(t * xh, axis=-1, keepdims=True))
        gi_ref[b, sub, :] = (dy_ref[b, at, :].astype(F32) + n).astype(BF16)

    def finish(b):
        for kind in (6, 8, 7, 9):
            ring(kind, b).wait_recv()
        finish_rows(b, 0)
        finish_rows(b, half)
        for kind in (10, 11):
            ring(kind, b).wait_recv()
        finish_rows(b, quarter)
        finish_rows(b, half + quarter)

    def gl_copy(kind, src, dst, target):
        return pltpu.make_async_remote_copy(
            src_ref=src, dst_ref=dst, send_sem=gl_send.at[kind], recv_sem=gl_recv.at[kind],
            device_id={"tp": target}, device_id_type=MESH_ID)

    def from_chip(off):
        return gl_ref.at[lax.rem(chip + off, nc)]

    gl_pair = gl_copy(0, gls_ref.at[0], gls_ref.at[1], partner)
    gl_plus = gl_copy(1, from_chip(0), from_chip(0), plus)
    gl_minus = gl_copy(2, from_chip(0), from_chip(0), minus)
    gl_far = gl_copy(3, from_chip(nc - 1), from_chip(nc - 1), plus)

    send_ring(0)
    send_partner(0)
    send_partner(1)

    for t, base in ((0, 0), (1, 2 * hd)):
        for part in range(2):
            for g in range(2):
                load_piece(g * 3 * hd + t * hd + part * hh, hh, base + part * hd + g * hh)
    for g in range(2):
        load_piece(g * 3 * hd + 2 * hd, hd, 4 * hd + g * hd)
    loads.append(pltpu.make_async_copy(wq_in, wq_ref, load_sem.at[2]))
    load(ln_in, ln_ref)
    load(cos_in, cos_ref)
    load(sin_in, sin_ref)
    load(wo_in, wo_ref)
    load(wu_in, wu_ref)
    load(wd_in, wd_ref)

    acc_ref[...] = jnp.zeros_like(acc_ref)
    for copy in loads[2:]:
        copy.wait()

    @pl.loop(0, batch)
    def _(b):
        @pl.loop(b * 2, nc + 1)
        def _(i):
            step = i - 1

            @pl.when(i == 0)
            def _():
                arrived(4, 0)
                arrived(5, 0)

            @pl.when((step == 0) & (b == 0))
            def _():
                arrived(4, 1)
                arrived(5, 1)

            @pl.when((step == 1) & (b == 0))
            def _():
                service_first(0)
                send_ring(1)
                service_second(0)

            @pl.when((step == 2) & (b == 1))
            def _():
                add_partner(0, 1)
                ring(6, 0).start()
                add_partner(0, 2)
                ring(8, 0).start()

            @pl.when(step == 1)
            def _():
                arrived(10, b)
                arrived(11, b)

            @pl.when(step == 2)
            def _():
                arrived(8, b)
                arrived(9, b)

            @pl.when(step == 3 - b)
            def _():
                service_far(b)

            @pl.when(step == 3)
            def _():
                arrived(12, b)
                arrived(13, b)

            which, cc = jnp.where(step == 0, 1, b), lax.rem(chip + pick(jnp.maximum(step, 0), GATHER_ORDER), nc)
            unit(which, cc)

            @pl.when((b == 0) | (step == 3))
            def _():
                unit_mlp(which, cc)

        @pl.when(b == 1)
        def _():
            ring_second(0)

        dka_ref[...] = jnp.zeros_like(dka_ref)
        dva_ref[...] = jnp.zeros_like(dva_ref)

        @pl.when(b == 1)
        def _():
            for j in range(nc):
                to_partner(0, j, SCATTER_ORDER[j]).wait_send()

        @pl.loop(0, 2)
        def _(h):
            attention_head(b, h)

            @pl.when((b == 0) & (h == 0))
            def _():
                service_first(1)

        @pl.loop(0, nc)
        def _(j):
            @pl.when((b == 1) & (j > 0) & (j < 3))
            def _():
                unit_mlp(1, lax.rem(chip + pick(j, SCATTER_ORDER), nc))

            input_grad(b, lax.rem(chip + pick(j, SCATTER_ORDER), nc))
            for jj in range(nc):
                @pl.when(j == jj)
                def _(jj=jj):
                    to_partner(b, jj, SCATTER_ORDER[jj]).start()

            @pl.when((b == 0) & (j == 1))
            def _():
                service_second(1)

            @pl.when((j == 1) & (b == 1))
            def _():
                for kind in (4, 5, 6, 8):
                    ring(kind, 0).wait_send()

            @pl.when(j == 3 - 2 * b)
            def _():
                add_partner(b, 0)
                ring(4, b).start()
                ring(5, b).start()

    for r in range(4):
        gls_ref[0, r:r + 1, :] = jnp.sum(acc_ref[r], axis=0, keepdims=True)
    gl_pair.start()
    add_partner(1, 1)
    add_partner(1, 2)
    gl_pair.wait_recv()
    gl_ref[chip] = gls_ref[0] + gls_ref[1]
    gl_plus.start()
    gl_minus.start()
    ring(6, 1).start()
    ring(8, 1).start()
    @pl.loop(0, width, step=BLK)
    def _(i):
        cols = pl.ds(pl.multiple_of(i, BLK), BLK)
        total = dot_tn(m_ref[0, :, cols], dh_ref[0])
        for b in range(1, batch):
            total += dot_tn(m_ref[b, :, cols], dh_ref[b])
        gu_ref[cols, :] = total.astype(BF16)


    @pl.loop(0, width, step=BLK)
    def _(i):
        cols = pl.ds(pl.multiple_of(i, BLK), BLK)
        total = dot_tn(u_ref[0], dy_ref[0, :, cols])
        for b in range(1, batch):
            total += dot_tn(u_ref[b], dy_ref[b, :, cols])
        gd_ref[:, cols] = total.astype(BF16)

    gl_copy(1, from_chip(nc - 1), from_chip(nc - 1), plus).wait_recv()
    gl_far.start()
    for kind in (7, 9, 10, 11):
        ring(kind, 0).wait_send()
    ring_second(1)

    @pl.loop(0, width, step=BLK)
    def _(i):
        cols = pl.ds(pl.multiple_of(i, BLK), BLK)
        total = dot_tn(dqkv_ref[0], a_ref[0, :, cols])
        out = dot_nn(ct_ref[0], dy_ref[0, :, cols])
        for b in range(1, batch):
            total += dot_tn(dqkv_ref[b], a_ref[b, :, cols])
            out += dot_nn(ct_ref[b], dy_ref[b, :, cols])
        total = total.astype(BF16)
        for t, base in ((0, 0), (1, 2 * hd)):
            for part in range(2):
                for g in range(2):
                    row, to = base + part * hd + g * hh, g * 3 * hd + t * hd + part * hh
                    gq_ref[to:to + hh, cols] = total[row:row + hh]
        for g in range(2):
            row, to = 4 * hd + g * hd, g * 3 * hd + 2 * hd
            gq_ref[to:to + hd, cols] = total[row:row + hd]
        go_ref[:, cols] = out.astype(BF16)

    add_partner(0, 3)
    add_partner(1, 3)
    finish(0)
    gl_copy(2, from_chip(1), from_chip(1), minus).wait_recv()
    gl_copy(3, from_chip(2), from_chip(2), plus).wait_recv()
    total = gl_ref[0]
    for j in range(1, nc):
        total += gl_ref[j]
    gl_out[...] = total

    for b in range(batch):
        for kind in range(6):
            own(kind, b).wait_send()
    for kind in range(6, 14):
        forward(kind, 1).wait_send()
    for j in range(nc):
        to_partner(1, j, SCATTER_ORDER[j]).wait_send()
    for kind in (4, 5, 6, 8):
        ring(kind, 1).wait_send()
    for copy in (gl_pair, gl_plus, gl_minus, gl_far):
        copy.wait_send()
    finish(1)
    for kind in (7, 9, 10, 11):
        ring(kind, 1).wait_send()


def store_kernel(*refs):
    n = len(refs) // 2
    copies = []
    for src, dst in zip(refs[:n], refs[n:2 * n]):
        parts = STORE_PARTS if src.shape[-2] % (16 * STORE_PARTS) == 0 else 1
        step = src.shape[-2] // parts
        for i in range(parts):
            at = (slice(None),) * (len(src.shape) - 2) + (pl.ds(i * step, step), slice(None))
            copies.append(pltpu.make_async_copy(src.at[at], dst.at[at], refs[2 * n].at[len(copies)]))
    for copy in copies:
        copy.start()
    for copy in copies:
        copy.wait()


def rope_tables(seq_len, head_dim):
    half_dim = head_dim // 2
    inv_freq = np.float32(ROPE_BASE) ** (np.float32(-2.0) * np.arange(half_dim, dtype=np.float32) / np.float32(head_dim))
    angles = np.arange(seq_len, dtype=np.float32)[:, None] * inv_freq[None, :]
    cos, sin = np.cos(angles), np.sin(angles)
    return jnp.asarray(np.concatenate([cos] * 4, axis=1)), jnp.asarray(np.concatenate([-sin, -sin, sin, sin], axis=1))


def solution(mesh):
    act_spec = P('dp', 'tp', None)
    nt = mesh.shape['tp']
    nc = nt // 2

    def device_step(layer_in, grad_out, w_qkv, w_out, w_up, w_down, ln_params):
        batch, rows, width = layer_in.shape
        seq = rows * nt
        groups, _, hd = w_qkv.shape[1:]
        ff = w_up.shape[1]
        wq = jnp.transpose(w_qkv, (1, 2, 3, 0)).reshape(groups * 3 * hd, width)
        wo = w_out.reshape(groups * hd, width)
        cos, sin = rope_tables(seq, hd)
        lanes = groups * hd
        any_spec = pl.BlockSpec(memory_space=pl.ANY)
        vmem_spec = pl.BlockSpec(memory_space=pltpu.VMEM)
        vm = pltpu.VMEM
        dma = pltpu.SemaphoreType.DMA
        shapes = (
            jax.ShapeDtypeStruct((batch, rows, width), BF16),
            jax.ShapeDtypeStruct((groups * 3 * hd, width), BF16),
            jax.ShapeDtypeStruct((lanes, width), BF16),
            jax.ShapeDtypeStruct((width, ff), BF16),
            jax.ShapeDtypeStruct((ff, width), BF16),
            jax.ShapeDtypeStruct((4, width), F32),
        )
        outs = pl.pallas_call(
            functools.partial(layer_kernel, nt),
            out_shape=tuple(vm(shape.shape, shape.dtype) for shape in shapes),
            in_specs=[any_spec] * 9,
            out_specs=(vmem_spec,) * 6,
            scratch_shapes=[
                vm((batch, seq, width), BF16), vm((batch, seq, width), BF16),
                vm((batch, seq, width), BF16), vm((batch, seq, width), BF16),
                vm((groups * 3 * hd, width), BF16), vm((lanes, width), BF16), vm((width, ff), BF16), vm((ff, width), BF16),
                vm((seq, lanes), F32), vm((seq, lanes), F32),
                vm((batch, seq, lanes), BF16), vm((batch, seq, lanes), BF16), vm((batch, seq, lanes), BF16), vm((batch, seq, lanes), BF16),
                vm((batch, lanes, seq), BF16), vm((batch, lanes, seq), BF16),
                vm((batch, seq, ff), BF16), vm((batch, seq, ff), BF16),
                vm((batch, seq, width), F32), vm((batch, nc, rows, width), F32),
                vm((batch, rows // 2, width), F32), vm((batch, rows // 2, width), F32),
                vm((batch, rows, width), F32), vm((batch, rows, width), F32),
                vm((batch, seq, 1), F32), vm((batch, seq, 1), F32),
                vm((seq, BLK), F32), vm((seq, BLK), F32), vm((seq, seq), BF16), vm((seq, seq), BF16),
                vm((seq, lanes), BF16), vm((seq, lanes), BF16), vm((seq, lanes), F32), vm((seq, lanes), F32),
                vm((lanes, seq), F32), vm((batch, seq, 3 * lanes), BF16), vm((batch, lanes, seq), BF16),
                vm((4, 8, width), F32), vm((nc, 4, width), F32), vm((2, 4, width), F32),
                vm((4, width), F32), dma((9,)), dma((20,)), dma((batch, 14)), dma((12,)), dma((batch, 12)), dma((4,)), dma((4,)),
            ],
            compiler_params=pltpu.CompilerParams(collective_id=0, has_side_effects=True, vmem_limit_bytes=VMEM_LIMIT),
            name="layer_backward",
        )(layer_in, grad_out, wq, wo, w_up, w_down, ln_params, cos, sin)
        outs = pl.pallas_call(
            store_kernel,
            out_shape=shapes,
            in_specs=[vmem_spec] * 6,
            out_specs=(any_spec,) * 6,
            scratch_shapes=[dma((6 * STORE_PARTS,))],
            compiler_params=pltpu.CompilerParams(vmem_limit_bytes=1 << 20),
            name="store_outputs",
        )(*(pltpu.with_memory_space_constraint(out, pltpu.VMEM) for out in outs))
        grad_in, gq, go, gu, gd, gl = outs
        gq = jnp.transpose(gq.reshape(groups, 3, hd, width), (3, 0, 1, 2))
        return grad_in, gq, go.reshape(w_out.shape), gu, gd, gl

    return jax.shard_map(
        device_step,
        mesh=mesh,
        in_specs=(act_spec, act_spec, P(None, 'tp', None, None), P('tp', None, None, None), P(None, 'tp'), P('tp', None), P(None, None)),
        out_specs=(act_spec, P('dp', 'tp', None, None), P(('dp', 'tp'), None, None, None), P('dp', 'tp'), P(('dp', 'tp'), None), P('dp', None)),
        check_vma=False,
    )
```
